32 devices in a mesh: gx: 8 (over z, y), gy: 4 (over x, core).
Axes of the slice: x: 2, y: 2, z: 4, core: 2. Of those that a mesh axis runs over, the one named last changes fastest.
Arguments:
- right_side: float32 [64, 128, 128], P('gy', 'gx'), may hold values from -6 to 9
- diagonal: float32 [64, 128, 128], P('gy', 'gx'), may hold values from 0.02 to 0.5
- horizontal: float32 [64, 128, 128], P('gy', 'gx'), may hold values from 0.1 to 1
- vertical: float32 [128], replicated, may hold values from 0.2 to 2
- precond: float32 [2, 128, 128], replicated, may hold values from -4 to 4
- edge_rows: int32 [2, 64], replicated, may hold values from 0 to 63, as said below
Outputs:
- solution_field: float32 [64, 128, 128], P('gy', 'gx')
- residual: float32 [64, 128, 128], P('gy', 'gx')
- residual_sq: float32 [3], replicated
The draws below stay inside these ranges and needn't reach their ends.
Inputs may be any that keep to these rules, and one draw needn't show every extreme that they name: Each row of edge_rows lists every number 0 to 63 exactly once.
All inputs are finite; a program needn't handle non-finite values.
Results may differ from the reference program's by a relative error of at most 0.00014.
Values sent between devices are 32-bit elements; how exact they have to be, the bound alone decides.
A program may use at most 64 MiB of HBM per device.

```python
import math
import jax
import jax.numpy as jnp
from jax import lax

LEV = 128
ITERS = 3
NX = 128
NY = 64


def draw_right_side(key, part):
    base = jnp.clip(jax.random.normal(key, (NY, NX, LEV), jnp.float32), -6.0, 6.0)
    return base


def draw_precond(key, part):
    keys = jax.random.split(key, 3)
    extra = jax.random.uniform(keys[0], (2, LEV), jnp.float32, 0.3, 1.0)
    couple = jax.random.uniform(keys[1], (2, LEV - 1), jnp.float32, 0.5, 2.0)
    padded = jnp.pad(couple, ((0, 0), (1, 1)))
    main = extra + padded[:, :-1] + padded[:, 1:]
    couple_row = jnp.pad(couple, ((0, 0), (0, 1)))
    upper = jnp.eye(LEV, k=1, dtype=jnp.float32)
    lower = jnp.eye(LEV, k=-1, dtype=jnp.float32)
    eye = jnp.eye(LEV, dtype=jnp.float32)
    tri = main[:, :, None] * eye[None] - couple_row[:, :, None] * upper[None] - couple_row[:, None, :] * lower[None]
    inverse = jnp.linalg.inv(tri)
    size = jnp.mean(jnp.abs(jnp.diagonal(inverse, axis1=1, axis2=2)), axis=1)
    noise = jax.random.normal(keys[2], (2, LEV, LEV), jnp.float32)
    return inverse + 0.05 * size[:, None, None] * noise


def draw_edge_rows(key, part):
    first = jax.random.permutation(jax.random.fold_in(key, 11), NY).astype(jnp.int32)
    second = jax.random.permutation(jax.random.fold_in(key, 23), NY).astype(jnp.int32)
    return jnp.stack([first, second]).astype(jnp.int32)


def block_scale(rng, dims, pieces, least, largest):
    loudness = 1.0
    for dim, parts in pieces:
        draws = jax.random.uniform(jax.random.fold_in(jax.random.fold_in(rng, 6), dim), (parts,), jnp.float32, least / len(pieces), largest / len(pieces))
        loudness = loudness * jnp.repeat(jnp.exp(draws), dims[dim] // parts).reshape((-1,) + (1,) * (len(dims) - 1 - dim))
    return loudness


def setup_inputs(seed: int = 0) -> dict:
    seeds = jax.random.split(jax.random.key(seed), 7)
    right_side = draw_right_side(jax.random.fold_in(seeds[6], 71), 0)
    diagonal = jnp.clip(jnp.exp(math.log(0.5) - 3.218876 * jax.random.uniform(seeds[1], (NY, NX, LEV), jnp.float32) ** block_scale(seeds[1], (NY, NX, LEV), ((0, 4), (1, 8)), -0.2, 0.2)), 0.02, 0.5)
    horizontal = jnp.clip(jnp.exp(math.log(1.0) - 2.3025851 * jax.random.uniform(seeds[2], (NY, NX, LEV), jnp.float32) ** block_scale(seeds[2], (NY, NX, LEV), ((0, 4), (1, 8)), -0.2, 0.2)), 0.1, 1.0)
    vertical = jnp.clip(jnp.exp(jax.random.uniform(seeds[3], (LEV,), jnp.float32, math.log(0.2), math.log(2.0))), 0.2, 2.0)
    precond = draw_precond(jax.random.fold_in(seeds[6], 71), 0)
    edge_rows = draw_edge_rows(jax.random.fold_in(seeds[6], 71), 0)
    return dict(right_side=right_side, diagonal=diagonal, horizontal=horizontal, vertical=vertical, precond=precond, edge_rows=edge_rows)


def operate(field, diagonal, horizontal, vertical, edge_rows):
    width = field.shape[1]
    half = width // 2
    east = jnp.roll(field, -1, 1)
    east = east.at[:, half - 1].set(field[edge_rows[0], half]).at[:, width - 1].set(field[edge_rows[1], 0])
    west = jnp.roll(field, 1, 1)
    west = west.at[:, half].set(field[edge_rows[0], half - 1]).at[:, 0].set(field[edge_rows[1], width - 1])
    tall = jnp.pad(field, ((1, 1), (0, 0), (0, 0)))
    flat = jnp.pad(field, ((0, 0), (0, 0), (1, 1)))
    beside = east + west + tall[2:] + tall[:-2]
    column = flat[:, :, 2:] + flat[:, :, :-2]
    return diagonal * field + horizontal * (4.0 * field - beside) + vertical * (2.0 * field - column)

def precondition(field, precond):
    half = field.shape[1] // 2
    left = jnp.einsum('yxl,kl->yxk', field[:, :half], precond[0], precision=lax.Precision.HIGHEST)
    right = jnp.einsum('yxl,kl->yxk', field[:, half:], precond[1], precision=lax.Precision.HIGHEST)
    return jnp.concatenate([left, right], 1)

def reference(right_side, diagonal, horizontal, vertical, precond, edge_rows):
    total_cells = float(right_side.size)

    def inner(left, right):
        return jnp.sum(left * right) / total_cells
    solution_field = jnp.zeros_like(right_side)
    residual = right_side
    directions = []
    images = []
    norms = []
    for step in range(ITERS):
        pre = precondition(residual, precond)
        image = operate(pre, diagonal, horizontal, vertical, edge_rows)
        coeffs = [inner(image, older) for older in images]
        for number in range(len(images)):
            pre = pre - coeffs[number] * directions[number]
            image = image - coeffs[number] * images[number]
        scale = 1.0 / jnp.sqrt(inner(image, image))
        direction = pre * scale
        image = image * scale
        alpha = inner(residual, image)
        solution_field = solution_field + alpha * direction
        residual = residual - alpha * image
        norms.append(inner(residual, residual))
        directions.append(direction)
        images.append(image)
    return (solution_field, residual, jnp.stack(norms))
```

```python
import functools

import jax
import jax.numpy as jnp
from jax import lax
from jax.experimental import pallas as pl
from jax.experimental.pallas import tpu as pltpu
from jax.sharding import PartitionSpec as P

ITERS = 3
KEYS = [(i, j) for j in range(ITERS + 1) for i in range(j + 1)]
MESH = pl.DeviceIdType.MESH
ANY = pl.BlockSpec(memory_space=pl.ANY)
VMEM = pl.BlockSpec(memory_space=pltpu.VMEM)


def kernel(
    n_gx,
    n_gy,
    out_rows,
    edge_table,
    right_side,
    diagonal,
    horizontal,
    vertical,
    precond,
    fields,
    images,
    out_totals,
    r0,
    diag,
    horiz,
    vert,
    matrix,
    send_cols,
    pack,
    from_east,
    from_west,
    from_north,
    from_south,
    far_pack,
    near_pack,
    far_z,
    near_z,
    gathered,
    strip,
    outside,
    partial,
    sums,
    edge_rows,
    load_sem,
    col_send,
    east_recv,
    west_recv,
    far_send,
    far_recv,
    near_send,
    near_recv,
    row_send,
    north_recv,
    south_recv,
    sum_send,
    sum_recv,
):
    rows, levels = out_rows, r0.shape[-1]
    cells = r0.shape[0]
    cols = cells // rows
    tall = n_gy * rows
    gx, gy = lax.axis_index("gx"), lax.axis_index("gy")
    n_all = n_gx * n_gy
    half = n_gx // 2
    me = gx * n_gy + gy

    def for_others(visit):
        def step(i, carry):
            for j in range(n_gy):
                visit(lax.rem(gx + i, n_gx), lax.rem(gy + j, n_gy))
            return carry

        if n_all <= 64:
            for i in sorted(range(1, n_gx), key=lambda i: min(i, n_gx - i)):
                step(i, 0)
        else:
            lax.fori_loop(1, n_gx, step, 0)
        for j in range(1, n_gy):
            visit(gx, lax.rem(gy + j, n_gy))

    barrier = pltpu.get_barrier_semaphore()

    def greet(x, y):
        pl.semaphore_signal(barrier, inc=1, device_id=(x, y), device_id_type=MESH)

    for_others(greet)

    panel = lax.convert_element_type(gx >= half, jnp.int32)
    loads = [
        pltpu.make_async_copy(right_side, r0, load_sem.at[0]),
        pltpu.make_async_copy(precond.at[panel], matrix.at[pl.ds(0, levels)], load_sem.at[1]),
        pltpu.make_async_copy(horizontal, horiz, load_sem.at[2]),
        pltpu.make_async_copy(diagonal, diag, load_sem.at[3]),
        pltpu.make_async_copy(vertical, vert, load_sem.at[4]),
        pltpu.make_async_copy(edge_table, edge_rows, load_sem.at[5]),
        pltpu.make_async_copy(precond.at[1 - panel], matrix.at[pl.ds(levels, levels)], load_sem.at[6]),
    ]
    for load in loads:
        load.start()

    east_x, west_x = lax.rem(gx + 1, n_gx), lax.rem(gx + n_gx - 1, n_gx)
    east_border = (gx == half - 1) | (gx == n_gx - 1)
    west_border = (gx == half) | (gx == 0)
    border = east_border | west_border
    far_x = jnp.where(east_border, east_x, west_x)
    side = jnp.where(east_border, 0, 1)
    table = jnp.where((gx == half - 1) | (gx == half), 0, 1)
    edge_cols = [
        pl.ds(jnp.where(east_border, cols - 1 - i, i), rows, stride=cols) for i in range(3)
    ]
    first_row = pl.multiple_of(gy * rows, rows)
    own = pl.ds(first_row, rows)
    has_north, has_south = gy < n_gy - 1, gy > 0

    @pl.when(jnp.logical_not(has_north))
    def _():
        from_north[...] = jnp.zeros_like(from_north)

    @pl.when(jnp.logical_not(has_south))
    def _():
        from_south[...] = jnp.zeros_like(from_south)

    outside[...] = jnp.zeros_like(outside)

    def precondition(v, panels=1):
        return lax.dot_general(
            v,
            matrix[pl.ds(0, panels * levels), :],
            (((1,), (1,)), ((), ())),
            precision=lax.Precision.HIGHEST,
            preferred_element_type=jnp.float32,
        )

    def col_copy(t, side):
        buffer, recv, x = (
            (from_west, west_recv, east_x) if side == 0 else (from_east, east_recv, west_x)
        )
        return pltpu.make_async_remote_copy(
            src_ref=send_cols.at[t, pl.ds(side * rows, rows)],
            dst_ref=buffer.at[t],
            send_sem=col_send.at[t, side],
            recv_sem=recv.at[t],
            device_id=(x, gy),
            device_id_type=MESH,
        )

    def far_copy(t, g):
        return pltpu.make_async_remote_copy(
            src_ref=pack.at[pl.ds(0, 3)] if t == 0 else pack.at[3 + t],
            dst_ref=far_pack.at[:, own] if t == 0 else far_z.at[t - 1, own],
            send_sem=far_send.at[t],
            recv_sem=far_recv.at[t],
            device_id=(far_x, g),
            device_id_type=MESH,
        )

    def near_copy(t, g):
        return pltpu.make_async_remote_copy(
            src_ref=pack.at[pl.ds(0, 4)] if t == 0 else pack.at[3 + t],
            dst_ref=near_pack.at[:, own] if t == 0 else near_z.at[own],
            send_sem=near_send.at[t],
            recv_sem=near_recv.at[t],
            device_id=(gx, g),
            device_id_type=MESH,
        )

    def row_copy(t, side):
        buffer, recv, y, row = (
            (from_south, south_recv, gy + 1, cells - cols)
            if side == 0
            else (from_north, north_recv, gy - 1, 0)
        )
        return pltpu.make_async_remote_copy(
            src_ref=fields.at[t, pl.ds(row, cols)],
            dst_ref=buffer.at[t],
            send_sem=row_send.at[t, side],
            recv_sem=recv.at[t],
            device_id=(gx, y),
            device_id_type=MESH,
        )

    def send_cols_on(t, edges):
        send_cols[t] = precondition(edges)

        @pl.when(border)
        def _():
            edge = send_cols[t, pl.ds(side * rows, rows), :]
            if t == 0:
                items = [
                    edge,
                    horiz[edge_cols[0], :],
                    diag[edge_cols[0], :],
                    horiz[edge_cols[1], :],
                ]
                for k, item in enumerate(items):
                    pack[k] = item
                    near_pack[k, own, :] = item
            else:
                pack[3 + t] = edge
                if t == 1:
                    near_z[own, :] = edge

        if t == 0:
            pl.semaphore_wait(barrier, n_all - 1)

        @pl.when(border)
        def _():
            for j in sorted(range(n_gy), key=lambda j: abs(2 * j - n_gy)):
                far_copy(t, lax.rem(gy + j, n_gy)).start()
            if t < 2:
                for j in range(1, n_gy):
                    near_copy(t, lax.rem(gy + j, n_gy)).start()

        @pl.when(jnp.logical_not(east_border))
        def _():
            col_copy(t, 0).start()

        @pl.when(jnp.logical_not(west_border))
        def _():
            col_copy(t, 1).start()

    def send_rows(t):
        @pl.when(has_north)
        def _():
            row_copy(t, 0).start()

        @pl.when(has_south)
        def _():
            row_copy(t, 1).start()

    def receive_rows(t):
        @pl.when(has_north)
        def _():
            row_copy(t, 1).wait_recv()

        @pl.when(has_south)
        def _():
            row_copy(t, 0).wait_recv()

    def receive_cols(t):
        @pl.when(jnp.logical_not(east_border))
        def _():
            col_copy(t, 1).wait_recv()
            outside[pl.ds(0, rows), :] = from_east[t]

        @pl.when(jnp.logical_not(west_border))
        def _():
            col_copy(t, 0).wait_recv()
            outside[pl.ds(rows, rows), :] = from_west[t]

    col_id = lax.rem(lax.broadcasted_iota(jnp.int32, (cells, levels), 0), cols)
    east_edge = pl.ds(cols - 1, rows, stride=cols)
    west_edge = pl.ds(0, rows, stride=cols)
    south_edge = pl.ds(0, cols)
    north_edge = pl.ds(cells - cols, cols)

    def edge_columns(ref):
        return jnp.concatenate([ref[east_edge, :], ref[west_edge, :]], 0)

    def column_part(z):
        lane = lax.broadcasted_iota(jnp.int32, z.shape, 1)
        up = jnp.where(lane < levels - 1, pltpu.roll(z, levels - 1, 1), 0.0)
        down = jnp.where(lane > 0, pltpu.roll(z, 1, 1), 0.0)
        return vert[...] * (2.0 * z - (up + down))

    def inner_image(z):
        east = jnp.where(col_id < cols - 1, pltpu.roll(z, cells - 1, 0), 0.0)
        west = jnp.where(col_id > 0, pltpu.roll(z, 1, 0), 0.0)
        none = jnp.zeros((cols, levels), jnp.float32)
        north = jnp.concatenate([z[cols:], none], 0)
        south = jnp.concatenate([none, z[:-cols]], 0)
        beside = east + west + north + south
        return diag[...] * z + horiz[...] * (4.0 * z - beside) + column_part(z)

    def product(a, b):
        both = (a * b).reshape(-1, 8, levels)
        return jnp.sum(jnp.sum(both, axis=0), axis=0, keepdims=True)

    tall_id = lax.broadcasted_iota(jnp.int32, (tall, levels), 0)

    def along(w):
        north = jnp.where(tall_id < tall - 1, pltpu.roll(w, tall - 1, 0), 0.0)
        south = jnp.where(tall_id > 0, pltpu.roll(w, 1, 0), 0.0)
        return north + south

    def stencil(w, d, h):
        return d * w + h * (4.0 * w - along(w)) + column_part(w)

    def gather_rows(start, count, pairs):
        def one(y):
            row = edge_rows[table, start + y]
            for dst, src in pairs:
                gathered[dst, pl.ds(y, 1), :] = src[pl.ds(row, 1), :]

        if count <= 64:
            for y in range(count):
                one(y)
        else:

            def body(y, carry):
                one(y)
                return carry

            lax.fori_loop(0, count, body, 0)

    def wait_bytes(ref, sem):
        pltpu.make_async_copy(ref, ref, sem).wait()

    near_rest = pl.ds(0, (n_gy - 1) * rows)

    def correct_first():
        wait_bytes(far_pack, far_recv.at[0])
        wait_bytes(near_pack.at[:, near_rest], near_recv.at[0])
        gather_rows(0, tall, [(0, far_pack.at[0]), (1, near_pack.at[0])])
        b_near = -(near_pack[1] * gathered[0])
        b_far = -(far_pack[1] * gathered[1])
        strip[0] = b_near
        both = precondition(jnp.concatenate([b_near, b_far], 0), 2)
        strip[1] = both[:tall, :levels]
        strip[2] = both[tall:, levels:]

    def correct_second():
        wait_bytes(far_z.at[0], far_recv.at[1])
        wait_bytes(near_z.at[near_rest], near_recv.at[1])
        w_near, w_far = strip[1], strip[2]
        strip[3] = far_z[0] + w_far
        strip[4] = near_z[...] + w_near
        gather_rows(0, tall, [(0, strip.at[3]), (1, strip.at[4])])
        h_near, h_far = near_pack[1], far_pack[1]
        b_near = stencil(w_near, near_pack[2], h_near) - h_near * gathered[0]
        b_far = stencil(w_far, far_pack[2], h_far) - h_far * gathered[1]
        b_next = -(near_pack[3] * w_near)
        all_three = precondition(jnp.concatenate([b_near, b_next, b_far], 0), 2)
        w_edge, w_next = all_three[:tall, :levels], all_three[tall : 2 * tall, :levels]
        strip[3] = b_near
        strip[4] = b_next
        strip[5] = all_three[2 * tall :, levels:]
        strip[6] = w_edge
        strip[7] = w_next
        strip[8] = along(w_next)
        strip[9] = stencil(w_edge, near_pack[2], h_near) - h_near * w_next

    def correct_third():
        c0, c1, c2 = edge_cols
        w_edge, w_next, beside = strip[6, own, :], strip[7, own, :], strip[8, own, :]
        h1 = horiz[c1, :]
        later = diag[c1, :] * w_next + h1 * (4.0 * w_next - beside - w_edge) + column_part(w_next)
        b_third = -(horiz[c2, :] * w_next)
        gather_rows(first_row, rows, [(2, strip.at[5])])
        wait_bytes(far_z.at[1], far_recv.at[2])
        gather_rows(first_row, rows, [(3, far_z.at[1])])
        across = gathered[2, pl.ds(0, rows), :] + gathered[3, pl.ds(0, rows), :]
        b_edge = strip[9, own, :] - horiz[c0, :] * across
        none = jnp.zeros((rows, levels), jnp.float32)
        changes = [
            [strip[0, own, :], none, none],
            [strip[3, own, :], strip[4, own, :], none],
            [b_edge, later, b_third],
        ]
        before = [jnp.concatenate([r0[c, :] for c in edge_cols], 0)]
        after = [before[0]]
        for t in range(ITERS):
            old = jnp.concatenate([images[t, c, :] for c in edge_cols], 0)
            new = old + jnp.concatenate(changes[t], 0)
            before.append(old)
            after.append(new)
            for k in range(t + 1):
                images[t, edge_cols[k], :] = new[k * rows : (k + 1) * rows]
        for k, (i, j) in enumerate(KEYS):
            if j > 0:
                partial[pl.ds(k, 1), :] += product(after[i], after[j]) - product(before[i], before[j])

    for load in loads:
        load.wait()
    terms = {}
    spaces = [r0]
    send_cols_on(0, edge_columns(r0))
    edge_horiz = edge_columns(horiz)
    for t in range(ITERS):
        image = images.at[t]
        z = precondition(spaces[-1][...])
        fields[t] = z
        send_rows(t)
        newest = len(spaces) - 1
        for i in range(len(spaces)):
            terms[(i, newest)] = product(spaces[i][...], spaces[newest][...])
        image[...] = inner_image(z)
        receive_rows(t)
        image[south_edge, :] = image[south_edge, :] - horiz[south_edge, :] * from_south[t]
        image[north_edge, :] = image[north_edge, :] - horiz[north_edge, :] * from_north[t]
        inside = edge_columns(image)
        receive_cols(t)
        edges = inside - edge_horiz * outside[...]
        if t < ITERS - 1:
            send_cols_on(t + 1, edges)
        image[east_edge, :] = edges[:rows]
        image[west_edge, :] = edges[rows:]
        spaces.append(image)
    newest = len(spaces) - 1
    for i in range(len(spaces)):
        terms[(i, newest)] = product(spaces[i][...], spaces[newest][...])
    for k, key in enumerate(KEYS):
        partial[pl.ds(k, 1), :] = terms[key]

    @pl.when(border)
    def _():
        correct_first()
        correct_second()
        correct_third()

    height = -(-len(KEYS) // 8) * 8
    row_id = lax.broadcasted_iota(jnp.int32, (height, levels), 0)
    lane = lax.broadcasted_iota(jnp.int32, (height, levels), 1)
    stacked = jnp.where(row_id < len(KEYS), partial[...], 0.0)
    summed = jnp.sum(stacked, axis=1, keepdims=True)
    sums[me] = jnp.sum(jnp.where(lane == row_id, summed, 0.0), axis=0, keepdims=True)

    def tell(x, y):
        pltpu.make_async_remote_copy(
            src_ref=sums.at[me],
            dst_ref=sums.at[me],
            send_sem=sum_send,
            recv_sem=sum_recv,
            device_id=(x, y),
            device_id_type=MESH,
        ).start()

    for_others(tell)
    for t in range(ITERS):

        @pl.when(jnp.logical_not(east_border))
        def _(t=t):
            col_copy(t, 0).wait_send()

        @pl.when(jnp.logical_not(west_border))
        def _(t=t):
            col_copy(t, 1).wait_send()

        @pl.when(has_north)
        def _(t=t):
            row_copy(t, 0).wait_send()

        @pl.when(has_south)
        def _(t=t):
            row_copy(t, 1).wait_send()

    @pl.when(border)
    def _():
        wait_bytes(far_pack, far_send.at[0])
        wait_bytes(far_z.at[0], far_send.at[1])
        wait_bytes(far_z.at[1], far_send.at[2])
        wait_bytes(near_pack.at[:, near_rest], near_send.at[0])
        wait_bytes(near_z.at[near_rest], near_send.at[1])
        c0, c1, c2 = edge_cols
        fields[1, c0, :] += strip[1, own, :]
        fields[2, c0, :] += strip[6, own, :]
        fields[2, c1, :] += strip[7, own, :]

    others = sums.at[pl.ds(0, n_all - 1)]
    wait_bytes(others, sum_recv)
    out_totals[...] = jnp.sum(sums[...], axis=0)
    wait_bytes(others, sum_send)


def finish(total_cells, all_totals, r0, fields, images, out_x, out_r, out_norms, x, r, sem):
    levels = r0.shape[-1]
    totals = all_totals[...]
    value = {key: totals[:, k : k + 1] for k, key in enumerate(KEYS)}

    rho, g0, g1, g2 = value[(0, 0)], value[(0, 1)], value[(0, 2)], value[(0, 3)]
    a00, a01, a02 = value[(1, 1)], value[(1, 2)], value[(1, 3)]
    a11, a12, a22 = value[(2, 2)], value[(2, 3)], value[(3, 3)]
    l10, l20, y0 = a01 / a00, a02 / a00, g0 / a00
    d1, e12, f1 = a11 - l10 * a01, a12 - l10 * a02, g1 - l10 * g0
    l21, y1 = e12 / d1, f1 / d1
    d2, f2 = a22 - l20 * a02 - l21 * e12, g2 - l20 * g0 - l21 * f1
    y2 = f2 / d2
    norm0 = rho - y0 * g0
    norm1 = norm0 - y1 * f1
    norm2 = norm1 - y2 * f2
    y1 = y1 - l21 * y2
    y0 = y0 - l10 * y1 - l20 * y2
    norm_lane = lax.broadcasted_iota(jnp.int32, (1, levels), 1)
    norms = jnp.where(norm_lane == 0, norm0, jnp.where(norm_lane == 1, norm1, norm2))
    out_norms[...] = norms[:, :ITERS] / total_cells
    rows = r0.shape[0]
    pieces = 2 if rows % 16 == 0 else 1
    size = rows // pieces
    copies = []
    for p in range(pieces):
        span = pl.ds(p * size, size)
        x[span] = y0 * fields[0, span] + y1 * fields[1, span] + y2 * fields[2, span]
        r[span] = (
            r0[span] - y0 * images[0, span] - y1 * images[1, span] - y2 * images[2, span]
        )
        for k, (src, dst) in enumerate(((x, out_x), (r, out_r))):
            copy = pltpu.make_async_copy(src.at[span], dst.at[span], sem.at[p, k])
            copy.start()
            copies.append(copy)
    for copy in copies:
        copy.wait()


def on_device(n_gx, n_gy, right_side, diagonal, horizontal, vertical, precond, edge_rows):
    rows, cols, levels = right_side.shape
    f32 = jnp.float32
    block = (rows * cols, levels)
    column = (n_gy * rows, levels)
    sems = pltpu.SemaphoreType.DMA
    basis = pltpu.VMEM((ITERS,) + block, f32)
    fields, images, totals, start = pl.pallas_call(
        functools.partial(kernel, n_gx, n_gy, rows),
        out_shape=(basis, basis, pltpu.VMEM((1, levels), f32), pltpu.VMEM(block, f32)),
        in_specs=[ANY, ANY, ANY, ANY, ANY, ANY],
        out_specs=(VMEM, VMEM, VMEM, VMEM),
        scratch_shapes=[
            pltpu.VMEM(block, f32),
            pltpu.VMEM(block, f32),
            pltpu.VMEM((1, levels), f32),
            pltpu.VMEM((2 * levels, levels), f32),
            pltpu.VMEM((ITERS, 2 * rows, levels), f32),
            pltpu.VMEM((6, rows, levels), f32),
            pltpu.VMEM((ITERS, rows, levels), f32),
            pltpu.VMEM((ITERS, rows, levels), f32),
            pltpu.VMEM((ITERS, cols, levels), f32),
            pltpu.VMEM((ITERS, cols, levels), f32),
            pltpu.VMEM((3,) + column, f32),
            pltpu.VMEM((4,) + column, f32),
            pltpu.VMEM((2,) + column, f32),
            pltpu.VMEM(column, f32),
            pltpu.VMEM((4,) + column, f32),
            pltpu.VMEM((10,) + column, f32),
            pltpu.VMEM((2 * rows, levels), f32),
            pltpu.VMEM((16, levels), f32),
            pltpu.VMEM((n_gx * n_gy, 1, levels), f32),
            pltpu.SMEM(edge_rows.shape, jnp.int32),
            sems((7,)),
            sems((ITERS, 2)),
            sems((ITERS,)),
            sems((ITERS,)),
            sems((ITERS,)),
            sems((ITERS,)),
            sems((2,)),
            sems((2,)),
            sems((ITERS, 2)),
            sems((ITERS,)),
            sems((ITERS,)),
            sems(()),
            sems(()),
        ],
        compiler_params=pltpu.CompilerParams(collective_id=0, has_side_effects=True),
    )(
        edge_rows,
        right_side.reshape(block),
        diagonal.reshape(block),
        horizontal.reshape(block),
        vertical.reshape(1, levels),
        precond,
    )
    in_vmem = functools.partial(
        pltpu.with_memory_space_constraint, memory_space=pltpu.VMEM
    )
    total_cells = float(rows * cols * levels * n_gx * n_gy)
    x, r, norms = pl.pallas_call(
        functools.partial(finish, total_cells),
        out_shape=(
            jax.ShapeDtypeStruct(block, f32),
            jax.ShapeDtypeStruct(block, f32),
            jax.ShapeDtypeStruct((1, ITERS), f32),
        ),
        in_specs=[VMEM, VMEM, VMEM, VMEM],
        out_specs=(ANY, ANY, VMEM),
        scratch_shapes=[pltpu.VMEM(block, f32), pltpu.VMEM(block, f32), sems((2, 2))],
    )(in_vmem(totals), in_vmem(start), in_vmem(fields), in_vmem(images))
    shape = right_side.shape
    return x.reshape(shape), r.reshape(shape), norms.reshape(ITERS)


def solution(mesh):
    n_gx, n_gy = mesh.shape["gx"], mesh.shape["gy"]
    field = P("gy", "gx", None)
    return jax.shard_map(
        functools.partial(on_device, n_gx, n_gy),
        mesh=mesh,
        in_specs=(field, field, field, P(), P(), P()),
        out_specs=(field, field, P()),
        check_vma=False,
    )
```

```python
import functools

import jax
import jax.numpy as jnp
from jax import lax
from jax.experimental import pallas as pl
from jax.experimental.pallas import tpu as pltpu
from jax.sharding import PartitionSpec as P

ITERS = 3
KEYS = [(i, j) for j in range(ITERS + 1) for i in range(j + 1)]
MESH = pl.DeviceIdType.MESH
ANY = pl.BlockSpec(memory_space=pl.ANY)
VMEM = pl.BlockSpec(memory_space=pltpu.VMEM)


def kernel(
    n_gx,
    n_gy,
    out_rows,
    edge_table,
    right_side,
    diagonal,
    horizontal,
    vertical,
    precond,
    fields,
    images,
    out_totals,
    r0,
    diag,
    horiz,
    vert,
    matrix,
    send_cols,
    pack,
    from_east,
    from_west,
    from_north,
    from_south,
    far_pack,
    near_pack,
    far_z,
    near_z,
    gathered,
    strip,
    outside,
    partial,
    sums,
    edge_rows,
    load_sem,
    col_send,
    east_recv,
    west_recv,
    far_send,
    far_recv,
    near_send,
    near_recv,
    row_send,
    north_recv,
    south_recv,
    sum_send,
    sum_recv,
    from_below,
    from_above,
):
    rows, levels = out_rows, r0.shape[-1]
    cells = r0.shape[0]
    cols = cells // rows
    tall = n_gy * rows
    gx, gy = lax.axis_index("gx"), lax.axis_index("gy")
    n_all = n_gx * n_gy
    half = n_gx // 2
    me = gx * n_gy + gy

    east_x, west_x = lax.rem(gx + 1, n_gx), lax.rem(gx + n_gx - 1, n_gx)
    east_border = (gx == half - 1) | (gx == n_gx - 1)
    west_border = (gx == half) | (gx == 0)
    border = east_border | west_border

    def for_others(visit):
        def step(i, carry):
            for j in range(n_gy):
                visit(lax.rem(gx + i, n_gx), lax.rem(gy + j, n_gy))
            return carry

        if n_all <= 64:
            for i in sorted(range(1, n_gx), key=lambda i: min(i, n_gx - i)):
                step(i, 0)
        else:
            lax.fori_loop(1, n_gx, step, 0)
        for j in range(1, n_gy):
            visit(gx, lax.rem(gy + j, n_gy))

    barrier = pltpu.get_barrier_semaphore()

    def greet(x, y):
        pl.semaphore_signal(barrier, inc=1, device_id=(x, y), device_id_type=MESH)

    span = max(n_gx // 4, 2)
    n_spans = n_gx // span
    place = gx // span
    inside_span = lax.rem(gx, span)
    lowest, highest = place == 0, place == n_spans - 1
    greets_east = (inside_span == span - 1) & jnp.logical_not(east_border)
    greets_west = (inside_span == 0) & jnp.logical_not(west_border)
    for i in range(span):
        for j in range(n_gy):
            if i or j:
                greet(place * span + lax.rem(inside_span + i, span), lax.rem(gy + j, n_gy))
    for condition, x in (
        (jnp.logical_not(lowest), gx - span),
        (jnp.logical_not(highest), gx + span),
        (greets_east, gx + 1),
        (greets_west, gx - 1),
    ):

        @pl.when(condition)
        def _(x=x):
            greet(x, gy)

    n_greets = span * n_gy - 1
    for condition in (
        jnp.logical_not(lowest),
        jnp.logical_not(highest),
        greets_east,
        greets_west,
    ):
        n_greets = n_greets + lax.convert_element_type(condition, jnp.int32)

    def hand_on(token, x):
        pl.semaphore_signal(token, inc=1, device_id=(x, gy), device_id_type=MESH)

    panel = lax.convert_element_type(gx >= half, jnp.int32)
    loads = [
        pltpu.make_async_copy(right_side, r0, load_sem.at[0]),
        pltpu.make_async_copy(precond.at[panel], matrix.at[pl.ds(0, levels)], load_sem.at[1]),
        pltpu.make_async_copy(horizontal, horiz, load_sem.at[2]),
        pltpu.make_async_copy(diagonal, diag, load_sem.at[3]),
        pltpu.make_async_copy(vertical, vert, load_sem.at[4]),
        pltpu.make_async_copy(edge_table, edge_rows, load_sem.at[5]),
        pltpu.make_async_copy(precond.at[1 - panel], matrix.at[pl.ds(levels, levels)], load_sem.at[6]),
    ]
    for load in loads:
        load.start()

    pl.semaphore_wait(barrier, n_greets)

    @pl.when(jnp.logical_not(lowest))
    def _():
        pl.semaphore_wait(from_below, 1)

    @pl.when(jnp.logical_not(highest))
    def _():
        hand_on(from_below, gx + span)

    @pl.when(highest)
    def _():
        hand_on(from_above, gx - span)

    far_stage = n_spans - 2 - place

    def learn_above(t):
        @pl.when(far_stage == t)
        def _():
            pl.semaphore_wait(from_above, 1)

            @pl.when(jnp.logical_not(lowest))
            def _():
                hand_on(from_above, gx - span)

            @pl.when(border)
            def _():
                for k in range(t + 1):
                    send_far(k)

    far_x = jnp.where(east_border, east_x, west_x)
    side = jnp.where(east_border, 0, 1)
    table = jnp.where((gx == half - 1) | (gx == half), 0, 1)
    edge_cols = [
        pl.ds(jnp.where(east_border, cols - 1 - i, i), rows, stride=cols) for i in range(3)
    ]
    first_row = pl.multiple_of(gy * rows, rows)
    own = pl.ds(first_row, rows)
    has_north, has_south = gy < n_gy - 1, gy > 0

    @pl.when(jnp.logical_not(has_north))
    def _():
        from_north[...] = jnp.zeros_like(from_north)

    @pl.when(jnp.logical_not(has_south))
    def _():
        from_south[...] = jnp.zeros_like(from_south)

    outside[...] = jnp.zeros_like(outside)

    def precondition(v, panels=1):
        return lax.dot_general(
            v,
            matrix[pl.ds(0, panels * levels), :],
            (((1,), (1,)), ((), ())),
            precision=lax.Precision.HIGHEST,
            preferred_element_type=jnp.float32,
        )

    def col_copy(t, side):
        buffer, recv, x = (
            (from_west, west_recv, east_x) if side == 0 else (from_east, east_recv, west_x)
        )
        return pltpu.make_async_remote_copy(
            src_ref=send_cols.at[t, pl.ds(side * rows, rows)],
            dst_ref=buffer.at[t],
            send_sem=col_send.at[t, side],
            recv_sem=recv.at[t],
            device_id=(x, gy),
            device_id_type=MESH,
        )

    def far_copy(t, g):
        return pltpu.make_async_remote_copy(
            src_ref=pack.at[pl.ds(0, 3)] if t == 0 else pack.at[3 + t],
            dst_ref=far_pack.at[:, own] if t == 0 else far_z.at[t - 1, own],
            send_sem=far_send.at[t],
            recv_sem=far_recv.at[t],
            device_id=(far_x, g),
            device_id_type=MESH,
        )

    def near_copy(t, g):
        return pltpu.make_async_remote_copy(
            src_ref=pack.at[pl.ds(0, 4)] if t == 0 else pack.at[3 + t],
            dst_ref=near_pack.at[:, own] if t == 0 else near_z.at[own],
            send_sem=near_send.at[t],
            recv_sem=near_recv.at[t],
            device_id=(gx, g),
            device_id_type=MESH,
        )

    def row_copy(t, side):
        buffer, recv, y, row = (
            (from_south, south_recv, gy + 1, cells - cols)
            if side == 0
            else (from_north, north_recv, gy - 1, 0)
        )
        return pltpu.make_async_remote_copy(
            src_ref=fields.at[t, pl.ds(row, cols)],
            dst_ref=buffer.at[t],
            send_sem=row_send.at[t, side],
            recv_sem=recv.at[t],
            device_id=(gx, y),
            device_id_type=MESH,
        )

    def send_cols_on(t, edges):
        send_cols[t] = precondition(edges)

        @pl.when(border)
        def _():
            edge = send_cols[t, pl.ds(side * rows, rows), :]
            if t == 0:
                items = [
                    edge,
                    horiz[edge_cols[0], :],
                    diag[edge_cols[0], :],
                    horiz[edge_cols[1], :],
                ]
                for k, item in enumerate(items):
                    pack[k] = item
                    near_pack[k, own, :] = item
            else:
                pack[3 + t] = edge
                if t == 1:
                    near_z[own, :] = edge

        @pl.when(border & (far_stage < t))
        def _():
            send_far(t)

        @pl.when(jnp.logical_not(east_border))
        def _():
            col_copy(t, 0).start()

        @pl.when(jnp.logical_not(west_border))
        def _():
            col_copy(t, 1).start()

        if t < 2:

            @pl.when(border)
            def _():
                for j in range(1, n_gy):
                    near_copy(t, lax.rem(gy + j, n_gy)).start()

    def send_far(t):
        for j in sorted(range(n_gy), key=lambda j: abs(2 * j - n_gy)):
            far_copy(t, lax.rem(gy + j, n_gy)).start()

    def send_rows(t):
        @pl.when(has_north)
        def _():
            row_copy(t, 0).start()

        @pl.when(has_south)
        def _():
            row_copy(t, 1).start()

    def receive_rows(t):
        @pl.when(has_north)
        def _():
            row_copy(t, 1).wait_recv()

        @pl.when(has_south)
        def _():
            row_copy(t, 0).wait_recv()

    def receive_cols(t):
        @pl.when(jnp.logical_not(east_border))
        def _():
            col_copy(t, 1).wait_recv()
            outside[pl.ds(0, rows), :] = from_east[t]

        @pl.when(jnp.logical_not(west_border))
        def _():
            col_copy(t, 0).wait_recv()
            outside[pl.ds(rows, rows), :] = from_west[t]

    col_id = lax.rem(lax.broadcasted_iota(jnp.int32, (cells, levels), 0), cols)
    east_edge = pl.ds(cols - 1, rows, stride=cols)
    west_edge = pl.ds(0, rows, stride=cols)
    south_edge = pl.ds(0, cols)
    north_edge = pl.ds(cells - cols, cols)

    def edge_columns(ref):
        return jnp.concatenate([ref[east_edge, :], ref[west_edge, :]], 0)

    def column_part(z):
        lane = lax.broadcasted_iota(jnp.int32, z.shape, 1)
        up = jnp.where(lane < levels - 1, pltpu.roll(z, levels - 1, 1), 0.0)
        down = jnp.where(lane > 0, pltpu.roll(z, 1, 1), 0.0)
        return vert[...] * (2.0 * z - (up + down))

    def inner_image(z):
        east = jnp.where(col_id < cols - 1, pltpu.roll(z, cells - 1, 0), 0.0)
        west = jnp.where(col_id > 0, pltpu.roll(z, 1, 0), 0.0)
        none = jnp.zeros((cols, levels), jnp.float32)
        north = jnp.concatenate([z[cols:], none], 0)
        south = jnp.concatenate([none, z[:-cols]], 0)
        beside = east + west + north + south
        return diag[...] * z + horiz[...] * (4.0 * z - beside) + column_part(z)

    def product(a, b):
        both = (a * b).reshape(-1, 8, levels)
        return jnp.sum(jnp.sum(both, axis=0), axis=0, keepdims=True)

    tall_id = lax.broadcasted_iota(jnp.int32, (tall, levels), 0)

    def along(w):
        north = jnp.where(tall_id < tall - 1, pltpu.roll(w, tall - 1, 0), 0.0)
        south = jnp.where(tall_id > 0, pltpu.roll(w, 1, 0), 0.0)
        return north + south

    def stencil(w, d, h):
        return d * w + h * (4.0 * w - along(w)) + column_part(w)

    def gather_rows(start, count, pairs):
        def one(y):
            row = edge_rows[table, start + y]
            for dst, src in pairs:
                gathered[dst, pl.ds(y, 1), :] = src[pl.ds(row, 1), :]

        if count <= 64:
            for y in range(count):
                one(y)
        else:

            def body(y, carry):
                one(y)
                return carry

            lax.fori_loop(0, count, body, 0)

    def wait_bytes(ref, sem):
        pltpu.make_async_copy(ref, ref, sem).wait()

    near_rest = pl.ds(0, (n_gy - 1) * rows)

    def correct_first():
        wait_bytes(far_pack, far_recv.at[0])
        wait_bytes(near_pack.at[:, near_rest], near_recv.at[0])
        gather_rows(0, tall, [(0, far_pack.at[0]), (1, near_pack.at[0])])
        b_near = -(near_pack[1] * gathered[0])
        b_far = -(far_pack[1] * gathered[1])
        strip[0] = b_near
        both = precondition(jnp.concatenate([b_near, b_far], 0), 2)
        strip[1] = both[:tall, :levels]
        strip[2] = both[tall:, levels:]

    def correct_second():
        wait_bytes(far_z.at[0], far_recv.at[1])
        wait_bytes(near_z.at[near_rest], near_recv.at[1])
        w_near, w_far = strip[1], strip[2]
        strip[3] = far_z[0] + w_far
        strip[4] = near_z[...] + w_near
        gather_rows(0, tall, [(0, strip.at[3]), (1, strip.at[4])])
        h_near, h_far = near_pack[1], far_pack[1]
        b_near = stencil(w_near, near_pack[2], h_near) - h_near * gathered[0]
        b_far = stencil(w_far, far_pack[2], h_far) - h_far * gathered[1]
        b_next = -(near_pack[3] * w_near)
        all_three = precondition(jnp.concatenate([b_near, b_next, b_far], 0), 2)
        w_edge, w_next = all_three[:tall, :levels], all_three[tall : 2 * tall, :levels]
        strip[3] = b_near
        strip[4] = b_next
        strip[5] = all_three[2 * tall :, levels:]
        strip[6] = w_edge
        strip[7] = w_next
        strip[8] = along(w_next)
        strip[9] = stencil(w_edge, near_pack[2], h_near) - h_near * w_next

    def correct_third():
        c0, c1, c2 = edge_cols
        w_edge, w_next, beside = strip[6, own, :], strip[7, own, :], strip[8, own, :]
        h1 = horiz[c1, :]
        later = diag[c1, :] * w_next + h1 * (4.0 * w_next - beside - w_edge) + column_part(w_next)
        b_third = -(horiz[c2, :] * w_next)
        gather_rows(first_row, rows, [(2, strip.at[5])])
        wait_bytes(far_z.at[1], far_recv.at[2])
        gather_rows(first_row, rows, [(3, far_z.at[1])])
        across = gathered[2, pl.ds(0, rows), :] + gathered[3, pl.ds(0, rows), :]
        b_edge = strip[9, own, :] - horiz[c0, :] * across
        none = jnp.zeros((rows, levels), jnp.float32)
        changes = [
            [strip[0, own, :], none, none],
            [strip[3, own, :], strip[4, own, :], none],
            [b_edge, later, b_third],
        ]
        before = [jnp.concatenate([r0[c, :] for c in edge_cols], 0)]
        after = [before[0]]
        for t in range(ITERS):
            old = jnp.concatenate([images[t, c, :] for c in edge_cols], 0)
            new = old + jnp.concatenate(changes[t], 0)
            before.append(old)
            after.append(new)
            for k in range(t + 1):
                images[t, edge_cols[k], :] = new[k * rows : (k + 1) * rows]
        for k, (i, j) in enumerate(KEYS):
            if j > 0:
                partial[pl.ds(k, 1), :] += product(after[i], after[j]) - product(before[i], before[j])

    for load in loads:
        load.wait()
    terms = {}
    spaces = [r0]
    send_cols_on(0, edge_columns(r0))
    edge_horiz = edge_columns(horiz)
    for t in range(ITERS):
        image = images.at[t]
        z = precondition(spaces[-1][...])
        fields[t] = z
        send_rows(t)
        newest = len(spaces) - 1
        for i in range(len(spaces)):
            terms[(i, newest)] = product(spaces[i][...], spaces[newest][...])
        image[...] = inner_image(z)
        learn_above(t)
        receive_rows(t)
        image[south_edge, :] = image[south_edge, :] - horiz[south_edge, :] * from_south[t]
        image[north_edge, :] = image[north_edge, :] - horiz[north_edge, :] * from_north[t]
        inside = edge_columns(image)
        receive_cols(t)
        edges = inside - edge_horiz * outside[...]
        if t < ITERS - 1:
            send_cols_on(t + 1, edges)
        image[east_edge, :] = edges[:rows]
        image[west_edge, :] = edges[rows:]
        spaces.append(image)
    newest = len(spaces) - 1
    for i in range(len(spaces)):
        terms[(i, newest)] = product(spaces[i][...], spaces[newest][...])
    for k, key in enumerate(KEYS):
        partial[pl.ds(k, 1), :] = terms[key]

    @pl.when(border)
    def _():
        correct_first()
        correct_second()
        correct_third()

    height = -(-len(KEYS) // 8) * 8
    row_id = lax.broadcasted_iota(jnp.int32, (height, levels), 0)
    lane = lax.broadcasted_iota(jnp.int32, (height, levels), 1)
    stacked = jnp.where(row_id < len(KEYS), partial[...], 0.0)
    summed = jnp.sum(stacked, axis=1, keepdims=True)
    sums[me] = jnp.sum(jnp.where(lane == row_id, summed, 0.0), axis=0, keepdims=True)

    def tell(x, y):
        pltpu.make_async_remote_copy(
            src_ref=sums.at[me],
            dst_ref=sums.at[me],
            send_sem=sum_send,
            recv_sem=sum_recv,
            device_id=(x, y),
            device_id_type=MESH,
        ).start()

    for_others(tell)
    for t in range(ITERS):

        @pl.when(jnp.logical_not(east_border))
        def _(t=t):
            col_copy(t, 0).wait_send()

        @pl.when(jnp.logical_not(west_border))
        def _(t=t):
            col_copy(t, 1).wait_send()

        @pl.when(has_north)
        def _(t=t):
            row_copy(t, 0).wait_send()

        @pl.when(has_south)
        def _(t=t):
            row_copy(t, 1).wait_send()

    @pl.when(border)
    def _():
        wait_bytes(far_pack, far_send.at[0])
        wait_bytes(far_z.at[0], far_send.at[1])
        wait_bytes(far_z.at[1], far_send.at[2])
        wait_bytes(near_pack.at[:, near_rest], near_send.at[0])
        wait_bytes(near_z.at[near_rest], near_send.at[1])
        c0, c1, c2 = edge_cols
        fields[1, c0, :] += strip[1, own, :]
        fields[2, c0, :] += strip[6, own, :]
        fields[2, c1, :] += strip[7, own, :]

    others = sums.at[pl.ds(0, n_all - 1)]
    wait_bytes(others, sum_recv)
    out_totals[...] = jnp.sum(sums[...], axis=0)
    wait_bytes(others, sum_send)


def finish(total_cells, all_totals, r0, fields, images, out_x, out_r, out_norms, x, r, sem):
    levels = r0.shape[-1]
    totals = all_totals[...]
    value = {key: totals[:, k : k + 1] for k, key in enumerate(KEYS)}

    rho, g0, g1, g2 = value[(0, 0)], value[(0, 1)], value[(0, 2)], value[(0, 3)]
    a00, a01, a02 = value[(1, 1)], value[(1, 2)], value[(1, 3)]
    a11, a12, a22 = value[(2, 2)], value[(2, 3)], value[(3, 3)]
    l10, l20, y0 = a01 / a00, a02 / a00, g0 / a00
    d1, e12, f1 = a11 - l10 * a01, a12 - l10 * a02, g1 - l10 * g0
    l21, y1 = e12 / d1, f1 / d1
    d2, f2 = a22 - l20 * a02 - l21 * e12, g2 - l20 * g0 - l21 * f1
    y2 = f2 / d2
    norm0 = rho - y0 * g0
    norm1 = norm0 - y1 * f1
    norm2 = norm1 - y2 * f2
    y1 = y1 - l21 * y2
    y0 = y0 - l10 * y1 - l20 * y2
    norm_lane = lax.broadcasted_iota(jnp.int32, (1, levels), 1)
    norms = jnp.where(norm_lane == 0, norm0, jnp.where(norm_lane == 1, norm1, norm2))
    out_norms[...] = norms[:, :ITERS] / total_cells
    rows = r0.shape[0]
    pieces = 2 if rows % 16 == 0 else 1
    size = rows // pieces
    copies = []
    for p in range(pieces):
        span = pl.ds(p * size, size)
        x[span] = y0 * fields[0, span] + y1 * fields[1, span] + y2 * fields[2, span]
        r[span] = (
            r0[span] - y0 * images[0, span] - y1 * images[1, span] - y2 * images[2, span]
        )
        for k, (src, dst) in enumerate(((x, out_x), (r, out_r))):
            copy = pltpu.make_async_copy(src.at[span], dst.at[span], sem.at[p, k])
            copy.start()
            copies.append(copy)
    for copy in copies:
        copy.wait()


def on_device(n_gx, n_gy, right_side, diagonal, horizontal, vertical, precond, edge_rows):
    rows, cols, levels = right_side.shape
    f32 = jnp.float32
    block = (rows * cols, levels)
    column = (n_gy * rows, levels)
    sems = pltpu.SemaphoreType.DMA
    basis = pltpu.VMEM((ITERS,) + block, f32)
    fields, images, totals, start = pl.pallas_call(
        functools.partial(kernel, n_gx, n_gy, rows),
        out_shape=(basis, basis, pltpu.VMEM((1, levels), f32), pltpu.VMEM(block, f32)),
        in_specs=[ANY, ANY, ANY, ANY, ANY, ANY],
        out_specs=(VMEM, VMEM, VMEM, VMEM),
        scratch_shapes=[
            pltpu.VMEM(block, f32),
            pltpu.VMEM(block, f32),
            pltpu.VMEM((1, levels), f32),
            pltpu.VMEM((2 * levels, levels), f32),
            pltpu.VMEM((ITERS, 2 * rows, levels), f32),
            pltpu.VMEM((6, rows, levels), f32),
            pltpu.VMEM((ITERS, rows, levels), f32),
            pltpu.VMEM((ITERS, rows, levels), f32),
            pltpu.VMEM((ITERS, cols, levels), f32),
            pltpu.VMEM((ITERS, cols, levels), f32),
            pltpu.VMEM((3,) + column, f32),
            pltpu.VMEM((4,) + column, f32),
            pltpu.VMEM((2,) + column, f32),
            pltpu.VMEM(column, f32),
            pltpu.VMEM((4,) + column, f32),
            pltpu.VMEM((10,) + column, f32),
            pltpu.VMEM((2 * rows, levels), f32),
            pltpu.VMEM((16, levels), f32),
            pltpu.VMEM((n_gx * n_gy, 1, levels), f32),
            pltpu.SMEM(edge_rows.shape, jnp.int32),
            sems((7,)),
            sems((ITERS, 2)),
            sems((ITERS,)),
            sems((ITERS,)),
            sems((ITERS,)),
            sems((ITERS,)),
            sems((2,)),
            sems((2,)),
            sems((ITERS, 2)),
            sems((ITERS,)),
            sems((ITERS,)),
            sems(()),
            sems(()),
            pltpu.SemaphoreType.REGULAR,
            pltpu.SemaphoreType.REGULAR,
        ],
        compiler_params=pltpu.CompilerParams(collective_id=0, has_side_effects=True),
    )(
        edge_rows,
        right_side.reshape(block),
        diagonal.reshape(block),
        horizontal.reshape(block),
        vertical.reshape(1, levels),
        precond,
    )
    in_vmem = functools.partial(
        pltpu.with_memory_space_constraint, memory_space=pltpu.VMEM
    )
    total_cells = float(rows * cols * levels * n_gx * n_gy)
    x, r, norms = pl.pallas_call(
        functools.partial(finish, total_cells),
        out_shape=(
            jax.ShapeDtypeStruct(block, f32),
            jax.ShapeDtypeStruct(block, f32),
            jax.ShapeDtypeStruct((1, ITERS), f32),
        ),
        in_specs=[VMEM, VMEM, VMEM, VMEM],
        out_specs=(ANY, ANY, VMEM),
        scratch_shapes=[pltpu.VMEM(block, f32), pltpu.VMEM(block, f32), sems((2, 2))],
    )(in_vmem(totals), in_vmem(start), in_vmem(fields), in_vmem(images))
    shape = right_side.shape
    return x.reshape(shape), r.reshape(shape), norms.reshape(ITERS)


def solution(mesh):
    n_gx, n_gy = mesh.shape["gx"], mesh.shape["gy"]
    field = P("gy", "gx", None)
    return jax.shard_map(
        functools.partial(on_device, n_gx, n_gy),
        mesh=mesh,
        in_specs=(field, field, field, P(), P(), P()),
        out_specs=(field, field, P()),
        check_vma=False,
    )
```

```python
import functools

import jax
import jax.numpy as jnp
from jax import lax
from jax.experimental import pallas as pl
from jax.experimental.pallas import tpu as pltpu
from jax.sharding import PartitionSpec as P

ITERS = 3
KEYS = [(i, j) for j in range(ITERS + 1) for i in range(j + 1)]
MESH = pl.DeviceIdType.MESH
ANY = pl.BlockSpec(memory_space=pl.ANY)
VMEM = pl.BlockSpec(memory_space=pltpu.VMEM)


def kernel(
    n_gx,
    n_gy,
    out_rows,
    edge_table,
    right_side,
    diagonal,
    horizontal,
    vertical,
    precond,
    fields,
    images,
    out_totals,
    r0,
    diag,
    horiz,
    vert,
    matrix,
    frame_z,
    pack,
    mini_out,
    mini_in,
    wide,
    from_east,
    from_west,
    from_north,
    from_south,
    far_pack,
    near_pack,
    far_last,
    gathered,
    strip,
    outside,
    partial,
    sums,
    edge_rows,
    load_sem,
    col_send,
    east_recv,
    west_recv,
    far_send,
    far_recv,
    near_send,
    near_recv,
    mini_send,
    mini_recv,
    row_send,
    north_recv,
    south_recv,
    sum_send,
    sum_recv,
):
    rows, levels = out_rows, r0.shape[-1]
    cells = r0.shape[0]
    cols = cells // rows
    tall = n_gy * rows
    gx, gy = lax.axis_index("gx"), lax.axis_index("gy")
    n_all = n_gx * n_gy
    half = n_gx // 2
    me = gx * n_gy + gy

    def for_others(visit):
        def step(i, carry):
            for j in range(n_gy):
                visit(lax.rem(gx + i, n_gx), lax.rem(gy + j, n_gy))
            return carry

        if n_all <= 64:
            for i in sorted(range(1, n_gx), key=lambda i: min(i, n_gx - i)):
                step(i, 0)
        else:
            lax.fori_loop(1, n_gx, step, 0)
        for j in range(1, n_gy):
            visit(gx, lax.rem(gy + j, n_gy))

    barrier = pltpu.get_barrier_semaphore()

    def greet(x, y):
        pl.semaphore_signal(barrier, inc=1, device_id=(x, y), device_id_type=MESH)

    for_others(greet)

    panel = lax.convert_element_type(gx >= half, jnp.int32)
    loads = [
        pltpu.make_async_copy(right_side, r0, load_sem.at[0]),
        pltpu.make_async_copy(precond.at[panel], matrix.at[pl.ds(0, levels)], load_sem.at[1]),
        pltpu.make_async_copy(horizontal, horiz, load_sem.at[2]),
        pltpu.make_async_copy(diagonal, diag, load_sem.at[3]),
        pltpu.make_async_copy(vertical, vert, load_sem.at[4]),
        pltpu.make_async_copy(edge_table, edge_rows, load_sem.at[5]),
        pltpu.make_async_copy(precond.at[1 - panel], matrix.at[pl.ds(levels, levels)], load_sem.at[6]),
    ]
    for load in loads:
        load.start()

    east_x, west_x = lax.rem(gx + 1, n_gx), lax.rem(gx + n_gx - 1, n_gx)
    east_border = (gx == half - 1) | (gx == n_gx - 1)
    west_border = (gx == half) | (gx == 0)
    border = east_border | west_border
    far_x = jnp.where(east_border, east_x, west_x)
    side = jnp.where(east_border, 0, 1)
    table = jnp.where((gx == half - 1) | (gx == half), 0, 1)
    edge_cols = [
        pl.ds(jnp.where(east_border, cols - 1 - i, i), rows, stride=cols) for i in range(3)
    ]
    first_row = pl.multiple_of(gy * rows, rows)
    own = pl.ds(first_row, rows)
    has_north, has_south = gy < n_gy - 1, gy > 0

    @pl.when(jnp.logical_not(has_north))
    def _():
        from_north[...] = jnp.zeros_like(from_north)

    @pl.when(jnp.logical_not(has_south))
    def _():
        from_south[...] = jnp.zeros_like(from_south)

    outside[...] = jnp.zeros_like(outside)

    def precondition(v, panels=1):
        return lax.dot_general(
            v,
            matrix[pl.ds(0, panels * levels), :],
            (((1,), (1,)), ((), ())),
            precision=lax.Precision.HIGHEST,
            preferred_element_type=jnp.float32,
        )

    def col_copy(t, side):
        buffer, recv, x = (
            (from_west, west_recv, east_x) if side == 0 else (from_east, east_recv, west_x)
        )
        return pltpu.make_async_remote_copy(
            src_ref=frame_z.at[t, pl.ds(side * rows, rows)],
            dst_ref=buffer.at[t],
            send_sem=col_send.at[t, side],
            recv_sem=recv.at[t],
            device_id=(x, gy),
            device_id_type=MESH,
        )

    def far_copy(t, g):
        return pltpu.make_async_remote_copy(
            src_ref=pack.at[pl.ds(0, 4)] if t == 0 else pack.at[5],
            dst_ref=far_pack.at[:, own] if t == 0 else far_last.at[own],
            send_sem=far_send.at[t],
            recv_sem=far_recv.at[t],
            device_id=(far_x, g),
            device_id_type=MESH,
        )

    def near_copy(g):
        return pltpu.make_async_remote_copy(
            src_ref=pack.at[pl.ds(0, 5)],
            dst_ref=near_pack.at[:, own],
            send_sem=near_send,
            recv_sem=near_recv,
            device_id=(gx, g),
            device_id_type=MESH,
        )

    def mini_copy(side):
        return pltpu.make_async_remote_copy(
            src_ref=mini_out.at[side],
            dst_ref=mini_in.at[side],
            send_sem=mini_send.at[side],
            recv_sem=mini_recv.at[side],
            device_id=(gx, gy + 1 if side == 0 else gy - 1),
            device_id_type=MESH,
        )

    def row_copy(t, side):
        buffer, recv, y, row = (
            (from_south, south_recv, gy + 1, 2 * rows + cols)
            if side == 0
            else (from_north, north_recv, gy - 1, 2 * rows)
        )
        return pltpu.make_async_remote_copy(
            src_ref=frame_z.at[t, pl.ds(row, cols)],
            dst_ref=buffer.at[t],
            send_sem=row_send.at[t, side],
            recv_sem=recv.at[t],
            device_id=(gx, y),
            device_id_type=MESH,
        )

    def for_rows(visit):
        @pl.when(has_north)
        def _():
            visit(0)

        @pl.when(has_south)
        def _():
            visit(1)

    def fill_packs():
        c0, c1, c2 = edge_cols
        inward = 2 * (rows + cols)
        items = [
            frame_z[0, pl.ds(side * rows, rows), :],
            frame_z[0, pl.ds(inward, rows), :],
            horiz[c0, :],
            diag[c0, :],
            horiz[c1, :],
        ]
        for k, item in enumerate(items):
            pack[k] = item
            near_pack[k, own, :] = item
            if k < 4:
                wide[k] = jnp.zeros_like(wide[k])
                wide[k, pl.ds(8, rows), :] = item
        for to, first, second in ((0, rows - 1, rows - 2), (1, 0, 1)):
            picks = [(0, first), (0, second), (1, first), (2, first), (3, first)]
            for k, (item, row) in enumerate(picks):
                mini_out[to, pl.ds(k, 1), :] = items[item][row : row + 1]
            mini_out[to, pl.ds(5, 3), :] = jnp.zeros((3, levels), jnp.float32)

    def send_frame(t, frame):
        z = precondition(frame)
        frame_z[t, pl.ds(0, z.shape[0]), :] = z
        if t == 0:
            pl.when(border)(fill_packs)
            pl.semaphore_wait(barrier, n_all - 1)

            @pl.when(border)
            def _():
                for_rows(lambda side: mini_copy(side).start())

        @pl.when(jnp.logical_not(east_border))
        def _():
            col_copy(t, 0).start()

        @pl.when(jnp.logical_not(west_border))
        def _():
            col_copy(t, 1).start()

        for_rows(lambda side: row_copy(t, side).start())
        if t == 0:

            @pl.when(border)
            def _():
                send_far(0)
                for j in range(1, n_gy):
                    near_copy(lax.rem(gy + j, n_gy)).start()

    def send_far(t):
        for j in sorted(range(n_gy), key=lambda j: abs(2 * j - n_gy)):
            far_copy(t, lax.rem(gy + j, n_gy)).start()

    def receive_rows(t):
        @pl.when(has_north)
        def _():
            row_copy(t, 1).wait_recv()

        @pl.when(has_south)
        def _():
            row_copy(t, 0).wait_recv()

    def receive_cols(t):
        @pl.when(jnp.logical_not(east_border))
        def _():
            col_copy(t, 1).wait_recv()
            outside[pl.ds(0, rows), :] = from_east[t]

        @pl.when(jnp.logical_not(west_border))
        def _():
            col_copy(t, 0).wait_recv()
            outside[pl.ds(rows, rows), :] = from_west[t]

    col_id = lax.rem(lax.broadcasted_iota(jnp.int32, (cells, levels), 0), cols)
    east_edge = pl.ds(cols - 1, rows, stride=cols)
    west_edge = pl.ds(0, rows, stride=cols)
    south_edge = pl.ds(0, cols)
    north_edge = pl.ds(cells - cols, cols)

    def edge_columns(ref):
        return jnp.concatenate([ref[east_edge, :], ref[west_edge, :]], 0)

    def column_part(z):
        lane = lax.broadcasted_iota(jnp.int32, z.shape, 1)
        up = jnp.where(lane < levels - 1, pltpu.roll(z, levels - 1, 1), 0.0)
        down = jnp.where(lane > 0, pltpu.roll(z, 1, 1), 0.0)
        return vert[...] * (2.0 * z - (up + down))

    def inner_image(z):
        east = jnp.where(col_id < cols - 1, pltpu.roll(z, cells - 1, 0), 0.0)
        west = jnp.where(col_id > 0, pltpu.roll(z, 1, 0), 0.0)
        none = jnp.zeros((cols, levels), jnp.float32)
        north = jnp.concatenate([z[cols:], none], 0)
        south = jnp.concatenate([none, z[:-cols]], 0)
        beside = east + west + north + south
        return diag[...] * z + horiz[...] * (4.0 * z - beside) + column_part(z)

    def product(a, b):
        both = (a * b).reshape(-1, 8, levels)
        return jnp.sum(jnp.sum(both, axis=0), axis=0, keepdims=True)

    tall_id = lax.broadcasted_iota(jnp.int32, (tall, levels), 0)

    def along(w):
        north = jnp.where(tall_id < tall - 1, pltpu.roll(w, tall - 1, 0), 0.0)
        south = jnp.where(tall_id > 0, pltpu.roll(w, 1, 0), 0.0)
        return north + south

    def stencil(w, d, h):
        return d * w + h * (4.0 * w - along(w)) + column_part(w)

    def gather_rows(start, count, pairs):
        def one(y):
            row = edge_rows[table, start + y]
            for dst, src in pairs:
                gathered[dst, pl.ds(y, 1), :] = src[pl.ds(row, 1), :]

        if count <= 64:
            for y in range(count):
                one(y)
        else:

            def body(y, carry):
                one(y)
                return carry

            lax.fori_loop(0, count, body, 0)

    def wait_bytes(ref, sem):
        pltpu.make_async_copy(ref, ref, sem).wait()

    near_rest = pl.ds(0, (n_gy - 1) * rows)

    def look_ahead():
        c1 = edge_cols[1]
        inner = pl.ds(8, rows)

        def take(side, near, far):
            mini_copy(side).wait_recv()
            wide[0, pl.ds(near, 1), :] = mini_in[side, pl.ds(0, 1), :]
            wide[0, pl.ds(far, 1), :] = mini_in[side, pl.ds(1, 1), :]
            for k in (1, 2, 3):
                wide[k, pl.ds(near, 1), :] = mini_in[side, pl.ds(k + 1, 1), :]

        pl.when(border & has_south)(functools.partial(take, 0, 7, 6))
        pl.when(border & has_north)(functools.partial(take, 1, 8 + rows, 9 + rows))

        def next_to(w):
            return pltpu.roll(w, w.shape[0] - 1, 0) + pltpu.roll(w, 1, 0)

        z_edge, z_next, h_edge, d_edge = wide[0], wide[1], wide[2], wide[3]
        v_edge = (
            d_edge * z_edge
            + h_edge * (4.0 * z_edge - z_next - next_to(z_edge))
            + column_part(z_edge)
        )
        beside = next_to(z_next)[8 : 8 + rows] + z_edge[8 : 8 + rows]
        z1 = z_next[8 : 8 + rows]
        z2 = frame_z[0, pl.ds(2 * (rows + cols) + rows, rows), :]
        v_next = (
            diag[c1, :] * z1 + horiz[c1, :] * (4.0 * z1 - beside - z2) + column_part(z1)
        )
        z = precondition(jnp.concatenate([v_edge, v_next], 0))
        z_edge, z_next = z[: rows + 16], z[rows + 16 :]
        beside = next_to(z_edge)[8 : 8 + rows] + z_next
        z_edge = z_edge[8 : 8 + rows]
        h_own, d_own = h_edge[8 : 8 + rows], d_edge[8 : 8 + rows]
        v = d_own * z_edge + h_own * (4.0 * z_edge - beside) + column_part(z_edge)
        pack[5] = precondition(v)
        pl.when(border)(functools.partial(send_far, 1))

    def correct_early():
        @pl.when(border)
        def _():
            wait_bytes(far_pack, far_recv.at[0])
            wait_bytes(near_pack.at[:, near_rest], near_recv)

        gather_rows(0, tall, [(0, far_pack.at[0]), (1, near_pack.at[0])])
        h_near, d_near = near_pack[2], near_pack[3]
        h_far, d_far = far_pack[2], far_pack[3]
        b_near, b_far = -(h_near * gathered[0]), -(h_far * gathered[1])
        v_near = stencil(near_pack[0], d_near, h_near) - h_near * near_pack[1] + b_near
        v_far = stencil(far_pack[0], d_far, h_far) - h_far * far_pack[1] + b_far
        out = precondition(jnp.concatenate([b_near, v_near, b_far, v_far], 0), 2)
        w_near, w_far = out[:tall, :levels], out[2 * tall : 3 * tall, levels:]
        strip[0] = b_near
        strip[1] = w_near
        strip[3] = out[3 * tall :, levels:]
        strip[4] = out[tall : 2 * tall, :levels]
        gather_rows(0, tall, [(0, strip.at[3]), (1, strip.at[4])])
        b_near = stencil(w_near, d_near, h_near) - h_near * gathered[0]
        b_far = stencil(w_far, d_far, h_far) - h_far * gathered[1]
        b_next = -(near_pack[4] * w_near)
        out = precondition(jnp.concatenate([b_near, b_next, b_far], 0), 2)
        w_edge, w_next = out[:tall, :levels], out[tall : 2 * tall, :levels]
        strip[3] = b_near
        strip[4] = b_next
        strip[5] = out[2 * tall :, levels:]
        strip[6] = w_edge
        strip[7] = w_next
        strip[8] = along(w_next)
        strip[9] = stencil(w_edge, d_near, h_near) - h_near * w_next

    def correct_third():
        c0, c1, c2 = edge_cols
        w_edge, w_next, beside = strip[6, own, :], strip[7, own, :], strip[8, own, :]
        h1 = horiz[c1, :]
        later = diag[c1, :] * w_next + h1 * (4.0 * w_next - beside - w_edge) + column_part(w_next)
        b_third = -(horiz[c2, :] * w_next)
        gather_rows(first_row, rows, [(2, strip.at[5])])
        wait_bytes(far_last, far_recv.at[1])
        gather_rows(first_row, rows, [(3, far_last)])
        across = gathered[2, pl.ds(0, rows), :] + gathered[3, pl.ds(0, rows), :]
        b_edge = strip[9, own, :] - horiz[c0, :] * across
        none = jnp.zeros((rows, levels), jnp.float32)
        changes = [
            [strip[0, own, :], none, none],
            [strip[3, own, :], strip[4, own, :], none],
            [b_edge, later, b_third],
        ]
        before = [jnp.concatenate([r0[c, :] for c in edge_cols], 0)]
        after = [before[0]]
        for t in range(ITERS):
            old = jnp.concatenate([images[t, c, :] for c in edge_cols], 0)
            new = old + jnp.concatenate(changes[t], 0)
            before.append(old)
            after.append(new)
            for k in range(t + 1):
                images[t, edge_cols[k], :] = new[k * rows : (k + 1) * rows]
        for k, (i, j) in enumerate(KEYS):
            if j > 0:
                partial[pl.ds(k, 1), :] += product(after[i], after[j]) - product(before[i], before[j])

    for load in loads:
        load.wait()
    terms = {}
    spaces = [r0]
    frame = [edge_columns(r0), r0[south_edge, :], r0[north_edge, :]]
    send_frame(0, jnp.concatenate(frame + [r0[c, :] for c in edge_cols[1:]], 0))
    edge_horiz = edge_columns(horiz)
    for t in range(ITERS):
        image = images.at[t]
        z = precondition(spaces[-1][...])
        fields[t] = z
        newest = len(spaces) - 1
        for i in range(len(spaces)):
            terms[(i, newest)] = product(spaces[i][...], spaces[newest][...])
        image[...] = inner_image(z)
        if t == 0:
            look_ahead()
        if t == ITERS - 1:
            correct_early()
        receive_rows(t)
        image[south_edge, :] = image[south_edge, :] - horiz[south_edge, :] * from_south[t]
        image[north_edge, :] = image[north_edge, :] - horiz[north_edge, :] * from_north[t]
        inside = edge_columns(image)
        receive_cols(t)
        edges = inside - edge_horiz * outside[...]
        image[east_edge, :] = edges[:rows]
        image[west_edge, :] = edges[rows:]
        if t < ITERS - 1:
            frame = [edges, image[south_edge, :], image[north_edge, :]]
            send_frame(t + 1, jnp.concatenate(frame, 0))
        spaces.append(image)
    newest = len(spaces) - 1
    for i in range(len(spaces)):
        terms[(i, newest)] = product(spaces[i][...], spaces[newest][...])
    for k, key in enumerate(KEYS):
        partial[pl.ds(k, 1), :] = terms[key]

    @pl.when(border)
    def _():
        correct_third()

    height = -(-len(KEYS) // 8) * 8
    row_id = lax.broadcasted_iota(jnp.int32, (height, levels), 0)
    lane = lax.broadcasted_iota(jnp.int32, (height, levels), 1)
    stacked = jnp.where(row_id < len(KEYS), partial[...], 0.0)
    summed = jnp.sum(stacked, axis=1, keepdims=True)
    sums[me] = jnp.sum(jnp.where(lane == row_id, summed, 0.0), axis=0, keepdims=True)

    def tell(x, y):
        pltpu.make_async_remote_copy(
            src_ref=sums.at[me],
            dst_ref=sums.at[me],
            send_sem=sum_send,
            recv_sem=sum_recv,
            device_id=(x, y),
            device_id_type=MESH,
        ).start()

    for_others(tell)
    for t in range(ITERS):

        @pl.when(jnp.logical_not(east_border))
        def _(t=t):
            col_copy(t, 0).wait_send()

        @pl.when(jnp.logical_not(west_border))
        def _(t=t):
            col_copy(t, 1).wait_send()

        @pl.when(has_north)
        def _(t=t):
            row_copy(t, 0).wait_send()

        @pl.when(has_south)
        def _(t=t):
            row_copy(t, 1).wait_send()

    @pl.when(border)
    def _():
        wait_bytes(far_pack, far_send.at[0])
        wait_bytes(far_last, far_send.at[1])
        wait_bytes(near_pack.at[:, near_rest], near_send)
        for_rows(lambda side: mini_copy(side).wait_send())
        c0, c1, c2 = edge_cols
        fields[1, c0, :] += strip[1, own, :]
        fields[2, c0, :] += strip[6, own, :]
        fields[2, c1, :] += strip[7, own, :]

    others = sums.at[pl.ds(0, n_all - 1)]
    wait_bytes(others, sum_recv)
    out_totals[...] = jnp.sum(sums[...], axis=0)
    wait_bytes(others, sum_send)


def finish(total_cells, all_totals, r0, fields, images, out_x, out_r, out_norms, x, r, sem):
    levels = r0.shape[-1]
    totals = all_totals[...]
    value = {key: totals[:, k : k + 1] for k, key in enumerate(KEYS)}

    rho, g0, g1, g2 = value[(0, 0)], value[(0, 1)], value[(0, 2)], value[(0, 3)]
    a00, a01, a02 = value[(1, 1)], value[(1, 2)], value[(1, 3)]
    a11, a12, a22 = value[(2, 2)], value[(2, 3)], value[(3, 3)]
    l10, l20, y0 = a01 / a00, a02 / a00, g0 / a00
    d1, e12, f1 = a11 - l10 * a01, a12 - l10 * a02, g1 - l10 * g0
    l21, y1 = e12 / d1, f1 / d1
    d2, f2 = a22 - l20 * a02 - l21 * e12, g2 - l20 * g0 - l21 * f1
    y2 = f2 / d2
    norm0 = rho - y0 * g0
    norm1 = norm0 - y1 * f1
    norm2 = norm1 - y2 * f2
    y1 = y1 - l21 * y2
    y0 = y0 - l10 * y1 - l20 * y2
    norm_lane = lax.broadcasted_iota(jnp.int32, (1, levels), 1)
    norms = jnp.where(norm_lane == 0, norm0, jnp.where(norm_lane == 1, norm1, norm2))
    out_norms[...] = norms[:, :ITERS] / total_cells
    rows = r0.shape[0]
    pieces = 2 if rows % 16 == 0 else 1
    size = rows // pieces
    copies = []
    for p in range(pieces):
        span = pl.ds(p * size, size)
        x[span] = y0 * fields[0, span] + y1 * fields[1, span] + y2 * fields[2, span]
        r[span] = (
            r0[span] - y0 * images[0, span] - y1 * images[1, span] - y2 * images[2, span]
        )
        for k, (src, dst) in enumerate(((x, out_x), (r, out_r))):
            copy = pltpu.make_async_copy(src.at[span], dst.at[span], sem.at[p, k])
            copy.start()
            copies.append(copy)
    for copy in copies:
        copy.wait()


def on_device(n_gx, n_gy, right_side, diagonal, horizontal, vertical, precond, edge_rows):
    rows, cols, levels = right_side.shape
    f32 = jnp.float32
    block = (rows * cols, levels)
    column = (n_gy * rows, levels)
    sems = pltpu.SemaphoreType.DMA
    basis = pltpu.VMEM((ITERS,) + block, f32)
    fields, images, totals, start = pl.pallas_call(
        functools.partial(kernel, n_gx, n_gy, rows),
        out_shape=(basis, basis, pltpu.VMEM((1, levels), f32), pltpu.VMEM(block, f32)),
        in_specs=[ANY, ANY, ANY, ANY, ANY, ANY],
        out_specs=(VMEM, VMEM, VMEM, VMEM),
        scratch_shapes=[
            pltpu.VMEM(block, f32),
            pltpu.VMEM(block, f32),
            pltpu.VMEM((1, levels), f32),
            pltpu.VMEM((2 * levels, levels), f32),
            pltpu.VMEM((ITERS, 4 * rows + 2 * cols, levels), f32),
            pltpu.VMEM((6, rows, levels), f32),
            pltpu.VMEM((2, 8, levels), f32),
            pltpu.VMEM((2, 8, levels), f32),
            pltpu.VMEM((4, rows + 16, levels), f32),
            pltpu.VMEM((ITERS, rows, levels), f32),
            pltpu.VMEM((ITERS, rows, levels), f32),
            pltpu.VMEM((ITERS, cols, levels), f32),
            pltpu.VMEM((ITERS, cols, levels), f32),
            pltpu.VMEM((4,) + column, f32),
            pltpu.VMEM((5,) + column, f32),
            pltpu.VMEM(column, f32),
            pltpu.VMEM((4,) + column, f32),
            pltpu.VMEM((10,) + column, f32),
            pltpu.VMEM((2 * rows, levels), f32),
            pltpu.VMEM((16, levels), f32),
            pltpu.VMEM((n_gx * n_gy, 1, levels), f32),
            pltpu.SMEM(edge_rows.shape, jnp.int32),
            sems((7,)),
            sems((ITERS, 2)),
            sems((ITERS,)),
            sems((ITERS,)),
            sems((2,)),
            sems((2,)),
            sems(()),
            sems(()),
            sems((2,)),
            sems((2,)),
            sems((ITERS, 2)),
            sems((ITERS,)),
            sems((ITERS,)),
            sems(()),
            sems(()),
        ],
        compiler_params=pltpu.CompilerParams(collective_id=0, has_side_effects=True),
    )(
        edge_rows,
        right_side.reshape(block),
        diagonal.reshape(block),
        horizontal.reshape(block),
        vertical.reshape(1, levels),
        precond,
    )
    in_vmem = functools.partial(
        pltpu.with_memory_space_constraint, memory_space=pltpu.VMEM
    )
    total_cells = float(rows * cols * levels * n_gx * n_gy)
    x, r, norms = pl.pallas_call(
        functools.partial(finish, total_cells),
        out_shape=(
            jax.ShapeDtypeStruct(block, f32),
            jax.ShapeDtypeStruct(block, f32),
            jax.ShapeDtypeStruct((1, ITERS), f32),
        ),
        in_specs=[VMEM, VMEM, VMEM, VMEM],
        out_specs=(ANY, ANY, VMEM),
        scratch_shapes=[pltpu.VMEM(block, f32), pltpu.VMEM(block, f32), sems((2, 2))],
    )(in_vmem(totals), in_vmem(start), in_vmem(fields), in_vmem(images))
    shape = right_side.shape
    return x.reshape(shape), r.reshape(shape), norms.reshape(ITERS)


def solution(mesh):
    n_gx, n_gy = mesh.shape["gx"], mesh.shape["gy"]
    field = P("gy", "gx", None)
    return jax.shard_map(
        functools.partial(on_device, n_gx, n_gy),
        mesh=mesh,
        in_specs=(field, field, field, P(), P(), P()),
        out_specs=(field, field, P()),
        check_vma=False,
    )
```

```python
import functools

import jax
import jax.numpy as jnp
from jax import lax
from jax.experimental import pallas as pl
from jax.experimental.pallas import tpu as pltpu
from jax.sharding import PartitionSpec as P

ITERS = 3
KEYS = [(i, j) for j in range(ITERS + 1) for i in range(j + 1)]
MESH = pl.DeviceIdType.MESH
ANY = pl.BlockSpec(memory_space=pl.ANY)
VMEM = pl.BlockSpec(memory_space=pltpu.VMEM)


def kernel(
    n_gx,
    n_gy,
    out_rows,
    edge_table,
    right_side,
    diagonal,
    horizontal,
    vertical,
    precond,
    fields,
    images,
    out_totals,
    r0,
    diag,
    horiz,
    vert,
    matrix,
    frame_z,
    pack,
    mini_out,
    mini_in,
    wide,
    from_east,
    from_west,
    from_north,
    from_south,
    far_pack,
    near_pack,
    far_last,
    gathered,
    strip,
    outside,
    partial,
    sums,
    edge_rows,
    load_sem,
    col_send,
    east_recv,
    west_recv,
    far_send,
    far_recv,
    relay_send,
    relay_recv,
    near_send,
    near_recv,
    mini_send,
    mini_recv,
    row_send,
    north_recv,
    south_recv,
    sum_send,
    sum_recv,
):
    rows, levels = out_rows, r0.shape[-1]
    cells = r0.shape[0]
    cols = cells // rows
    tall = n_gy * rows
    gx, gy = lax.axis_index("gx"), lax.axis_index("gy")
    n_all = n_gx * n_gy
    half = n_gx // 2
    me = gx * n_gy + gy

    def for_others(visit):
        def step(i, carry):
            for j in range(n_gy):
                visit(lax.rem(gx + i, n_gx), lax.rem(gy + j, n_gy))
            return carry

        if n_all <= 64:
            for i in sorted(range(1, n_gx), key=lambda i: min(i, n_gx - i)):
                step(i, 0)
        else:
            lax.fori_loop(1, n_gx, step, 0)
        for j in range(1, n_gy):
            visit(gx, lax.rem(gy + j, n_gy))

    barrier = pltpu.get_barrier_semaphore()

    def greet(x, y):
        pl.semaphore_signal(barrier, inc=1, device_id=(x, y), device_id_type=MESH)

    for_others(greet)

    panel = lax.convert_element_type(gx >= half, jnp.int32)
    loads = [
        pltpu.make_async_copy(right_side, r0, load_sem.at[0]),
        pltpu.make_async_copy(precond.at[panel], matrix.at[pl.ds(0, levels)], load_sem.at[1]),
        pltpu.make_async_copy(horizontal, horiz, load_sem.at[2]),
        pltpu.make_async_copy(diagonal, diag, load_sem.at[3]),
        pltpu.make_async_copy(vertical, vert, load_sem.at[4]),
        pltpu.make_async_copy(edge_table, edge_rows, load_sem.at[5]),
        pltpu.make_async_copy(precond.at[1 - panel], matrix.at[pl.ds(levels, levels)], load_sem.at[6]),
    ]
    for load in loads:
        load.start()

    east_x, west_x = lax.rem(gx + 1, n_gx), lax.rem(gx + n_gx - 1, n_gx)
    east_border = (gx == half - 1) | (gx == n_gx - 1)
    west_border = (gx == half) | (gx == 0)
    border = east_border | west_border
    far_x = jnp.where(east_border, east_x, west_x)
    side = jnp.where(east_border, 0, 1)
    table = jnp.where((gx == half - 1) | (gx == half), 0, 1)
    edge_cols = [
        pl.ds(jnp.where(east_border, cols - 1 - i, i), rows, stride=cols) for i in range(3)
    ]
    first_row = pl.multiple_of(gy * rows, rows)
    own = pl.ds(first_row, rows)
    has_north, has_south = gy < n_gy - 1, gy > 0

    @pl.when(jnp.logical_not(has_north))
    def _():
        from_north[...] = jnp.zeros_like(from_north)

    @pl.when(jnp.logical_not(has_south))
    def _():
        from_south[...] = jnp.zeros_like(from_south)

    outside[...] = jnp.zeros_like(outside)

    def precondition(v, panels=1):
        return lax.dot_general(
            v,
            matrix[pl.ds(0, panels * levels), :],
            (((1,), (1,)), ((), ())),
            precision=lax.Precision.HIGHEST,
            preferred_element_type=jnp.float32,
        )

    def col_copy(t, side):
        buffer, recv, x = (
            (from_west, west_recv, east_x) if side == 0 else (from_east, east_recv, west_x)
        )
        return pltpu.make_async_remote_copy(
            src_ref=frame_z.at[t, pl.ds(side * rows, rows)],
            dst_ref=buffer.at[t],
            send_sem=col_send.at[t, side],
            recv_sem=recv.at[t],
            device_id=(x, gy),
            device_id_type=MESH,
        )

    def far_copy(t, g):
        return pltpu.make_async_remote_copy(
            src_ref=pack.at[pl.ds(0, 4)] if t == 0 else pack.at[5],
            dst_ref=far_pack.at[:, own] if t == 0 else far_last.at[own],
            send_sem=far_send.at[t],
            recv_sem=far_recv.at[t],
            device_id=(far_x, g),
            device_id_type=MESH,
        )

    def relay_copy(g):
        return pltpu.make_async_remote_copy(
            src_ref=far_pack.at[:, own],
            dst_ref=far_pack.at[:, own],
            send_sem=relay_send,
            recv_sem=relay_recv,
            device_id=(gx, g),
            device_id_type=MESH,
        )

    def near_copy(g):
        return pltpu.make_async_remote_copy(
            src_ref=pack.at[pl.ds(0, 5)],
            dst_ref=near_pack.at[:, own],
            send_sem=near_send,
            recv_sem=near_recv,
            device_id=(gx, g),
            device_id_type=MESH,
        )

    def mini_copy(side):
        return pltpu.make_async_remote_copy(
            src_ref=mini_out.at[side],
            dst_ref=mini_in.at[side],
            send_sem=mini_send.at[side],
            recv_sem=mini_recv.at[side],
            device_id=(gx, gy + 1 if side == 0 else gy - 1),
            device_id_type=MESH,
        )

    def row_copy(t, side):
        buffer, recv, y, row = (
            (from_south, south_recv, gy + 1, 2 * rows + cols)
            if side == 0
            else (from_north, north_recv, gy - 1, 2 * rows)
        )
        return pltpu.make_async_remote_copy(
            src_ref=frame_z.at[t, pl.ds(row, cols)],
            dst_ref=buffer.at[t],
            send_sem=row_send.at[t, side],
            recv_sem=recv.at[t],
            device_id=(gx, y),
            device_id_type=MESH,
        )

    def for_rows(visit):
        @pl.when(has_north)
        def _():
            visit(0)

        @pl.when(has_south)
        def _():
            visit(1)

    def fill_packs():
        c0, c1, c2 = edge_cols
        inward = 2 * (rows + cols)
        items = [
            frame_z[0, pl.ds(side * rows, rows), :],
            frame_z[0, pl.ds(inward, rows), :],
            horiz[c0, :],
            diag[c0, :],
            horiz[c1, :],
        ]
        for k, item in enumerate(items):
            pack[k] = item
            near_pack[k, own, :] = item
            if k < 4:
                wide[k] = jnp.zeros_like(wide[k])
                wide[k, pl.ds(8, rows), :] = item
        for to, first, second in ((0, rows - 1, rows - 2), (1, 0, 1)):
            picks = [(0, first), (0, second), (1, first), (2, first), (3, first)]
            for k, (item, row) in enumerate(picks):
                mini_out[to, pl.ds(k, 1), :] = items[item][row : row + 1]
            mini_out[to, pl.ds(5, 3), :] = jnp.zeros((3, levels), jnp.float32)

    def send_frame(t, frame):
        z = precondition(frame)
        frame_z[t, pl.ds(0, z.shape[0]), :] = z
        if t == 0:
            pl.when(border)(fill_packs)
            pl.semaphore_wait(barrier, n_all - 1)

            @pl.when(border)
            def _():
                for_rows(lambda side: mini_copy(side).start())

        @pl.when(jnp.logical_not(east_border))
        def _():
            col_copy(t, 0).start()

        @pl.when(jnp.logical_not(west_border))
        def _():
            col_copy(t, 1).start()

        for_rows(lambda side: row_copy(t, side).start())
        if t == 0:

            @pl.when(border)
            def _():
                far_copy(0, gy).start()
                pl.when(gx == 0)(functools.partial(send_far, 0, 1))
                for j in range(1, n_gy):
                    near_copy(lax.rem(gy + j, n_gy)).start()

    def send_far(t, first=0):
        for j in sorted(range(first, n_gy), key=lambda j: abs(2 * j - n_gy)):
            far_copy(t, lax.rem(gy + j, n_gy)).start()

    def receive_rows(t):
        @pl.when(has_north)
        def _():
            row_copy(t, 1).wait_recv()

        @pl.when(has_south)
        def _():
            row_copy(t, 0).wait_recv()

    def receive_cols(t):
        @pl.when(jnp.logical_not(east_border))
        def _():
            col_copy(t, 1).wait_recv()
            outside[pl.ds(0, rows), :] = from_east[t]

        @pl.when(jnp.logical_not(west_border))
        def _():
            col_copy(t, 0).wait_recv()
            outside[pl.ds(rows, rows), :] = from_west[t]

    col_id = lax.rem(lax.broadcasted_iota(jnp.int32, (cells, levels), 0), cols)
    east_edge = pl.ds(cols - 1, rows, stride=cols)
    west_edge = pl.ds(0, rows, stride=cols)
    south_edge = pl.ds(0, cols)
    north_edge = pl.ds(cells - cols, cols)

    def edge_columns(ref):
        return jnp.concatenate([ref[east_edge, :], ref[west_edge, :]], 0)

    def column_part(z):
        lane = lax.broadcasted_iota(jnp.int32, z.shape, 1)
        up = jnp.where(lane < levels - 1, pltpu.roll(z, levels - 1, 1), 0.0)
        down = jnp.where(lane > 0, pltpu.roll(z, 1, 1), 0.0)
        return vert[...] * (2.0 * z - (up + down))

    def inner_image(z):
        east = jnp.where(col_id < cols - 1, pltpu.roll(z, cells - 1, 0), 0.0)
        west = jnp.where(col_id > 0, pltpu.roll(z, 1, 0), 0.0)
        none = jnp.zeros((cols, levels), jnp.float32)
        north = jnp.concatenate([z[cols:], none], 0)
        south = jnp.concatenate([none, z[:-cols]], 0)
        beside = east + west + north + south
        return diag[...] * z + horiz[...] * (4.0 * z - beside) + column_part(z)

    def product(a, b):
        both = (a * b).reshape(-1, 8, levels)
        return jnp.sum(jnp.sum(both, axis=0), axis=0, keepdims=True)

    tall_id = lax.broadcasted_iota(jnp.int32, (tall, levels), 0)

    def along(w):
        north = jnp.where(tall_id < tall - 1, pltpu.roll(w, tall - 1, 0), 0.0)
        south = jnp.where(tall_id > 0, pltpu.roll(w, 1, 0), 0.0)
        return north + south

    def stencil(w, d, h):
        return d * w + h * (4.0 * w - along(w)) + column_part(w)

    def gather_rows(start, count, pairs):
        def one(y):
            row = edge_rows[table, start + y]
            for dst, src in pairs:
                gathered[dst, pl.ds(y, 1), :] = src[pl.ds(row, 1), :]

        if count <= 64:
            for y in range(count):
                one(y)
        else:

            def body(y, carry):
                one(y)
                return carry

            lax.fori_loop(0, count, body, 0)

    def wait_bytes(ref, sem):
        pltpu.make_async_copy(ref, ref, sem).wait()

    near_rest = pl.ds(0, (n_gy - 1) * rows)
    last = gx == n_gx - 1
    relays = border & jnp.logical_not(last)

    def relay():
        wait_bytes(far_pack.at[:, own], far_recv.at[0])
        for j in sorted(range(1, n_gy), key=lambda j: abs(2 * j - n_gy)):
            relay_copy(lax.rem(gy + j, n_gy)).start()


    def look_ahead():
        c1 = edge_cols[1]
        inner = pl.ds(8, rows)

        def take(side, near, far):
            mini_copy(side).wait_recv()
            wide[0, pl.ds(near, 1), :] = mini_in[side, pl.ds(0, 1), :]
            wide[0, pl.ds(far, 1), :] = mini_in[side, pl.ds(1, 1), :]
            for k in (1, 2, 3):
                wide[k, pl.ds(near, 1), :] = mini_in[side, pl.ds(k + 1, 1), :]

        pl.when(border & has_south)(functools.partial(take, 0, 7, 6))
        pl.when(border & has_north)(functools.partial(take, 1, 8 + rows, 9 + rows))

        def next_to(w):
            return pltpu.roll(w, w.shape[0] - 1, 0) + pltpu.roll(w, 1, 0)

        z_edge, z_next, h_edge, d_edge = wide[0], wide[1], wide[2], wide[3]
        v_edge = (
            d_edge * z_edge
            + h_edge * (4.0 * z_edge - z_next - next_to(z_edge))
            + column_part(z_edge)
        )
        beside = next_to(z_next)[8 : 8 + rows] + z_edge[8 : 8 + rows]
        z1 = z_next[8 : 8 + rows]
        z2 = frame_z[0, pl.ds(2 * (rows + cols) + rows, rows), :]
        v_next = (
            diag[c1, :] * z1 + horiz[c1, :] * (4.0 * z1 - beside - z2) + column_part(z1)
        )
        z = precondition(jnp.concatenate([v_edge, v_next], 0))
        z_edge, z_next = z[: rows + 16], z[rows + 16 :]
        beside = next_to(z_edge)[8 : 8 + rows] + z_next
        z_edge = z_edge[8 : 8 + rows]
        h_own, d_own = h_edge[8 : 8 + rows], d_edge[8 : 8 + rows]
        v = d_own * z_edge + h_own * (4.0 * z_edge - beside) + column_part(z_edge)
        pack[5] = precondition(v)
        pl.when(border)(functools.partial(send_far, 1))

    def correct_early():
        @pl.when(border)
        def _():
            pl.when(last)(lambda: wait_bytes(far_pack, far_recv.at[0]))
            pl.when(relays)(lambda: wait_bytes(far_pack.at[:, near_rest], relay_recv))
            wait_bytes(near_pack.at[:, near_rest], near_recv)

        gather_rows(0, tall, [(0, far_pack.at[0]), (1, near_pack.at[0])])
        h_near, d_near = near_pack[2], near_pack[3]
        h_far, d_far = far_pack[2], far_pack[3]
        b_near, b_far = -(h_near * gathered[0]), -(h_far * gathered[1])
        v_near = stencil(near_pack[0], d_near, h_near) - h_near * near_pack[1] + b_near
        v_far = stencil(far_pack[0], d_far, h_far) - h_far * far_pack[1] + b_far
        out = precondition(jnp.concatenate([b_near, v_near, b_far, v_far], 0), 2)
        w_near, w_far = out[:tall, :levels], out[2 * tall : 3 * tall, levels:]
        strip[0] = b_near
        strip[1] = w_near
        strip[3] = out[3 * tall :, levels:]
        strip[4] = out[tall : 2 * tall, :levels]
        gather_rows(0, tall, [(0, strip.at[3]), (1, strip.at[4])])
        b_near = stencil(w_near, d_near, h_near) - h_near * gathered[0]
        b_far = stencil(w_far, d_far, h_far) - h_far * gathered[1]
        b_next = -(near_pack[4] * w_near)
        out = precondition(jnp.concatenate([b_near, b_next, b_far], 0), 2)
        w_edge, w_next = out[:tall, :levels], out[tall : 2 * tall, :levels]
        strip[3] = b_near
        strip[4] = b_next
        strip[5] = out[2 * tall :, levels:]
        strip[6] = w_edge
        strip[7] = w_next
        strip[8] = along(w_next)
        strip[9] = stencil(w_edge, d_near, h_near) - h_near * w_next

    def correct_third():
        c0, c1, c2 = edge_cols
        w_edge, w_next, beside = strip[6, own, :], strip[7, own, :], strip[8, own, :]
        h1 = horiz[c1, :]
        later = diag[c1, :] * w_next + h1 * (4.0 * w_next - beside - w_edge) + column_part(w_next)
        b_third = -(horiz[c2, :] * w_next)
        gather_rows(first_row, rows, [(2, strip.at[5])])
        wait_bytes(far_last, far_recv.at[1])
        gather_rows(first_row, rows, [(3, far_last)])
        across = gathered[2, pl.ds(0, rows), :] + gathered[3, pl.ds(0, rows), :]
        b_edge = strip[9, own, :] - horiz[c0, :] * across
        none = jnp.zeros((rows, levels), jnp.float32)
        changes = [
            [strip[0, own, :], none, none],
            [strip[3, own, :], strip[4, own, :], none],
            [b_edge, later, b_third],
        ]
        before = [jnp.concatenate([r0[c, :] for c in edge_cols], 0)]
        after = [before[0]]
        for t in range(ITERS):
            old = jnp.concatenate([images[t, c, :] for c in edge_cols], 0)
            new = old + jnp.concatenate(changes[t], 0)
            before.append(old)
            after.append(new)
            for k in range(t + 1):
                images[t, edge_cols[k], :] = new[k * rows : (k + 1) * rows]
        for k, (i, j) in enumerate(KEYS):
            if j > 0:
                partial[pl.ds(k, 1), :] += product(after[i], after[j]) - product(before[i], before[j])

    for load in loads:
        load.wait()
    terms = {}
    spaces = [r0]
    frame = [edge_columns(r0), r0[south_edge, :], r0[north_edge, :]]
    send_frame(0, jnp.concatenate(frame + [r0[c, :] for c in edge_cols[1:]], 0))
    edge_horiz = edge_columns(horiz)
    for t in range(ITERS):
        image = images.at[t]
        z = precondition(spaces[-1][...])
        fields[t] = z
        newest = len(spaces) - 1
        for i in range(len(spaces)):
            terms[(i, newest)] = product(spaces[i][...], spaces[newest][...])
        image[...] = inner_image(z)
        if t == 0:
            look_ahead()
        if t == 1:
            pl.when(relays)(relay)
        if t == ITERS - 1:
            correct_early()
        receive_rows(t)
        image[south_edge, :] = image[south_edge, :] - horiz[south_edge, :] * from_south[t]
        image[north_edge, :] = image[north_edge, :] - horiz[north_edge, :] * from_north[t]
        inside = edge_columns(image)
        receive_cols(t)
        edges = inside - edge_horiz * outside[...]
        image[east_edge, :] = edges[:rows]
        image[west_edge, :] = edges[rows:]
        if t < ITERS - 1:
            frame = [edges, image[south_edge, :], image[north_edge, :]]
            send_frame(t + 1, jnp.concatenate(frame, 0))
        spaces.append(image)
    newest = len(spaces) - 1
    for i in range(len(spaces)):
        terms[(i, newest)] = product(spaces[i][...], spaces[newest][...])
    for k, key in enumerate(KEYS):
        partial[pl.ds(k, 1), :] = terms[key]

    @pl.when(border)
    def _():
        correct_third()

    height = -(-len(KEYS) // 8) * 8
    row_id = lax.broadcasted_iota(jnp.int32, (height, levels), 0)
    lane = lax.broadcasted_iota(jnp.int32, (height, levels), 1)
    stacked = jnp.where(row_id < len(KEYS), partial[...], 0.0)
    summed = jnp.sum(stacked, axis=1, keepdims=True)
    sums[me] = jnp.sum(jnp.where(lane == row_id, summed, 0.0), axis=0, keepdims=True)

    def tell(x, y):
        pltpu.make_async_remote_copy(
            src_ref=sums.at[me],
            dst_ref=sums.at[me],
            send_sem=sum_send,
            recv_sem=sum_recv,
            device_id=(x, y),
            device_id_type=MESH,
        ).start()

    for_others(tell)
    for t in range(ITERS):

        @pl.when(jnp.logical_not(east_border))
        def _(t=t):
            col_copy(t, 0).wait_send()

        @pl.when(jnp.logical_not(west_border))
        def _(t=t):
            col_copy(t, 1).wait_send()

        @pl.when(has_north)
        def _(t=t):
            row_copy(t, 0).wait_send()

        @pl.when(has_south)
        def _(t=t):
            row_copy(t, 1).wait_send()

    @pl.when(border)
    def _():
        wait_bytes(far_pack.at[:, own], far_send.at[0])
        pl.when(gx == 0)(lambda: wait_bytes(far_pack.at[:, near_rest], far_send.at[0]))
        pl.when(relays)(lambda: wait_bytes(far_pack.at[:, near_rest], relay_send))
        wait_bytes(far_last, far_send.at[1])
        wait_bytes(near_pack.at[:, near_rest], near_send)
        for_rows(lambda side: mini_copy(side).wait_send())
        c0, c1, c2 = edge_cols
        fields[1, c0, :] += strip[1, own, :]
        fields[2, c0, :] += strip[6, own, :]
        fields[2, c1, :] += strip[7, own, :]

    others = sums.at[pl.ds(0, n_all - 1)]
    wait_bytes(others, sum_recv)
    out_totals[...] = jnp.sum(sums[...], axis=0)
    wait_bytes(others, sum_send)


def finish(total_cells, all_totals, r0, fields, images, out_x, out_r, out_norms, x, r, sem):
    levels = r0.shape[-1]
    totals = all_totals[...]
    value = {key: totals[:, k : k + 1] for k, key in enumerate(KEYS)}

    rho, g0, g1, g2 = value[(0, 0)], value[(0, 1)], value[(0, 2)], value[(0, 3)]
    a00, a01, a02 = value[(1, 1)], value[(1, 2)], value[(1, 3)]
    a11, a12, a22 = value[(2, 2)], value[(2, 3)], value[(3, 3)]
    l10, l20, y0 = a01 / a00, a02 / a00, g0 / a00
    d1, e12, f1 = a11 - l10 * a01, a12 - l10 * a02, g1 - l10 * g0
    l21, y1 = e12 / d1, f1 / d1
    d2, f2 = a22 - l20 * a02 - l21 * e12, g2 - l20 * g0 - l21 * f1
    y2 = f2 / d2
    norm0 = rho - y0 * g0
    norm1 = norm0 - y1 * f1
    norm2 = norm1 - y2 * f2
    y1 = y1 - l21 * y2
    y0 = y0 - l10 * y1 - l20 * y2
    norm_lane = lax.broadcasted_iota(jnp.int32, (1, levels), 1)
    norms = jnp.where(norm_lane == 0, norm0, jnp.where(norm_lane == 1, norm1, norm2))
    out_norms[...] = norms[:, :ITERS] / total_cells
    rows = r0.shape[0]
    pieces = 2 if rows % 16 == 0 else 1
    size = rows // pieces
    copies = []
    for p in range(pieces):
        span = pl.ds(p * size, size)
        x[span] = y0 * fields[0, span] + y1 * fields[1, span] + y2 * fields[2, span]
        r[span] = (
            r0[span] - y0 * images[0, span] - y1 * images[1, span] - y2 * images[2, span]
        )
        for k, (src, dst) in enumerate(((x, out_x), (r, out_r))):
            copy = pltpu.make_async_copy(src.at[span], dst.at[span], sem.at[p, k])
            copy.start()
            copies.append(copy)
    for copy in copies:
        copy.wait()


def on_device(n_gx, n_gy, right_side, diagonal, horizontal, vertical, precond, edge_rows):
    rows, cols, levels = right_side.shape
    f32 = jnp.float32
    block = (rows * cols, levels)
    column = (n_gy * rows, levels)
    sems = pltpu.SemaphoreType.DMA
    basis = pltpu.VMEM((ITERS,) + block, f32)
    fields, images, totals, start = pl.pallas_call(
        functools.partial(kernel, n_gx, n_gy, rows),
        out_shape=(basis, basis, pltpu.VMEM((1, levels), f32), pltpu.VMEM(block, f32)),
        in_specs=[ANY, ANY, ANY, ANY, ANY, ANY],
        out_specs=(VMEM, VMEM, VMEM, VMEM),
        scratch_shapes=[
            pltpu.VMEM(block, f32),
            pltpu.VMEM(block, f32),
            pltpu.VMEM((1, levels), f32),
            pltpu.VMEM((2 * levels, levels), f32),
            pltpu.VMEM((ITERS, 4 * rows + 2 * cols, levels), f32),
            pltpu.VMEM((6, rows, levels), f32),
            pltpu.VMEM((2, 8, levels), f32),
            pltpu.VMEM((2, 8, levels), f32),
            pltpu.VMEM((4, rows + 16, levels), f32),
            pltpu.VMEM((ITERS, rows, levels), f32),
            pltpu.VMEM((ITERS, rows, levels), f32),
            pltpu.VMEM((ITERS, cols, levels), f32),
            pltpu.VMEM((ITERS, cols, levels), f32),
            pltpu.VMEM((4,) + column, f32),
            pltpu.VMEM((5,) + column, f32),
            pltpu.VMEM(column, f32),
            pltpu.VMEM((4,) + column, f32),
            pltpu.VMEM((10,) + column, f32),
            pltpu.VMEM((2 * rows, levels), f32),
            pltpu.VMEM((16, levels), f32),
            pltpu.VMEM((n_gx * n_gy, 1, levels), f32),
            pltpu.SMEM(edge_rows.shape, jnp.int32),
            sems((7,)),
            sems((ITERS, 2)),
            sems((ITERS,)),
            sems((ITERS,)),
            sems((2,)),
            sems((2,)),
            sems(()),
            sems(()),
            sems(()),
            sems(()),
            sems((2,)),
            sems((2,)),
            sems((ITERS, 2)),
            sems((ITERS,)),
            sems((ITERS,)),
            sems(()),
            sems(()),
        ],
        compiler_params=pltpu.CompilerParams(collective_id=0, has_side_effects=True),
    )(
        edge_rows,
        right_side.reshape(block),
        diagonal.reshape(block),
        horizontal.reshape(block),
        vertical.reshape(1, levels),
        precond,
    )
    in_vmem = functools.partial(
        pltpu.with_memory_space_constraint, memory_space=pltpu.VMEM
    )
    total_cells = float(rows * cols * levels * n_gx * n_gy)
    x, r, norms = pl.pallas_call(
        functools.partial(finish, total_cells),
        out_shape=(
            jax.ShapeDtypeStruct(block, f32),
            jax.ShapeDtypeStruct(block, f32),
            jax.ShapeDtypeStruct((1, ITERS), f32),
        ),
        in_specs=[VMEM, VMEM, VMEM, VMEM],
        out_specs=(ANY, ANY, VMEM),
        scratch_shapes=[pltpu.VMEM(block, f32), pltpu.VMEM(block, f32), sems((2, 2))],
    )(in_vmem(totals), in_vmem(start), in_vmem(fields), in_vmem(images))
    shape = right_side.shape
    return x.reshape(shape), r.reshape(shape), norms.reshape(ITERS)


def solution(mesh):
    n_gx, n_gy = mesh.shape["gx"], mesh.shape["gy"]
    field = P("gy", "gx", None)
    return jax.shard_map(
        functools.partial(on_device, n_gx, n_gy),
        mesh=mesh,
        in_specs=(field, field, field, P(), P(), P()),
        out_specs=(field, field, P()),
        check_vma=False,
    )
```

```python
import functools

import jax
import jax.numpy as jnp
from jax import lax
from jax.experimental import pallas as pl
from jax.experimental.pallas import tpu as pltpu
from jax.sharding import PartitionSpec as P

ITERS = 3
KEYS = [(i, j) for j in range(ITERS + 1) for i in range(j + 1)]
MESH = pl.DeviceIdType.MESH
ANY = pl.BlockSpec(memory_space=pl.ANY)
VMEM = pl.BlockSpec(memory_space=pltpu.VMEM)


def kernel(
    n_gx,
    n_gy,
    out_rows,
    edge_table,
    right_side,
    diagonal,
    horizontal,
    vertical,
    precond,
    fields,
    images,
    out_totals,
    r0,
    diag,
    horiz,
    vert,
    matrix,
    weights,
    frame_z,
    pack,
    mini_out,
    mini_in,
    wide,
    from_east,
    from_west,
    from_north,
    from_south,
    far_pack,
    near_pack,
    far_last,
    gathered,
    strip,
    outside,
    partial,
    sums,
    edge_rows,
    load_sem,
    col_send,
    east_recv,
    west_recv,
    far_send,
    far_recv,
    relay_send,
    relay_recv,
    near_send,
    near_recv,
    mini_send,
    mini_recv,
    row_send,
    north_recv,
    south_recv,
    sum_send,
    sum_recv,
):
    rows, levels = out_rows, r0.shape[-1]
    cells = r0.shape[0]
    cols = cells // rows
    tall = n_gy * rows
    gx, gy = lax.axis_index("gx"), lax.axis_index("gy")
    n_all = n_gx * n_gy
    half = n_gx // 2
    me = gx * n_gy + gy

    def for_others(visit):
        def step(i, carry):
            for j in range(n_gy):
                visit(lax.rem(gx + i, n_gx), lax.rem(gy + j, n_gy))
            return carry

        if n_all <= 64:
            for i in sorted(range(1, n_gx), key=lambda i: min(i, n_gx - i)):
                step(i, 0)
        else:
            lax.fori_loop(1, n_gx, step, 0)
        for j in range(1, n_gy):
            visit(gx, lax.rem(gy + j, n_gy))

    barrier = pltpu.get_barrier_semaphore()

    def greet(x, y):
        pl.semaphore_signal(barrier, inc=1, device_id=(x, y), device_id_type=MESH)

    for_others(greet)

    panel = lax.convert_element_type(gx >= half, jnp.int32)
    loads = [
        pltpu.make_async_copy(right_side, r0, load_sem.at[0]),
        pltpu.make_async_copy(precond.at[panel], matrix.at[pl.ds(0, levels)], load_sem.at[1]),
        pltpu.make_async_copy(horizontal, horiz, load_sem.at[2]),
        pltpu.make_async_copy(diagonal, diag, load_sem.at[3]),
        pltpu.make_async_copy(vertical, vert, load_sem.at[4]),
        pltpu.make_async_copy(edge_table, edge_rows, load_sem.at[5]),
        pltpu.make_async_copy(precond.at[1 - panel], matrix.at[pl.ds(levels, levels)], load_sem.at[6]),
    ]
    for load in loads:
        load.start()

    east_x, west_x = lax.rem(gx + 1, n_gx), lax.rem(gx + n_gx - 1, n_gx)
    east_border = (gx == half - 1) | (gx == n_gx - 1)
    west_border = (gx == half) | (gx == 0)
    border = east_border | west_border
    far_x = jnp.where(east_border, east_x, west_x)
    side = jnp.where(east_border, 0, 1)
    table = jnp.where((gx == half - 1) | (gx == half), 0, 1)
    edge_cols = [
        pl.ds(jnp.where(east_border, cols - 1 - i, i), rows, stride=cols) for i in range(3)
    ]
    first_row = pl.multiple_of(gy * rows, rows)
    own = pl.ds(first_row, rows)
    has_north, has_south = gy < n_gy - 1, gy > 0

    @pl.when(jnp.logical_not(has_north))
    def _():
        from_north[...] = jnp.zeros_like(from_north)

    @pl.when(jnp.logical_not(has_south))
    def _():
        from_south[...] = jnp.zeros_like(from_south)

    outside[...] = jnp.zeros_like(outside)

    def split(v):
        high = v.astype(jnp.bfloat16)
        return high, (v - high.astype(jnp.float32)).astype(jnp.bfloat16)

    def prepare_weights():
        for which in range(2):
            for part, value in enumerate(split(matrix[pl.ds(which * levels, levels), :])):
                for twice in range(2):
                    weights[
                        which, pl.ds(part * levels, levels), pl.ds(twice * levels, levels)
                    ] = value

    def precondition(v, which=0):
        out = lax.dot_general(
            jnp.concatenate(split(v), 1),
            weights[which],
            (((1,), (1,)), ((), ())),
            preferred_element_type=jnp.float32,
        )
        return out[:, :levels] + out[:, levels:]

    def col_copy(t, side):
        buffer, recv, x = (
            (from_west, west_recv, east_x) if side == 0 else (from_east, east_recv, west_x)
        )
        return pltpu.make_async_remote_copy(
            src_ref=frame_z.at[t, pl.ds(side * rows, rows)],
            dst_ref=buffer.at[t],
            send_sem=col_send.at[t, side],
            recv_sem=recv.at[t],
            device_id=(x, gy),
            device_id_type=MESH,
        )

    def far_copy(t, g):
        return pltpu.make_async_remote_copy(
            src_ref=pack.at[pl.ds(0, 4)] if t == 0 else pack.at[5],
            dst_ref=far_pack.at[:, own] if t == 0 else far_last.at[own],
            send_sem=far_send.at[t],
            recv_sem=far_recv.at[t],
            device_id=(far_x, g),
            device_id_type=MESH,
        )

    def relay_copy(g):
        return pltpu.make_async_remote_copy(
            src_ref=far_pack.at[:, own],
            dst_ref=far_pack.at[:, own],
            send_sem=relay_send,
            recv_sem=relay_recv,
            device_id=(gx, g),
            device_id_type=MESH,
        )

    def near_copy(g):
        return pltpu.make_async_remote_copy(
            src_ref=pack.at[pl.ds(0, 5)],
            dst_ref=near_pack.at[:, own],
            send_sem=near_send,
            recv_sem=near_recv,
            device_id=(gx, g),
            device_id_type=MESH,
        )

    def mini_copy(side):
        return pltpu.make_async_remote_copy(
            src_ref=mini_out.at[side],
            dst_ref=mini_in.at[side],
            send_sem=mini_send.at[side],
            recv_sem=mini_recv.at[side],
            device_id=(gx, gy + 1 if side == 0 else gy - 1),
            device_id_type=MESH,
        )

    def row_copy(t, side):
        buffer, recv, y, row = (
            (from_south, south_recv, gy + 1, 2 * rows + cols)
            if side == 0
            else (from_north, north_recv, gy - 1, 2 * rows)
        )
        return pltpu.make_async_remote_copy(
            src_ref=frame_z.at[t, pl.ds(row, cols)],
            dst_ref=buffer.at[t],
            send_sem=row_send.at[t, side],
            recv_sem=recv.at[t],
            device_id=(gx, y),
            device_id_type=MESH,
        )

    def for_rows(visit):
        @pl.when(has_north)
        def _():
            visit(0)

        @pl.when(has_south)
        def _():
            visit(1)

    def fill_packs():
        c0, c1, c2 = edge_cols
        inward = 2 * (rows + cols)
        items = [
            frame_z[0, pl.ds(side * rows, rows), :],
            frame_z[0, pl.ds(inward, rows), :],
            horiz[c0, :],
            diag[c0, :],
            horiz[c1, :],
        ]
        for k, item in enumerate(items):
            pack[k] = item
            near_pack[k, own, :] = item
            if k < 4:
                wide[k] = jnp.zeros_like(wide[k])
                wide[k, pl.ds(8, rows), :] = item
        for to, first, second in ((0, rows - 1, rows - 2), (1, 0, 1)):
            picks = [(0, first), (0, second), (1, first), (2, first), (3, first)]
            for k, (item, row) in enumerate(picks):
                mini_out[to, pl.ds(k, 1), :] = items[item][row : row + 1]
            mini_out[to, pl.ds(5, 3), :] = jnp.zeros((3, levels), jnp.float32)

    def send_frame(t, frame):
        z = precondition(frame)
        frame_z[t, pl.ds(0, z.shape[0]), :] = z
        if t == 0:
            pl.when(border)(fill_packs)
            pl.semaphore_wait(barrier, n_all - 1)

            @pl.when(border)
            def _():
                for_rows(lambda side: mini_copy(side).start())

        @pl.when(jnp.logical_not(east_border))
        def _():
            col_copy(t, 0).start()

        @pl.when(jnp.logical_not(west_border))
        def _():
            col_copy(t, 1).start()

        for_rows(lambda side: row_copy(t, side).start())
        if t == 0:

            @pl.when(border)
            def _():
                far_copy(0, gy).start()
                pl.when(gx == 0)(functools.partial(send_far, 0, 1))
                for j in range(1, n_gy):
                    near_copy(lax.rem(gy + j, n_gy)).start()

    def send_far(t, first=0):
        for j in sorted(range(first, n_gy), key=lambda j: abs(2 * j - n_gy)):
            far_copy(t, lax.rem(gy + j, n_gy)).start()

    def receive_rows(t):
        @pl.when(has_north)
        def _():
            row_copy(t, 1).wait_recv()

        @pl.when(has_south)
        def _():
            row_copy(t, 0).wait_recv()

    def receive_cols(t):
        @pl.when(jnp.logical_not(east_border))
        def _():
            col_copy(t, 1).wait_recv()
            outside[pl.ds(0, rows), :] = from_east[t]

        @pl.when(jnp.logical_not(west_border))
        def _():
            col_copy(t, 0).wait_recv()
            outside[pl.ds(rows, rows), :] = from_west[t]

    col_id = lax.rem(lax.broadcasted_iota(jnp.int32, (cells, levels), 0), cols)
    east_edge = pl.ds(cols - 1, rows, stride=cols)
    west_edge = pl.ds(0, rows, stride=cols)
    south_edge = pl.ds(0, cols)
    north_edge = pl.ds(cells - cols, cols)

    def edge_columns(ref):
        return jnp.concatenate([ref[east_edge, :], ref[west_edge, :]], 0)

    def column_part(z):
        lane = lax.broadcasted_iota(jnp.int32, z.shape, 1)
        up = jnp.where(lane < levels - 1, pltpu.roll(z, levels - 1, 1), 0.0)
        down = jnp.where(lane > 0, pltpu.roll(z, 1, 1), 0.0)
        return vert[...] * (2.0 * z - (up + down))

    def inner_image(z):
        east = jnp.where(col_id < cols - 1, pltpu.roll(z, cells - 1, 0), 0.0)
        west = jnp.where(col_id > 0, pltpu.roll(z, 1, 0), 0.0)
        none = jnp.zeros((cols, levels), jnp.float32)
        north = jnp.concatenate([z[cols:], none], 0)
        south = jnp.concatenate([none, z[:-cols]], 0)
        beside = east + west + north + south
        return diag[...] * z + horiz[...] * (4.0 * z - beside) + column_part(z)

    def product(a, b):
        both = (a * b).reshape(-1, 8, levels)
        return jnp.sum(jnp.sum(both, axis=0), axis=0, keepdims=True)

    tall_id = lax.broadcasted_iota(jnp.int32, (tall, levels), 0)

    def along(w):
        north = jnp.where(tall_id < tall - 1, pltpu.roll(w, tall - 1, 0), 0.0)
        south = jnp.where(tall_id > 0, pltpu.roll(w, 1, 0), 0.0)
        return north + south

    def stencil(w, d, h):
        return d * w + h * (4.0 * w - along(w)) + column_part(w)

    def gather_rows(start, count, pairs):
        def one(y):
            row = edge_rows[table, start + y]
            for dst, src in pairs:
                gathered[dst, pl.ds(y, 1), :] = src[pl.ds(row, 1), :]

        if count <= 64:
            for y in range(count):
                one(y)
        else:

            def body(y, carry):
                one(y)
                return carry

            lax.fori_loop(0, count, body, 0)

    def wait_bytes(ref, sem):
        pltpu.make_async_copy(ref, ref, sem).wait()

    near_rest = pl.ds(0, (n_gy - 1) * rows)
    last = gx == n_gx - 1
    relays = border & jnp.logical_not(last)

    def relay():
        wait_bytes(far_pack.at[:, own], far_recv.at[0])
        for j in sorted(range(1, n_gy), key=lambda j: abs(2 * j - n_gy)):
            relay_copy(lax.rem(gy + j, n_gy)).start()


    def look_ahead():
        c1 = edge_cols[1]
        inner = pl.ds(8, rows)

        def take(side, near, far):
            mini_copy(side).wait_recv()
            wide[0, pl.ds(near, 1), :] = mini_in[side, pl.ds(0, 1), :]
            wide[0, pl.ds(far, 1), :] = mini_in[side, pl.ds(1, 1), :]
            for k in (1, 2, 3):
                wide[k, pl.ds(near, 1), :] = mini_in[side, pl.ds(k + 1, 1), :]

        pl.when(border & has_south)(functools.partial(take, 0, 7, 6))
        pl.when(border & has_north)(functools.partial(take, 1, 8 + rows, 9 + rows))

        def next_to(w):
            return pltpu.roll(w, w.shape[0] - 1, 0) + pltpu.roll(w, 1, 0)

        z_edge, z_next, h_edge, d_edge = wide[0], wide[1], wide[2], wide[3]
        v_edge = (
            d_edge * z_edge
            + h_edge * (4.0 * z_edge - z_next - next_to(z_edge))
            + column_part(z_edge)
        )
        beside = next_to(z_next)[8 : 8 + rows] + z_edge[8 : 8 + rows]
        z1 = z_next[8 : 8 + rows]
        z2 = frame_z[0, pl.ds(2 * (rows + cols) + rows, rows), :]
        v_next = (
            diag[c1, :] * z1 + horiz[c1, :] * (4.0 * z1 - beside - z2) + column_part(z1)
        )
        z = precondition(jnp.concatenate([v_edge, v_next], 0))
        z_edge, z_next = z[: rows + 16], z[rows + 16 :]
        beside = next_to(z_edge)[8 : 8 + rows] + z_next
        z_edge = z_edge[8 : 8 + rows]
        h_own, d_own = h_edge[8 : 8 + rows], d_edge[8 : 8 + rows]
        v = d_own * z_edge + h_own * (4.0 * z_edge - beside) + column_part(z_edge)
        pack[5] = precondition(v)
        pl.when(border)(functools.partial(send_far, 1))

    def correct_early():
        @pl.when(border)
        def _():
            pl.when(last)(lambda: wait_bytes(far_pack, far_recv.at[0]))
            pl.when(relays)(lambda: wait_bytes(far_pack.at[:, near_rest], relay_recv))
            wait_bytes(near_pack.at[:, near_rest], near_recv)

        gather_rows(0, tall, [(0, far_pack.at[0]), (1, near_pack.at[0])])
        h_near, d_near = near_pack[2], near_pack[3]
        h_far, d_far = far_pack[2], far_pack[3]
        b_near, b_far = -(h_near * gathered[0]), -(h_far * gathered[1])
        v_near = stencil(near_pack[0], d_near, h_near) - h_near * near_pack[1] + b_near
        v_far = stencil(far_pack[0], d_far, h_far) - h_far * far_pack[1] + b_far
        near = precondition(jnp.concatenate([b_near, v_near], 0))
        far = precondition(jnp.concatenate([b_far, v_far], 0), 1)
        w_near, w_far = near[:tall], far[:tall]
        strip[0] = b_near
        strip[1] = w_near
        strip[3] = far[tall:]
        strip[4] = near[tall:]
        gather_rows(0, tall, [(0, strip.at[3]), (1, strip.at[4])])
        b_near = stencil(w_near, d_near, h_near) - h_near * gathered[0]
        b_far = stencil(w_far, d_far, h_far) - h_far * gathered[1]
        b_next = -(near_pack[4] * w_near)
        near = precondition(jnp.concatenate([b_near, b_next], 0))
        w_edge, w_next = near[:tall], near[tall:]
        strip[3] = b_near
        strip[4] = b_next
        strip[5] = precondition(b_far, 1)
        strip[6] = w_edge
        strip[7] = w_next
        strip[8] = along(w_next)
        strip[9] = stencil(w_edge, d_near, h_near) - h_near * w_next

    def correct_third():
        c0, c1, c2 = edge_cols
        w_edge, w_next, beside = strip[6, own, :], strip[7, own, :], strip[8, own, :]
        h1 = horiz[c1, :]
        later = diag[c1, :] * w_next + h1 * (4.0 * w_next - beside - w_edge) + column_part(w_next)
        b_third = -(horiz[c2, :] * w_next)
        gather_rows(first_row, rows, [(2, strip.at[5])])
        wait_bytes(far_last, far_recv.at[1])
        gather_rows(first_row, rows, [(3, far_last)])
        across = gathered[2, pl.ds(0, rows), :] + gathered[3, pl.ds(0, rows), :]
        b_edge = strip[9, own, :] - horiz[c0, :] * across
        none = jnp.zeros((rows, levels), jnp.float32)
        changes = [
            [strip[0, own, :], none, none],
            [strip[3, own, :], strip[4, own, :], none],
            [b_edge, later, b_third],
        ]
        before = [jnp.concatenate([r0[c, :] for c in edge_cols], 0)]
        after = [before[0]]
        for t in range(ITERS):
            old = jnp.concatenate([images[t, c, :] for c in edge_cols], 0)
            new = old + jnp.concatenate(changes[t], 0)
            before.append(old)
            after.append(new)
            for k in range(t + 1):
                images[t, edge_cols[k], :] = new[k * rows : (k + 1) * rows]
        for k, (i, j) in enumerate(KEYS):
            if j > 0:
                partial[pl.ds(k, 1), :] += product(after[i], after[j]) - product(before[i], before[j])

    for load in loads:
        load.wait()
    prepare_weights()
    terms = {}
    spaces = [r0]
    frame = [edge_columns(r0), r0[south_edge, :], r0[north_edge, :]]
    send_frame(0, jnp.concatenate(frame + [r0[c, :] for c in edge_cols[1:]], 0))
    edge_horiz = edge_columns(horiz)
    for t in range(ITERS):
        image = images.at[t]
        z = precondition(spaces[-1][...])
        fields[t] = z
        newest = len(spaces) - 1
        for i in range(len(spaces)):
            terms[(i, newest)] = product(spaces[i][...], spaces[newest][...])
        image[...] = inner_image(z)
        if t == 0:
            look_ahead()
        if t == 1:
            pl.when(relays)(relay)
        if t == ITERS - 1:
            correct_early()
        receive_rows(t)
        image[south_edge, :] = image[south_edge, :] - horiz[south_edge, :] * from_south[t]
        image[north_edge, :] = image[north_edge, :] - horiz[north_edge, :] * from_north[t]
        inside = edge_columns(image)
        receive_cols(t)
        edges = inside - edge_horiz * outside[...]
        image[east_edge, :] = edges[:rows]
        image[west_edge, :] = edges[rows:]
        if t < ITERS - 1:
            frame = [edges, image[south_edge, :], image[north_edge, :]]
            send_frame(t + 1, jnp.concatenate(frame, 0))
        spaces.append(image)
    newest = len(spaces) - 1
    for i in range(len(spaces)):
        terms[(i, newest)] = product(spaces[i][...], spaces[newest][...])
    for k, key in enumerate(KEYS):
        partial[pl.ds(k, 1), :] = terms[key]

    @pl.when(border)
    def _():
        correct_third()

    height = -(-len(KEYS) // 8) * 8
    row_id = lax.broadcasted_iota(jnp.int32, (height, levels), 0)
    lane = lax.broadcasted_iota(jnp.int32, (height, levels), 1)
    stacked = jnp.where(row_id < len(KEYS), partial[...], 0.0)
    summed = jnp.sum(stacked, axis=1, keepdims=True)
    sums[me] = jnp.sum(jnp.where(lane == row_id, summed, 0.0), axis=0, keepdims=True)

    def tell(x, y):
        pltpu.make_async_remote_copy(
            src_ref=sums.at[me],
            dst_ref=sums.at[me],
            send_sem=sum_send,
            recv_sem=sum_recv,
            device_id=(x, y),
            device_id_type=MESH,
        ).start()

    for_others(tell)
    for t in range(ITERS):

        @pl.when(jnp.logical_not(east_border))
        def _(t=t):
            col_copy(t, 0).wait_send()

        @pl.when(jnp.logical_not(west_border))
        def _(t=t):
            col_copy(t, 1).wait_send()

        @pl.when(has_north)
        def _(t=t):
            row_copy(t, 0).wait_send()

        @pl.when(has_south)
        def _(t=t):
            row_copy(t, 1).wait_send()

    @pl.when(border)
    def _():
        wait_bytes(far_pack.at[:, own], far_send.at[0])
        pl.when(gx == 0)(lambda: wait_bytes(far_pack.at[:, near_rest], far_send.at[0]))
        pl.when(relays)(lambda: wait_bytes(far_pack.at[:, near_rest], relay_send))
        wait_bytes(far_last, far_send.at[1])
        wait_bytes(near_pack.at[:, near_rest], near_send)
        for_rows(lambda side: mini_copy(side).wait_send())
        c0, c1, c2 = edge_cols
        fields[1, c0, :] += strip[1, own, :]
        fields[2, c0, :] += strip[6, own, :]
        fields[2, c1, :] += strip[7, own, :]

    others = sums.at[pl.ds(0, n_all - 1)]
    wait_bytes(others, sum_recv)
    out_totals[...] = jnp.sum(sums[...], axis=0)
    wait_bytes(others, sum_send)


def finish(total_cells, all_totals, r0, fields, images, out_x, out_r, out_norms, x, r, sem):
    levels = r0.shape[-1]
    totals = all_totals[...]
    value = {key: totals[:, k : k + 1] for k, key in enumerate(KEYS)}

    rho, g0, g1, g2 = value[(0, 0)], value[(0, 1)], value[(0, 2)], value[(0, 3)]
    a00, a01, a02 = value[(1, 1)], value[(1, 2)], value[(1, 3)]
    a11, a12, a22 = value[(2, 2)], value[(2, 3)], value[(3, 3)]
    l10, l20, y0 = a01 / a00, a02 / a00, g0 / a00
    d1, e12, f1 = a11 - l10 * a01, a12 - l10 * a02, g1 - l10 * g0
    l21, y1 = e12 / d1, f1 / d1
    d2, f2 = a22 - l20 * a02 - l21 * e12, g2 - l20 * g0 - l21 * f1
    y2 = f2 / d2
    norm0 = rho - y0 * g0
    norm1 = norm0 - y1 * f1
    norm2 = norm1 - y2 * f2
    y1 = y1 - l21 * y2
    y0 = y0 - l10 * y1 - l20 * y2
    norm_lane = lax.broadcasted_iota(jnp.int32, (1, levels), 1)
    norms = jnp.where(norm_lane == 0, norm0, jnp.where(norm_lane == 1, norm1, norm2))
    out_norms[...] = norms[:, :ITERS] / total_cells
    rows = r0.shape[0]
    pieces = 2 if rows % 16 == 0 else 1
    size = rows // pieces
    copies = []
    for p in range(pieces):
        span = pl.ds(p * size, size)
        x[span] = y0 * fields[0, span] + y1 * fields[1, span] + y2 * fields[2, span]
        r[span] = (
            r0[span] - y0 * images[0, span] - y1 * images[1, span] - y2 * images[2, span]
        )
        for k, (src, dst) in enumerate(((x, out_x), (r, out_r))):
            copy = pltpu.make_async_copy(src.at[span], dst.at[span], sem.at[p, k])
            copy.start()
            copies.append(copy)
    for copy in copies:
        copy.wait()


def on_device(n_gx, n_gy, right_side, diagonal, horizontal, vertical, precond, edge_rows):
    rows, cols, levels = right_side.shape
    f32 = jnp.float32
    block = (rows * cols, levels)
    column = (n_gy * rows, levels)
    sems = pltpu.SemaphoreType.DMA
    basis = pltpu.VMEM((ITERS,) + block, f32)
    fields, images, totals, start = pl.pallas_call(
        functools.partial(kernel, n_gx, n_gy, rows),
        out_shape=(basis, basis, pltpu.VMEM((1, levels), f32), pltpu.VMEM(block, f32)),
        in_specs=[ANY, ANY, ANY, ANY, ANY, ANY],
        out_specs=(VMEM, VMEM, VMEM, VMEM),
        scratch_shapes=[
            pltpu.VMEM(block, f32),
            pltpu.VMEM(block, f32),
            pltpu.VMEM((1, levels), f32),
            pltpu.VMEM((2 * levels, levels), f32),
            pltpu.VMEM((2, 2 * levels, 2 * levels), jnp.bfloat16),
            pltpu.VMEM((ITERS, 4 * rows + 2 * cols, levels), f32),
            pltpu.VMEM((6, rows, levels), f32),
            pltpu.VMEM((2, 8, levels), f32),
            pltpu.VMEM((2, 8, levels), f32),
            pltpu.VMEM((4, rows + 16, levels), f32),
            pltpu.VMEM((ITERS, rows, levels), f32),
            pltpu.VMEM((ITERS, rows, levels), f32),
            pltpu.VMEM((ITERS, cols, levels), f32),
            pltpu.VMEM((ITERS, cols, levels), f32),
            pltpu.VMEM((4,) + column, f32),
            pltpu.VMEM((5,) + column, f32),
            pltpu.VMEM(column, f32),
            pltpu.VMEM((4,) + column, f32),
            pltpu.VMEM((10,) + column, f32),
            pltpu.VMEM((2 * rows, levels), f32),
            pltpu.VMEM((16, levels), f32),
            pltpu.VMEM((n_gx * n_gy, 1, levels), f32),
            pltpu.SMEM(edge_rows.shape, jnp.int32),
            sems((7,)),
            sems((ITERS, 2)),
            sems((ITERS,)),
            sems((ITERS,)),
            sems((2,)),
            sems((2,)),
            sems(()),
            sems(()),
            sems(()),
            sems(()),
            sems((2,)),
            sems((2,)),
            sems((ITERS, 2)),
            sems((ITERS,)),
            sems((ITERS,)),
            sems(()),
            sems(()),
        ],
        compiler_params=pltpu.CompilerParams(collective_id=0, has_side_effects=True),
    )(
        edge_rows,
        right_side.reshape(block),
        diagonal.reshape(block),
        horizontal.reshape(block),
        vertical.reshape(1, levels),
        precond,
    )
    in_vmem = functools.partial(
        pltpu.with_memory_space_constraint, memory_space=pltpu.VMEM
    )
    total_cells = float(rows * cols * levels * n_gx * n_gy)
    x, r, norms = pl.pallas_call(
        functools.partial(finish, total_cells),
        out_shape=(
            jax.ShapeDtypeStruct(block, f32),
            jax.ShapeDtypeStruct(block, f32),
            jax.ShapeDtypeStruct((1, ITERS), f32),
        ),
        in_specs=[VMEM, VMEM, VMEM, VMEM],
        out_specs=(ANY, ANY, VMEM),
        scratch_shapes=[pltpu.VMEM(block, f32), pltpu.VMEM(block, f32), sems((2, 2))],
    )(in_vmem(totals), in_vmem(start), in_vmem(fields), in_vmem(images))
    shape = right_side.shape
    return x.reshape(shape), r.reshape(shape), norms.reshape(ITERS)


def solution(mesh):
    n_gx, n_gy = mesh.shape["gx"], mesh.shape["gy"]
    field = P("gy", "gx", None)
    return jax.shard_map(
        functools.partial(on_device, n_gx, n_gy),
        mesh=mesh,
        in_specs=(field, field, field, P(), P(), P()),
        out_specs=(field, field, P()),
        check_vma=False,
    )
```

```python
import functools

import jax
import jax.numpy as jnp
from jax import lax
from jax.experimental import pallas as pl
from jax.experimental.pallas import tpu as pltpu
from jax.sharding import PartitionSpec as P

ITERS = 3
KEYS = [(i, j) for j in range(ITERS + 1) for i in range(j + 1)]
MESH = pl.DeviceIdType.MESH
ANY = pl.BlockSpec(memory_space=pl.ANY)
VMEM = pl.BlockSpec(memory_space=pltpu.VMEM)


def kernel(
    n_gx,
    n_gy,
    out_rows,
    edge_table,
    right_side,
    diagonal,
    horizontal,
    vertical,
    precond,
    fields,
    images,
    out_totals,
    r0,
    diag,
    horiz,
    vert,
    matrix,
    weights,
    frame_z,
    pack,
    mini_out,
    mini_in,
    wide,
    from_east,
    from_west,
    from_north,
    from_south,
    far_pack,
    near_pack,
    far_last,
    gathered,
    strip,
    outside,
    partial,
    sums,
    edge_rows,
    load_sem,
    col_send,
    east_recv,
    west_recv,
    far_send,
    far_recv,
    relay_send,
    relay_recv,
    near_send,
    near_recv,
    mini_send,
    mini_recv,
    row_send,
    north_recv,
    south_recv,
    sum_send,
    sum_recv,
):
    rows, levels = out_rows, r0.shape[-1]
    cells = r0.shape[0]
    cols = cells // rows
    tall = n_gy * rows
    gx, gy = lax.axis_index("gx"), lax.axis_index("gy")
    n_all = n_gx * n_gy
    half = n_gx // 2
    me = gx * n_gy + gy

    def for_others(visit):
        def step(i, carry):
            for j in range(n_gy):
                visit(lax.rem(gx + i, n_gx), lax.rem(gy + j, n_gy))
            return carry

        if n_all <= 64:
            for i in sorted(range(1, n_gx), key=lambda i: min(i, n_gx - i)):
                step(i, 0)
        else:
            lax.fori_loop(1, n_gx, step, 0)
        for j in range(1, n_gy):
            visit(gx, lax.rem(gy + j, n_gy))

    barrier = pltpu.get_barrier_semaphore()

    def greet(x, y):
        pl.semaphore_signal(barrier, inc=1, device_id=(x, y), device_id_type=MESH)

    for_others(greet)

    panel = lax.convert_element_type(gx >= half, jnp.int32)
    loads = [
        pltpu.make_async_copy(right_side, r0, load_sem.at[0]),
        pltpu.make_async_copy(precond.at[panel], matrix.at[pl.ds(0, levels)], load_sem.at[1]),
        pltpu.make_async_copy(horizontal, horiz, load_sem.at[2]),
        pltpu.make_async_copy(diagonal, diag, load_sem.at[3]),
        pltpu.make_async_copy(vertical, vert, load_sem.at[4]),
        pltpu.make_async_copy(edge_table, edge_rows, load_sem.at[5]),
        pltpu.make_async_copy(precond.at[1 - panel], matrix.at[pl.ds(levels, levels)], load_sem.at[6]),
    ]
    for load in loads:
        load.start()

    east_x, west_x = lax.rem(gx + 1, n_gx), lax.rem(gx + n_gx - 1, n_gx)
    east_border = (gx == half - 1) | (gx == n_gx - 1)
    west_border = (gx == half) | (gx == 0)
    border = east_border | west_border
    far_x = jnp.where(east_border, east_x, west_x)
    side = jnp.where(east_border, 0, 1)
    table = jnp.where((gx == half - 1) | (gx == half), 0, 1)
    edge_cols = [
        pl.ds(jnp.where(east_border, cols - 1 - i, i), rows, stride=cols) for i in range(3)
    ]
    first_row = pl.multiple_of(gy * rows, rows)
    own = pl.ds(first_row, rows)
    has_north, has_south = gy < n_gy - 1, gy > 0

    @pl.when(jnp.logical_not(has_north))
    def _():
        from_north[...] = jnp.zeros_like(from_north)

    @pl.when(jnp.logical_not(has_south))
    def _():
        from_south[...] = jnp.zeros_like(from_south)

    outside[...] = jnp.zeros_like(outside)

    def split(v):
        high = v.astype(jnp.bfloat16)
        return high, (v - high.astype(jnp.float32)).astype(jnp.bfloat16)

    def prepare_weights():
        for which in range(2):
            for part, value in enumerate(split(matrix[pl.ds(which * levels, levels), :])):
                for twice in range(2):
                    weights[
                        which, pl.ds(part * levels, levels), pl.ds(twice * levels, levels)
                    ] = value

    def precondition(v, which=0):
        out = lax.dot_general(
            jnp.concatenate(split(v), 1),
            weights[which],
            (((1,), (1,)), ((), ())),
            preferred_element_type=jnp.float32,
        )
        return out[:, :levels] + out[:, levels:]

    def col_copy(t, side):
        buffer, recv, x = (
            (from_west, west_recv, east_x) if side == 0 else (from_east, east_recv, west_x)
        )
        return pltpu.make_async_remote_copy(
            src_ref=frame_z.at[t, pl.ds(side * rows, rows)],
            dst_ref=buffer.at[t],
            send_sem=col_send.at[t, side],
            recv_sem=recv.at[t],
            device_id=(x, gy),
            device_id_type=MESH,
        )

    def far_copy(t, g):
        return pltpu.make_async_remote_copy(
            src_ref=pack.at[pl.ds(0, 4)] if t == 0 else pack.at[5],
            dst_ref=far_pack.at[:, own] if t == 0 else far_last.at[own],
            send_sem=far_send.at[t],
            recv_sem=far_recv.at[t],
            device_id=(far_x, g),
            device_id_type=MESH,
        )

    def relay_copy(g):
        return pltpu.make_async_remote_copy(
            src_ref=far_pack.at[:, own],
            dst_ref=far_pack.at[:, own],
            send_sem=relay_send,
            recv_sem=relay_recv,
            device_id=(gx, g),
            device_id_type=MESH,
        )

    def near_copy(g):
        return pltpu.make_async_remote_copy(
            src_ref=pack.at[pl.ds(0, 5)],
            dst_ref=near_pack.at[:, own],
            send_sem=near_send,
            recv_sem=near_recv,
            device_id=(gx, g),
            device_id_type=MESH,
        )

    def mini_copy(side):
        return pltpu.make_async_remote_copy(
            src_ref=mini_out.at[side],
            dst_ref=mini_in.at[side],
            send_sem=mini_send.at[side],
            recv_sem=mini_recv.at[side],
            device_id=(gx, gy + 1 if side == 0 else gy - 1),
            device_id_type=MESH,
        )

    def row_copy(t, side):
        buffer, recv, y, row = (
            (from_south, south_recv, gy + 1, 2 * rows + cols)
            if side == 0
            else (from_north, north_recv, gy - 1, 2 * rows)
        )
        return pltpu.make_async_remote_copy(
            src_ref=frame_z.at[t, pl.ds(row, cols)],
            dst_ref=buffer.at[t],
            send_sem=row_send.at[t, side],
            recv_sem=recv.at[t],
            device_id=(gx, y),
            device_id_type=MESH,
        )

    def for_rows(visit):
        @pl.when(has_north)
        def _():
            visit(0)

        @pl.when(has_south)
        def _():
            visit(1)

    def fill_packs():
        c0, c1, c2 = edge_cols
        inward = 2 * (rows + cols)
        items = [
            frame_z[0, pl.ds(side * rows, rows), :],
            frame_z[0, pl.ds(inward, rows), :],
            horiz[c0, :],
            diag[c0, :],
            horiz[c1, :],
        ]
        for k, item in enumerate(items):
            pack[k] = item
            near_pack[k, own, :] = item
            if k < 4:
                wide[k] = jnp.zeros_like(wide[k])
                wide[k, pl.ds(8, rows), :] = item
        for to, first, second in ((0, rows - 1, rows - 2), (1, 0, 1)):
            picks = [(0, first), (0, second), (1, first), (2, first), (3, first)]
            for k, (item, row) in enumerate(picks):
                mini_out[to, pl.ds(k, 1), :] = items[item][row : row + 1]
            mini_out[to, pl.ds(5, 3), :] = jnp.zeros((3, levels), jnp.float32)

    def send_frame(t, frame):
        z = precondition(frame)
        frame_z[t, pl.ds(0, z.shape[0]), :] = z
        if t == 0:
            pl.when(border)(fill_packs)
            pl.semaphore_wait(barrier, n_all - 1)

            @pl.when(border)
            def _():
                for_rows(lambda side: mini_copy(side).start())

        @pl.when(jnp.logical_not(east_border))
        def _():
            col_copy(t, 0).start()

        @pl.when(jnp.logical_not(west_border))
        def _():
            col_copy(t, 1).start()

        for_rows(lambda side: row_copy(t, side).start())
        if t == 0:

            @pl.when(border)
            def _():
                far_copy(0, gy).start()
                pl.when(gx == 0)(functools.partial(send_far, 0, 1))
                for j in range(1, n_gy):
                    near_copy(lax.rem(gy + j, n_gy)).start()

    def send_far(t, first=0):
        for j in sorted(range(first, n_gy), key=lambda j: abs(2 * j - n_gy)):
            far_copy(t, lax.rem(gy + j, n_gy)).start()

    def receive_rows(t):
        @pl.when(has_north)
        def _():
            row_copy(t, 1).wait_recv()

        @pl.when(has_south)
        def _():
            row_copy(t, 0).wait_recv()

    def receive_cols(t):
        @pl.when(jnp.logical_not(east_border))
        def _():
            col_copy(t, 1).wait_recv()
            outside[pl.ds(0, rows), :] = from_east[t]

        @pl.when(jnp.logical_not(west_border))
        def _():
            col_copy(t, 0).wait_recv()
            outside[pl.ds(rows, rows), :] = from_west[t]

    col_id = lax.rem(lax.broadcasted_iota(jnp.int32, (cells, levels), 0), cols)
    east_edge = pl.ds(cols - 1, rows, stride=cols)
    west_edge = pl.ds(0, rows, stride=cols)
    south_edge = pl.ds(0, cols)
    north_edge = pl.ds(cells - cols, cols)

    def edge_columns(ref):
        return jnp.concatenate([ref[east_edge, :], ref[west_edge, :]], 0)

    def column_part(z):
        lane = lax.broadcasted_iota(jnp.int32, z.shape, 1)
        up = jnp.where(lane < levels - 1, pltpu.roll(z, levels - 1, 1), 0.0)
        down = jnp.where(lane > 0, pltpu.roll(z, 1, 1), 0.0)
        return vert[...] * (2.0 * z - (up + down))

    def inner_image(z):
        east = jnp.where(col_id < cols - 1, pltpu.roll(z, cells - 1, 0), 0.0)
        west = jnp.where(col_id > 0, pltpu.roll(z, 1, 0), 0.0)
        none = jnp.zeros((cols, levels), jnp.float32)
        north = jnp.concatenate([z[cols:], none], 0)
        south = jnp.concatenate([none, z[:-cols]], 0)
        beside = east + west + north + south
        return diag[...] * z + horiz[...] * (4.0 * z - beside) + column_part(z)

    def product(a, b):
        both = (a * b).reshape(-1, 8, levels)
        return jnp.sum(jnp.sum(both, axis=0), axis=0, keepdims=True)

    tall_id = lax.broadcasted_iota(jnp.int32, (tall, levels), 0)

    def along(w):
        north = jnp.where(tall_id < tall - 1, pltpu.roll(w, tall - 1, 0), 0.0)
        south = jnp.where(tall_id > 0, pltpu.roll(w, 1, 0), 0.0)
        return north + south

    def stencil(w, d, h):
        return d * w + h * (4.0 * w - along(w)) + column_part(w)

    def gather_rows(start, count, pairs):
        def one(y):
            row = edge_rows[table, start + y]
            for dst, src in pairs:
                gathered[dst, pl.ds(y, 1), :] = src[pl.ds(row, 1), :]

        if count <= 64:
            for y in range(count):
                one(y)
        else:

            def body(y, carry):
                one(y)
                return carry

            lax.fori_loop(0, count, body, 0)

    def wait_bytes(ref, sem):
        pltpu.make_async_copy(ref, ref, sem).wait()

    near_rest = pl.ds(0, (n_gy - 1) * rows)
    last = gx == n_gx - 1
    relays = border & jnp.logical_not(last)

    def relay():
        wait_bytes(far_pack.at[:, own], far_recv.at[0])
        for j in sorted(range(1, n_gy), key=lambda j: abs(2 * j - n_gy)):
            relay_copy(lax.rem(gy + j, n_gy)).start()


    def look_ahead():
        c1 = edge_cols[1]
        inner = pl.ds(8, rows)

        def take(side, near, far):
            mini_copy(side).wait_recv()
            wide[0, pl.ds(near, 1), :] = mini_in[side, pl.ds(0, 1), :]
            wide[0, pl.ds(far, 1), :] = mini_in[side, pl.ds(1, 1), :]
            for k in (1, 2, 3):
                wide[k, pl.ds(near, 1), :] = mini_in[side, pl.ds(k + 1, 1), :]

        pl.when(border & has_south)(functools.partial(take, 0, 7, 6))
        pl.when(border & has_north)(functools.partial(take, 1, 8 + rows, 9 + rows))

        def next_to(w):
            return pltpu.roll(w, w.shape[0] - 1, 0) + pltpu.roll(w, 1, 0)

        z_edge, z_next, h_edge, d_edge = wide[0], wide[1], wide[2], wide[3]
        v_edge = (
            d_edge * z_edge
            + h_edge * (4.0 * z_edge - z_next - next_to(z_edge))
            + column_part(z_edge)
        )
        beside = next_to(z_next)[8 : 8 + rows] + z_edge[8 : 8 + rows]
        z1 = z_next[8 : 8 + rows]
        z2 = frame_z[0, pl.ds(2 * (rows + cols) + rows, rows), :]
        v_next = (
            diag[c1, :] * z1 + horiz[c1, :] * (4.0 * z1 - beside - z2) + column_part(z1)
        )
        z = precondition(jnp.concatenate([v_edge, v_next], 0))
        z_edge, z_next = z[: rows + 16], z[rows + 16 :]
        beside = next_to(z_edge)[8 : 8 + rows] + z_next
        z_edge = z_edge[8 : 8 + rows]
        h_own, d_own = h_edge[8 : 8 + rows], d_edge[8 : 8 + rows]
        v = d_own * z_edge + h_own * (4.0 * z_edge - beside) + column_part(z_edge)
        pack[5] = precondition(v)
        pl.when(border)(functools.partial(send_far, 1))

    def correct_early():
        @pl.when(border)
        def _():
            pl.when(last)(lambda: wait_bytes(far_pack, far_recv.at[0]))
            pl.when(relays)(lambda: wait_bytes(far_pack.at[:, near_rest], relay_recv))
            wait_bytes(near_pack.at[:, near_rest], near_recv)

        gather_rows(0, tall, [(0, far_pack.at[0]), (1, near_pack.at[0])])
        h_near, d_near = near_pack[2], near_pack[3]
        h_far, d_far = far_pack[2], far_pack[3]
        b_near, b_far = -(h_near * gathered[0]), -(h_far * gathered[1])
        v_near = stencil(near_pack[0], d_near, h_near) - h_near * near_pack[1] + b_near
        v_far = stencil(far_pack[0], d_far, h_far) - h_far * far_pack[1] + b_far
        near = precondition(jnp.concatenate([b_near, v_near], 0))
        far = precondition(jnp.concatenate([b_far, v_far], 0), 1)
        w_near, w_far = near[:tall], far[:tall]
        strip[0] = b_near
        strip[1] = w_near
        strip[3] = far[tall:]
        strip[4] = near[tall:]
        gather_rows(0, tall, [(0, strip.at[3]), (1, strip.at[4])])
        b_near = stencil(w_near, d_near, h_near) - h_near * gathered[0]
        b_far = stencil(w_far, d_far, h_far) - h_far * gathered[1]
        b_next = -(near_pack[4] * w_near)
        near = precondition(jnp.concatenate([b_near, b_next], 0))
        w_edge, w_next = near[:tall], near[tall:]
        strip[3] = b_near
        strip[4] = b_next
        strip[5] = precondition(b_far, 1)
        strip[6] = w_edge
        strip[7] = w_next
        strip[8] = along(w_next)
        strip[9] = stencil(w_edge, d_near, h_near) - h_near * w_next

    def correct_third():
        c0, c1, c2 = edge_cols
        w_edge, w_next, beside = strip[6, own, :], strip[7, own, :], strip[8, own, :]
        h1 = horiz[c1, :]
        later = diag[c1, :] * w_next + h1 * (4.0 * w_next - beside - w_edge) + column_part(w_next)
        b_third = -(horiz[c2, :] * w_next)
        gather_rows(first_row, rows, [(2, strip.at[5])])
        wait_bytes(far_last, far_recv.at[1])
        gather_rows(first_row, rows, [(3, far_last)])
        across = gathered[2, pl.ds(0, rows), :] + gathered[3, pl.ds(0, rows), :]
        b_edge = strip[9, own, :] - horiz[c0, :] * across
        none = jnp.zeros((rows, levels), jnp.float32)
        changes = [
            [strip[0, own, :], none, none],
            [strip[3, own, :], strip[4, own, :], none],
            [b_edge, later, b_third],
        ]
        before = [jnp.concatenate([r0[c, :] for c in edge_cols], 0)]
        after = [before[0]]
        for t in range(ITERS):
            old = jnp.concatenate([images[t, c, :] for c in edge_cols], 0)
            new = old + jnp.concatenate(changes[t], 0)
            before.append(old)
            after.append(new)
            for k in range(t + 1):
                images[t, edge_cols[k], :] = new[k * rows : (k + 1) * rows]
        for k, (i, j) in enumerate(KEYS):
            if j > 0:
                partial[pl.ds(k, 1), :] += product(after[i], after[j]) - product(before[i], before[j])

    for load in loads:
        load.wait()
    prepare_weights()
    terms = {}
    spaces = [r0]
    frame = [edge_columns(r0), r0[south_edge, :], r0[north_edge, :]]
    send_frame(0, jnp.concatenate(frame + [r0[c, :] for c in edge_cols[1:]], 0))
    edge_horiz = edge_columns(horiz)
    for t in range(ITERS):
        image = images.at[t]
        z = precondition(spaces[-1][...])
        fields[t] = z
        newest = len(spaces) - 1
        for i in range(len(spaces)):
            terms[(i, newest)] = product(spaces[i][...], spaces[newest][...])
        image[...] = inner_image(z)
        if t == 0:
            look_ahead()
        if t == 1:
            pl.when(relays)(relay)
        if t == ITERS - 1:
            correct_early()
        receive_rows(t)
        image[south_edge, :] = image[south_edge, :] - horiz[south_edge, :] * from_south[t]
        image[north_edge, :] = image[north_edge, :] - horiz[north_edge, :] * from_north[t]
        inside = edge_columns(image)
        receive_cols(t)
        edges = inside - edge_horiz * outside[...]
        image[east_edge, :] = edges[:rows]
        image[west_edge, :] = edges[rows:]
        if t < ITERS - 1:
            frame = [edges, image[south_edge, :], image[north_edge, :]]
            send_frame(t + 1, jnp.concatenate(frame, 0))
        spaces.append(image)
    newest = len(spaces) - 1
    for i in range(len(spaces)):
        terms[(i, newest)] = product(spaces[i][...], spaces[newest][...])
    for k, key in enumerate(KEYS):
        partial[pl.ds(k, 1), :] = terms[key]

    @pl.when(border)
    def _():
        correct_third()

    height = -(-len(KEYS) // 8) * 8
    row_id = lax.broadcasted_iota(jnp.int32, (height, levels), 0)
    lane = lax.broadcasted_iota(jnp.int32, (height, levels), 1)
    stacked = jnp.where(row_id < len(KEYS), partial[...], 0.0)
    summed = jnp.sum(stacked, axis=1, keepdims=True)
    sums[me] = jnp.sum(jnp.where(lane == row_id, summed, 0.0), axis=0, keepdims=True)

    def tell(x, y):
        pltpu.make_async_remote_copy(
            src_ref=sums.at[me],
            dst_ref=sums.at[me],
            send_sem=sum_send,
            recv_sem=sum_recv,
            device_id=(x, y),
            device_id_type=MESH,
        ).start()

    for_others(tell)
    for t in range(ITERS):

        @pl.when(jnp.logical_not(east_border))
        def _(t=t):
            col_copy(t, 0).wait_send()

        @pl.when(jnp.logical_not(west_border))
        def _(t=t):
            col_copy(t, 1).wait_send()

        @pl.when(has_north)
        def _(t=t):
            row_copy(t, 0).wait_send()

        @pl.when(has_south)
        def _(t=t):
            row_copy(t, 1).wait_send()

    @pl.when(border)
    def _():
        wait_bytes(far_pack.at[:, own], far_send.at[0])
        pl.when(gx == 0)(lambda: wait_bytes(far_pack.at[:, near_rest], far_send.at[0]))
        pl.when(relays)(lambda: wait_bytes(far_pack.at[:, near_rest], relay_send))
        wait_bytes(far_last, far_send.at[1])
        wait_bytes(near_pack.at[:, near_rest], near_send)
        for_rows(lambda side: mini_copy(side).wait_send())
        c0, c1, c2 = edge_cols
        fields[1, c0, :] += strip[1, own, :]
        fields[2, c0, :] += strip[6, own, :]
        fields[2, c1, :] += strip[7, own, :]

    others = sums.at[pl.ds(0, n_all - 1)]
    wait_bytes(others, sum_recv)
    out_totals[...] = jnp.sum(sums[...], axis=0)
    wait_bytes(others, sum_send)


def finish(
    total_cells, all_totals, r0, fields, images, out_x, out_r, out_norms, x, r, norms_out, sem, norm_sem
):
    levels = r0.shape[-1]
    totals = all_totals[...]
    value = {
        key: jnp.broadcast_to(totals[:, k : k + 1], (8, levels)) for k, key in enumerate(KEYS)
    }

    rho, g0, g1, g2 = value[(0, 0)], value[(0, 1)], value[(0, 2)], value[(0, 3)]
    a00, a01, a02 = value[(1, 1)], value[(1, 2)], value[(1, 3)]
    a11, a12, a22 = value[(2, 2)], value[(2, 3)], value[(3, 3)]
    l10, l20, y0 = a01 / a00, a02 / a00, g0 / a00
    d1, e12, f1 = a11 - l10 * a01, a12 - l10 * a02, g1 - l10 * g0
    l21, y1 = e12 / d1, f1 / d1
    d2, f2 = a22 - l20 * a02 - l21 * e12, g2 - l20 * g0 - l21 * f1
    y2 = f2 / d2
    norm0 = rho - y0 * g0
    norm1 = norm0 - y1 * f1
    norm2 = norm1 - y2 * f2
    y1 = y1 - l21 * y2
    y0 = y0 - l10 * y1 - l20 * y2
    norm_lane = lax.broadcasted_iota(jnp.int32, (8, levels), 1)
    norms = jnp.where(norm_lane == 0, norm0, jnp.where(norm_lane == 1, norm1, norm2))
    norms_out[...] = norms[:1, :ITERS] / total_cells
    copies = [pltpu.make_async_copy(norms_out, out_norms, norm_sem)]
    copies[0].start()
    rows = r0.shape[0]
    pieces = 2 if rows % 16 == 0 else 1
    size = rows // pieces
    y0, y1, y2 = (jnp.tile(y, (size // 8, 1)) for y in (y0, y1, y2))
    for p in range(pieces):
        span = pl.ds(p * size, size)
        x[span] = y0 * fields[0, span] + y1 * fields[1, span] + y2 * fields[2, span]
        r[span] = (
            r0[span] - y0 * images[0, span] - y1 * images[1, span] - y2 * images[2, span]
        )
        for k, (src, dst) in enumerate(((x, out_x), (r, out_r))):
            copy = pltpu.make_async_copy(src.at[span], dst.at[span], sem.at[p, k])
            copy.start()
            copies.append(copy)
    for copy in copies:
        copy.wait()


def on_device(n_gx, n_gy, right_side, diagonal, horizontal, vertical, precond, edge_rows):
    rows, cols, levels = right_side.shape
    f32 = jnp.float32
    block = (rows * cols, levels)
    column = (n_gy * rows, levels)
    sems = pltpu.SemaphoreType.DMA
    basis = pltpu.VMEM((ITERS,) + block, f32)
    fields, images, totals, start = pl.pallas_call(
        functools.partial(kernel, n_gx, n_gy, rows),
        out_shape=(basis, basis, pltpu.VMEM((1, levels), f32), pltpu.VMEM(block, f32)),
        in_specs=[ANY, ANY, ANY, ANY, ANY, ANY],
        out_specs=(VMEM, VMEM, VMEM, VMEM),
        scratch_shapes=[
            pltpu.VMEM(block, f32),
            pltpu.VMEM(block, f32),
            pltpu.VMEM((1, levels), f32),
            pltpu.VMEM((2 * levels, levels), f32),
            pltpu.VMEM((2, 2 * levels, 2 * levels), jnp.bfloat16),
            pltpu.VMEM((ITERS, 4 * rows + 2 * cols, levels), f32),
            pltpu.VMEM((6, rows, levels), f32),
            pltpu.VMEM((2, 8, levels), f32),
            pltpu.VMEM((2, 8, levels), f32),
            pltpu.VMEM((4, rows + 16, levels), f32),
            pltpu.VMEM((ITERS, rows, levels), f32),
            pltpu.VMEM((ITERS, rows, levels), f32),
            pltpu.VMEM((ITERS, cols, levels), f32),
            pltpu.VMEM((ITERS, cols, levels), f32),
            pltpu.VMEM((4,) + column, f32),
            pltpu.VMEM((5,) + column, f32),
            pltpu.VMEM(column, f32),
            pltpu.VMEM((4,) + column, f32),
            pltpu.VMEM((10,) + column, f32),
            pltpu.VMEM((2 * rows, levels), f32),
            pltpu.VMEM((16, levels), f32),
            pltpu.VMEM((n_gx * n_gy, 1, levels), f32),
            pltpu.SMEM(edge_rows.shape, jnp.int32),
            sems((7,)),
            sems((ITERS, 2)),
            sems((ITERS,)),
            sems((ITERS,)),
            sems((2,)),
            sems((2,)),
            sems(()),
            sems(()),
            sems(()),
            sems(()),
            sems((2,)),
            sems((2,)),
            sems((ITERS, 2)),
            sems((ITERS,)),
            sems((ITERS,)),
            sems(()),
            sems(()),
        ],
        compiler_params=pltpu.CompilerParams(collective_id=0, has_side_effects=True),
    )(
        edge_rows,
        right_side.reshape(block),
        diagonal.reshape(block),
        horizontal.reshape(block),
        vertical.reshape(1, levels),
        precond,
    )
    in_vmem = functools.partial(
        pltpu.with_memory_space_constraint, memory_space=pltpu.VMEM
    )
    total_cells = float(rows * cols * levels * n_gx * n_gy)
    x, r, norms = pl.pallas_call(
        functools.partial(finish, total_cells),
        out_shape=(
            jax.ShapeDtypeStruct(block, f32),
            jax.ShapeDtypeStruct(block, f32),
            jax.ShapeDtypeStruct((1, ITERS), f32),
        ),
        in_specs=[VMEM, VMEM, VMEM, VMEM],
        out_specs=(ANY, ANY, ANY),
        scratch_shapes=[
            pltpu.VMEM(block, f32),
            pltpu.VMEM(block, f32),
            pltpu.VMEM((1, ITERS), f32),
            sems((2, 2)),
            sems(()),
        ],
    )(in_vmem(totals), in_vmem(start), in_vmem(fields), in_vmem(images))
    shape = right_side.shape
    return x.reshape(shape), r.reshape(shape), norms.reshape(ITERS)


def solution(mesh):
    n_gx, n_gy = mesh.shape["gx"], mesh.shape["gy"]
    field = P("gy", "gx", None)
    return jax.shard_map(
        functools.partial(on_device, n_gx, n_gy),
        mesh=mesh,
        in_specs=(field, field, field, P(), P(), P()),
        out_specs=(field, field, P()),
        check_vma=False,
    )
```

```python
import functools

import jax
import jax.numpy as jnp
from jax import lax
from jax.experimental import pallas as pl
from jax.experimental.pallas import tpu as pltpu
from jax.sharding import PartitionSpec as P

ITERS = 3
KEYS = [(i, j) for j in range(ITERS + 1) for i in range(j + 1)]
MESH = pl.DeviceIdType.MESH
ANY = pl.BlockSpec(memory_space=pl.ANY)
VMEM = pl.BlockSpec(memory_space=pltpu.VMEM)


def kernel(
    n_gx,
    n_gy,
    out_rows,
    edge_table,
    right_side,
    diagonal,
    horizontal,
    vertical,
    precond,
    fields,
    images,
    out_totals,
    r0,
    diag,
    horiz,
    vert,
    matrix,
    weights,
    frame_z,
    pack,
    mini_out,
    mini_in,
    wide,
    edge_out,
    edge_in,
    corner_out,
    corner_in,
    beyond,
    from_east,
    from_west,
    from_north,
    from_south,
    far_pack,
    near_pack,
    far_last,
    gathered,
    strip,
    strip_out,
    outside,
    partial,
    sums,
    edge_rows,
    load_sem,
    col_send,
    east_recv,
    west_recv,
    far_send,
    far_recv,
    relay_send,
    relay_recv,
    near_send,
    near_recv,
    mini_send,
    mini_recv,
    edge_send,
    edge_recv,
    corner_send,
    corner_recv,
    row_send,
    north_recv,
    south_recv,
    sum_send,
    sum_recv,
):
    rows, levels = out_rows, r0.shape[-1]
    cells = r0.shape[0]
    cols = cells // rows
    tall = n_gy * rows
    gx, gy = lax.axis_index("gx"), lax.axis_index("gy")
    n_all = n_gx * n_gy
    half = n_gx // 2
    me = gx * n_gy + gy

    def for_others(visit):
        def step(i, carry):
            for j in range(n_gy):
                visit(lax.rem(gx + i, n_gx), lax.rem(gy + j, n_gy))
            return carry

        if n_all <= 64:
            for i in sorted(range(1, n_gx), key=lambda i: min(i, n_gx - i)):
                step(i, 0)
        else:
            lax.fori_loop(1, n_gx, step, 0)
        for j in range(1, n_gy):
            visit(gx, lax.rem(gy + j, n_gy))

    barrier = pltpu.get_barrier_semaphore()

    def greet(x, y):
        pl.semaphore_signal(barrier, inc=1, device_id=(x, y), device_id_type=MESH)

    for_others(greet)

    panel = lax.convert_element_type(gx >= half, jnp.int32)
    loads = [
        pltpu.make_async_copy(right_side, r0, load_sem.at[0]),
        pltpu.make_async_copy(precond.at[panel], matrix.at[pl.ds(0, levels)], load_sem.at[1]),
        pltpu.make_async_copy(horizontal, horiz, load_sem.at[2]),
        pltpu.make_async_copy(diagonal, diag, load_sem.at[3]),
        pltpu.make_async_copy(vertical, vert, load_sem.at[4]),
        pltpu.make_async_copy(edge_table, edge_rows, load_sem.at[5]),
        pltpu.make_async_copy(precond.at[1 - panel], matrix.at[pl.ds(levels, levels)], load_sem.at[6]),
    ]
    for load in loads:
        load.start()

    east_x, west_x = lax.rem(gx + 1, n_gx), lax.rem(gx + n_gx - 1, n_gx)
    east_border = (gx == half - 1) | (gx == n_gx - 1)
    west_border = (gx == half) | (gx == 0)
    border = east_border | west_border
    far_x = jnp.where(east_border, east_x, west_x)
    side = jnp.where(east_border, 0, 1)
    table = jnp.where((gx == half - 1) | (gx == half), 0, 1)
    edge_cols = [
        pl.ds(jnp.where(east_border, cols - 1 - i, i), rows, stride=cols) for i in range(3)
    ]
    first_row = pl.multiple_of(gy * rows, rows)
    own = pl.ds(first_row, rows)
    has_north, has_south = gy < n_gy - 1, gy > 0

    @pl.when(jnp.logical_not(has_north))
    def _():
        from_north[...] = jnp.zeros_like(from_north)

    @pl.when(jnp.logical_not(has_south))
    def _():
        from_south[...] = jnp.zeros_like(from_south)

    outside[...] = jnp.zeros_like(outside)

    def split(v):
        high = v.astype(jnp.bfloat16)
        return high, (v - high.astype(jnp.float32)).astype(jnp.bfloat16)

    def prepare_weights():
        for which in range(2):
            for part, value in enumerate(split(matrix[pl.ds(which * levels, levels), :])):
                for twice in range(2):
                    weights[
                        which, pl.ds(part * levels, levels), pl.ds(twice * levels, levels)
                    ] = value

    def precondition(v, which=0):
        out = lax.dot_general(
            jnp.concatenate(split(v), 1),
            weights[which],
            (((1,), (1,)), ((), ())),
            preferred_element_type=jnp.float32,
        )
        return out[:, :levels] + out[:, levels:]

    def col_copy(t, side):
        buffer, recv, x = (
            (from_west, west_recv, east_x) if side == 0 else (from_east, east_recv, west_x)
        )
        return pltpu.make_async_remote_copy(
            src_ref=frame_z.at[t, pl.ds(side * rows, rows)],
            dst_ref=buffer.at[t],
            send_sem=col_send.at[t, side],
            recv_sem=recv.at[t],
            device_id=(x, gy),
            device_id_type=MESH,
        )

    def far_copy(t, g):
        return pltpu.make_async_remote_copy(
            src_ref=pack.at[pl.ds(0, 4)] if t == 0 else pack.at[5],
            dst_ref=far_pack.at[:, own] if t == 0 else far_last.at[own],
            send_sem=far_send.at[t],
            recv_sem=far_recv.at[t],
            device_id=(far_x, g),
            device_id_type=MESH,
        )

    def relay_copy(g, block):
        return pltpu.make_async_remote_copy(
            src_ref=far_pack.at[:, block],
            dst_ref=far_pack.at[:, block],
            send_sem=relay_send,
            recv_sem=relay_recv,
            device_id=(gx, g),
            device_id_type=MESH,
        )

    def near_copy(g):
        return pltpu.make_async_remote_copy(
            src_ref=pack.at[pl.ds(0, 5)],
            dst_ref=near_pack.at[:, own],
            send_sem=near_send,
            recv_sem=near_recv,
            device_id=(gx, g),
            device_id_type=MESH,
        )

    def mini_copy(side):
        return pltpu.make_async_remote_copy(
            src_ref=mini_out.at[side],
            dst_ref=mini_in.at[side],
            send_sem=mini_send.at[side],
            recv_sem=mini_recv.at[side],
            device_id=(gx, gy + 1 if side == 0 else gy - 1),
            device_id_type=MESH,
        )

    def row_copy(t, side):
        buffer, recv, y, row = (
            (from_south, south_recv, gy + 1, 2 * rows + cols)
            if side == 0
            else (from_north, north_recv, gy - 1, 2 * rows)
        )
        return pltpu.make_async_remote_copy(
            src_ref=frame_z.at[t, pl.ds(row, cols)],
            dst_ref=buffer.at[t],
            send_sem=row_send.at[t, side],
            recv_sem=recv.at[t],
            device_id=(gx, y),
            device_id_type=MESH,
        )

    def edge_copy(side):
        return pltpu.make_async_remote_copy(
            src_ref=edge_out.at[side],
            dst_ref=edge_in.at[1 - side],
            send_sem=edge_send.at[side],
            recv_sem=edge_recv.at[1 - side],
            device_id=(east_x if side == 0 else west_x, gy),
            device_id_type=MESH,
        )

    def corner_copy(k):
        return pltpu.make_async_remote_copy(
            src_ref=corner_out.at[k],
            dst_ref=corner_in.at[k],
            send_sem=corner_send.at[k],
            recv_sem=corner_recv.at[k],
            device_id=(west_x if k < 2 else east_x, gy + 1 if k % 2 == 0 else gy - 1),
            device_id_type=MESH,
        )

    def for_sides(visit):
        pl.when(jnp.logical_not(east_border))(functools.partial(visit, 0))
        pl.when(jnp.logical_not(west_border))(functools.partial(visit, 1))

    def for_corners(visit, sending):
        for k in range(4):
            east = (k < 2) != sending
            north = (k % 2 == 0) == sending
            condition = jnp.logical_not(east_border if east else west_border)
            pl.when(condition & (has_north if north else has_south))(functools.partial(visit, k))

    def for_rows(visit):
        @pl.when(has_north)
        def _():
            visit(0)

        @pl.when(has_south)
        def _():
            visit(1)

    inward = 2 * (rows + cols)
    mid = pl.ds(8, rows)

    def side_cols(side, k):
        return pl.ds(k if side else cols - 1 - k, rows, stride=cols)

    def fill_edges():
        for side in range(2):
            items = [
                frame_z[0, pl.ds(side * rows, rows), :],
                frame_z[0, pl.ds(inward + side * rows, rows), :],
                horiz[side_cols(side, 0), :],
                diag[side_cols(side, 0), :],
            ]
            for k, item in enumerate(items):
                wide[side, k] = jnp.zeros_like(wide[side, k])
                wide[side, k, mid, :] = item
                if k:
                    edge_out[side, k - 1] = item
            for to, first, second in ((0, rows - 1, rows - 2), (1, 0, 1)):
                picks = [(0, first), (0, second), (1, first), (2, first), (3, first)]
                for k, (item, row) in enumerate(picks):
                    mini_out[to, pl.ds(8 * side + k, 1), :] = items[item][row : row + 1]
                mini_out[to, pl.ds(8 * side + 5, 3), :] = jnp.zeros((3, levels), jnp.float32)
                corner_out[2 * (1 - side) + to] = jnp.zeros((8, levels), jnp.float32)
                corner_out[2 * (1 - side) + to, pl.ds(0, 1), :] = items[0][first : first + 1]
        beyond[...] = jnp.zeros_like(beyond)

    def fill_packs():
        c0, c1, c2 = edge_cols
        items = [
            frame_z[0, pl.ds(side * rows, rows), :],
            frame_z[0, pl.ds(inward + side * rows, rows), :],
            horiz[c0, :],
            diag[c0, :],
            horiz[c1, :],
        ]
        for k, item in enumerate(items):
            pack[k] = item
            near_pack[k, own, :] = item

    def send_first(frame):
        frame_z[0] = precondition(frame)
        fill_edges()
        pl.when(border)(fill_packs)
        pl.semaphore_wait(barrier, n_all - 1)

        @pl.when(gx == 0)
        def _():
            for j in range(0, n_gy, 2):
                far_copy(0, lax.rem(gy + j, n_gy)).start()

        for_sides(lambda side: col_copy(0, side).start())
        for_rows(lambda side: mini_copy(side).start())
        for_rows(lambda side: row_copy(0, side).start())
        for_corners(lambda k: corner_copy(k).start(), True)
        for_sides(lambda side: edge_copy(side).start())

        @pl.when(border)
        def _():
            pl.when(gx > 0)(lambda: far_copy(0, gy).start())
            for j in range(1, n_gy):
                near_copy(lax.rem(gy + j, n_gy)).start()

    def send_rows(t, frame):
        frame_z[t, pl.ds(2 * rows, 2 * cols), :] = precondition(frame)
        for_rows(lambda side: row_copy(t, side).start())

    def send_far_last():
        for j in sorted(range(n_gy), key=lambda j: abs(2 * j - n_gy)):
            far_copy(1, lax.rem(gy + j, n_gy)).start()

    def receive_rows(t):
        @pl.when(has_north)
        def _():
            row_copy(t, 1).wait_recv()

        @pl.when(has_south)
        def _():
            row_copy(t, 0).wait_recv()

    def receive_cols(t):
        def take(side):
            buffer = from_west if side else from_east
            col_copy(t, 1 - side).wait_recv()
            outside[pl.ds(side * rows, rows), :] = buffer[t]
            if t == 0:
                beyond[side, mid, :] = buffer[t]

        for_sides(take)

    col_id = lax.rem(lax.broadcasted_iota(jnp.int32, (cells, levels), 0), cols)
    east_edge = pl.ds(cols - 1, rows, stride=cols)
    west_edge = pl.ds(0, rows, stride=cols)
    south_edge = pl.ds(0, cols)
    north_edge = pl.ds(cells - cols, cols)

    def edge_columns(ref):
        return jnp.concatenate([ref[east_edge, :], ref[west_edge, :]], 0)

    def column_part(z):
        lane = lax.broadcasted_iota(jnp.int32, z.shape, 1)
        up = jnp.where(lane < levels - 1, pltpu.roll(z, levels - 1, 1), 0.0)
        down = jnp.where(lane > 0, pltpu.roll(z, 1, 1), 0.0)
        return vert[...] * (2.0 * z - (up + down))

    def inner_image(z):
        east = jnp.where(col_id < cols - 1, pltpu.roll(z, cells - 1, 0), 0.0)
        west = jnp.where(col_id > 0, pltpu.roll(z, 1, 0), 0.0)
        none = jnp.zeros((cols, levels), jnp.float32)
        north = jnp.concatenate([z[cols:], none], 0)
        south = jnp.concatenate([none, z[:-cols]], 0)
        beside = east + west + north + south
        return diag[...] * z + horiz[...] * (4.0 * z - beside) + column_part(z)

    def product(a, b):
        both = (a * b).reshape(-1, 8, levels)
        return jnp.sum(jnp.sum(both, axis=0), axis=0, keepdims=True)

    tall_id = lax.broadcasted_iota(jnp.int32, (tall, levels), 0)

    def along(w):
        north = jnp.where(tall_id < tall - 1, pltpu.roll(w, tall - 1, 0), 0.0)
        south = jnp.where(tall_id > 0, pltpu.roll(w, 1, 0), 0.0)
        return north + south

    def stencil(w, d, h):
        return d * w + h * (4.0 * w - along(w)) + column_part(w)

    def gather_rows(start, count, pairs):
        def one(y):
            row = edge_rows[table, start + y]
            for dst, src in pairs:
                gathered[dst, pl.ds(y, 1), :] = src[pl.ds(row, 1), :]

        if count <= 64:
            for y in range(count):
                one(y)
        else:

            def body(y, carry):
                one(y)
                return carry

            lax.fori_loop(0, count, body, 0)

    def wait_bytes(ref, sem):
        pltpu.make_async_copy(ref, ref, sem).wait()

    near_rest = pl.ds(0, (n_gy - 1) * rows)
    last = gx == n_gx - 1
    relays = border & jnp.logical_not(last)
    alike = pl.ds(0, n_gy // 2 * rows)

    def relay_across():
        wait_bytes(far_pack.at[:, alike], far_recv.at[0])
        for k in range(n_gy // 2):
            g = lax.rem(gy, 2) + 2 * k
            block = pl.ds(pl.multiple_of(g * rows, rows), rows)
            relay_copy(gy + 1 - 2 * lax.rem(gy, 2), block).start()

    def relay():
        wait_bytes(far_pack.at[:, own], far_recv.at[0])
        for j in sorted(range(1, n_gy), key=lambda j: abs(2 * j - n_gy)):
            relay_copy(lax.rem(gy + j, n_gy), own).start()


    def next_to(w):
        return pltpu.roll(w, w.shape[0] - 1, 0) + pltpu.roll(w, 1, 0)

    def strip_image(side, k, z, left, right):
        c = side_cols(side, k)
        return diag[c, :] * z + horiz[c, :] * (4.0 * z - left - right) + column_part(z)

    def look_ahead():
        c1 = edge_cols[1]

        def take(direction, near, far):
            mini_copy(direction).wait_recv()
            for side in range(2):
                row = mini_in.at[direction]
                wide[side, 0, pl.ds(near, 1), :] = row[pl.ds(8 * side, 1), :]
                wide[side, 0, pl.ds(far, 1), :] = row[pl.ds(8 * side + 1, 1), :]
                for k in (1, 2, 3):
                    wide[side, k, pl.ds(near, 1), :] = row[pl.ds(8 * side + k + 1, 1), :]

        pl.when(has_south)(functools.partial(take, 0, 7, 6))
        pl.when(has_north)(functools.partial(take, 1, 8 + rows, 9 + rows))
        z_edge, z_next, h_edge, d_edge = (wide[side, k] for k in range(4))
        v_edge = (
            d_edge * z_edge
            + h_edge * (4.0 * z_edge - z_next - next_to(z_edge))
            + column_part(z_edge)
        )
        beside = next_to(z_next)[8 : 8 + rows] + z_edge[8 : 8 + rows]
        z1 = z_next[8 : 8 + rows]
        z2 = frame_z[0, pl.ds(inward + (2 + side) * rows, rows), :]
        v_next = (
            diag[c1, :] * z1 + horiz[c1, :] * (4.0 * z1 - beside - z2) + column_part(z1)
        )
        z = precondition(jnp.concatenate([v_edge, v_next], 0))
        z_edge, z_next = z[: rows + 16], z[rows + 16 :]
        beside = next_to(z_edge)[8 : 8 + rows] + z_next
        z_edge = z_edge[8 : 8 + rows]
        h_own, d_own = h_edge[8 : 8 + rows], d_edge[8 : 8 + rows]
        v = d_own * z_edge + h_own * (4.0 * z_edge - beside) + column_part(z_edge)
        pack[5] = precondition(v)
        pl.when(border)(send_far_last)

    def look_across():
        for_sides(lambda side: edge_copy(1 - side).wait_recv())

        def take(k):
            corner_copy(k).wait_recv()
            row = 8 + rows if k % 2 else 7
            beyond[k // 2, pl.ds(row, 1), :] = corner_in[k, pl.ds(0, 1), :]

        for_corners(take, False)
        images_first = []
        for side in range(2):
            z_edge, z_next, h_edge, d_edge = (wide[side, k] for k in range(4))
            z_out = beyond[side]
            own_edge, own_out = z_edge[8 : 8 + rows], z_out[8 : 8 + rows]
            v_edge = (
                d_edge * z_edge
                + h_edge * (4.0 * z_edge - z_next - z_out - next_to(z_edge))
                + column_part(z_edge)
            )
            z1 = z_next[8 : 8 + rows]
            z2 = frame_z[0, pl.ds(inward + (2 + side) * rows, rows), :]
            v_next = strip_image(side, 1, z1, next_to(z_next)[8 : 8 + rows] + own_edge, z2)
            v_out = (
                edge_in[side, 2] * own_out
                + edge_in[side, 1]
                * (4.0 * own_out - edge_in[side, 0] - own_edge - next_to(z_out)[8 : 8 + rows])
                + column_part(own_out)
            )
            images_first += [v_edge, v_next, v_out]
        z = precondition(jnp.concatenate(images_first, 0))
        second = []
        each = 3 * rows + 16
        for side in range(2):
            part = z[side * each : (side + 1) * each]
            z_edge, z_next, z_out = part[: rows + 16], part[rows + 16 : each - rows], part[each - rows :]
            strip_out[pl.ds(side * rows, rows), :] = z_out
            beside = next_to(z_edge)[8 : 8 + rows]
            second.append(strip_image(side, 0, z_edge[8 : 8 + rows], beside + z_next, z_out))
        frame_z[2, pl.ds(0, 2 * rows), :] = precondition(jnp.concatenate(second, 0))

        def give(side):
            col_copy(2, side).start()
            outside[pl.ds(side * rows, rows), :] = strip_out[pl.ds(side * rows, rows), :]

        for_sides(give)

    def correct_early():
        @pl.when(border)
        def _():
            pl.when(last)(lambda: wait_bytes(far_pack.at[:, alike], relay_recv))
            pl.when(relays)(lambda: wait_bytes(far_pack.at[:, near_rest], relay_recv))
            wait_bytes(near_pack.at[:, near_rest], near_recv)

        gather_rows(0, tall, [(0, far_pack.at[0]), (1, near_pack.at[0])])
        h_near, d_near = near_pack[2], near_pack[3]
        h_far, d_far = far_pack[2], far_pack[3]
        b_near, b_far = -(h_near * gathered[0]), -(h_far * gathered[1])
        v_near = stencil(near_pack[0], d_near, h_near) - h_near * near_pack[1] + b_near
        v_far = stencil(far_pack[0], d_far, h_far) - h_far * far_pack[1] + b_far
        near = precondition(jnp.concatenate([b_near, v_near], 0))
        far = precondition(jnp.concatenate([b_far, v_far], 0), 1)
        w_near, w_far = near[:tall], far[:tall]
        strip[0] = b_near
        strip[1] = w_near
        strip[3] = far[tall:]
        strip[4] = near[tall:]
        gather_rows(0, tall, [(0, strip.at[3]), (1, strip.at[4])])
        b_near = stencil(w_near, d_near, h_near) - h_near * gathered[0]
        b_far = stencil(w_far, d_far, h_far) - h_far * gathered[1]
        b_next = -(near_pack[4] * w_near)
        near = precondition(jnp.concatenate([b_near, b_next], 0))
        w_edge, w_next = near[:tall], near[tall:]
        strip[3] = b_near
        strip[4] = b_next
        strip[5] = precondition(b_far, 1)
        strip[6] = w_edge
        strip[7] = w_next
        strip[8] = along(w_next)
        strip[9] = stencil(w_edge, d_near, h_near) - h_near * w_next

    def correct_third():
        c0, c1, c2 = edge_cols
        w_edge, w_next, beside = strip[6, own, :], strip[7, own, :], strip[8, own, :]
        h1 = horiz[c1, :]
        later = diag[c1, :] * w_next + h1 * (4.0 * w_next - beside - w_edge) + column_part(w_next)
        b_third = -(horiz[c2, :] * w_next)
        gather_rows(first_row, rows, [(2, strip.at[5])])
        wait_bytes(far_last, far_recv.at[1])
        gather_rows(first_row, rows, [(3, far_last)])
        across = gathered[2, pl.ds(0, rows), :] + gathered[3, pl.ds(0, rows), :]
        b_edge = strip[9, own, :] - horiz[c0, :] * across
        none = jnp.zeros((rows, levels), jnp.float32)
        changes = [
            [strip[0, own, :], none, none],
            [strip[3, own, :], strip[4, own, :], none],
            [b_edge, later, b_third],
        ]
        before = [jnp.concatenate([r0[c, :] for c in edge_cols], 0)]
        after = [before[0]]
        for t in range(ITERS):
            old = jnp.concatenate([images[t, c, :] for c in edge_cols], 0)
            new = old + jnp.concatenate(changes[t], 0)
            before.append(old)
            after.append(new)
            for k in range(t + 1):
                images[t, edge_cols[k], :] = new[k * rows : (k + 1) * rows]
        for k, (i, j) in enumerate(KEYS):
            if j > 0:
                partial[pl.ds(k, 1), :] += product(after[i], after[j]) - product(before[i], before[j])

    for load in loads:
        load.wait()
    prepare_weights()
    terms = {}
    spaces = [r0]
    frame = [edge_columns(r0), r0[south_edge, :], r0[north_edge, :]]
    frame += [r0[side_cols(side, k), :] for k in (1, 2) for side in range(2)]
    send_first(jnp.concatenate(frame, 0))
    edge_horiz = edge_columns(horiz)
    for t in range(ITERS):
        image = images.at[t]
        z = precondition(spaces[-1][...])
        fields[t] = z
        newest = len(spaces) - 1
        for i in range(len(spaces)):
            terms[(i, newest)] = product(spaces[i][...], spaces[newest][...])
        image[...] = inner_image(z)
        if t == 0:
            look_ahead()
        if t == 1:
            pl.when(relays)(relay)
            look_across()
        if t == 2:
            pl.when(last)(relay_across)
            correct_early()
        receive_rows(t)
        image[south_edge, :] = image[south_edge, :] - horiz[south_edge, :] * from_south[t]
        image[north_edge, :] = image[north_edge, :] - horiz[north_edge, :] * from_north[t]
        inside = edge_columns(image)
        if t != 1:
            receive_cols(t)
        edges = inside - edge_horiz * outside[...]
        image[east_edge, :] = edges[:rows]
        image[west_edge, :] = edges[rows:]
        if t < ITERS - 1:
            send_rows(t + 1, jnp.concatenate([image[south_edge, :], image[north_edge, :]], 0))
        spaces.append(image)
    newest = len(spaces) - 1
    for i in range(len(spaces)):
        terms[(i, newest)] = product(spaces[i][...], spaces[newest][...])
    for k, key in enumerate(KEYS):
        partial[pl.ds(k, 1), :] = terms[key]

    @pl.when(border)
    def _():
        correct_third()

    height = -(-len(KEYS) // 8) * 8
    row_id = lax.broadcasted_iota(jnp.int32, (height, levels), 0)
    lane = lax.broadcasted_iota(jnp.int32, (height, levels), 1)
    stacked = jnp.where(row_id < len(KEYS), partial[...], 0.0)
    summed = jnp.sum(stacked, axis=1, keepdims=True)
    sums[me] = jnp.sum(jnp.where(lane == row_id, summed, 0.0), axis=0, keepdims=True)

    def tell(x, y):
        pltpu.make_async_remote_copy(
            src_ref=sums.at[me],
            dst_ref=sums.at[me],
            send_sem=sum_send,
            recv_sem=sum_recv,
            device_id=(x, y),
            device_id_type=MESH,
        ).start()

    for_others(tell)
    for t in range(ITERS):
        if t != 1:
            for_sides(lambda side, t=t: col_copy(t, side).wait_send())

        @pl.when(has_north)
        def _(t=t):
            row_copy(t, 0).wait_send()

        @pl.when(has_south)
        def _(t=t):
            row_copy(t, 1).wait_send()

    for_rows(lambda side: mini_copy(side).wait_send())
    for_sides(lambda side: edge_copy(side).wait_send())
    for_corners(lambda k: corner_copy(k).wait_send(), True)

    @pl.when(border)
    def _():
        pl.when(gx == 0)(lambda: wait_bytes(far_pack.at[:, alike], far_send.at[0]))
        pl.when(gx > 0)(lambda: wait_bytes(far_pack.at[:, own], far_send.at[0]))
        pl.when(relays)(lambda: wait_bytes(far_pack.at[:, near_rest], relay_send))
        pl.when(last)(lambda: wait_bytes(far_pack.at[:, alike], relay_send))
        wait_bytes(far_last, far_send.at[1])
        wait_bytes(near_pack.at[:, near_rest], near_send)
        c0, c1, c2 = edge_cols
        fields[1, c0, :] += strip[1, own, :]
        fields[2, c0, :] += strip[6, own, :]
        fields[2, c1, :] += strip[7, own, :]

    others = sums.at[pl.ds(0, n_all - 1)]
    wait_bytes(others, sum_recv)
    out_totals[...] = jnp.sum(sums[...], axis=0)
    wait_bytes(others, sum_send)


def finish(
    total_cells, all_totals, r0, fields, images, out_x, out_r, out_norms, x, r, norms_out, sem, norm_sem
):
    levels = r0.shape[-1]
    totals = all_totals[...]
    value = {
        key: jnp.broadcast_to(totals[:, k : k + 1], (8, levels)) for k, key in enumerate(KEYS)
    }

    rho, g0, g1, g2 = value[(0, 0)], value[(0, 1)], value[(0, 2)], value[(0, 3)]
    a00, a01, a02 = value[(1, 1)], value[(1, 2)], value[(1, 3)]
    a11, a12, a22 = value[(2, 2)], value[(2, 3)], value[(3, 3)]
    l10, l20, y0 = a01 / a00, a02 / a00, g0 / a00
    d1, e12, f1 = a11 - l10 * a01, a12 - l10 * a02, g1 - l10 * g0
    l21, y1 = e12 / d1, f1 / d1
    d2, f2 = a22 - l20 * a02 - l21 * e12, g2 - l20 * g0 - l21 * f1
    y2 = f2 / d2
    norm0 = rho - y0 * g0
    norm1 = norm0 - y1 * f1
    norm2 = norm1 - y2 * f2
    y1 = y1 - l21 * y2
    y0 = y0 - l10 * y1 - l20 * y2
    norm_lane = lax.broadcasted_iota(jnp.int32, (8, levels), 1)
    norms = jnp.where(norm_lane == 0, norm0, jnp.where(norm_lane == 1, norm1, norm2))
    norms_out[...] = norms[:1, :ITERS] / total_cells
    copies = [pltpu.make_async_copy(norms_out, out_norms, norm_sem)]
    copies[0].start()
    rows = r0.shape[0]
    pieces = 2 if rows % 16 == 0 else 1
    size = rows // pieces
    y0, y1, y2 = (jnp.tile(y, (size // 8, 1)) for y in (y0, y1, y2))
    for p in range(pieces):
        span = pl.ds(p * size, size)
        x[span] = y0 * fields[0, span] + y1 * fields[1, span] + y2 * fields[2, span]
        r[span] = (
            r0[span] - y0 * images[0, span] - y1 * images[1, span] - y2 * images[2, span]
        )
        for k, (src, dst) in enumerate(((x, out_x), (r, out_r))):
            copy = pltpu.make_async_copy(src.at[span], dst.at[span], sem.at[p, k])
            copy.start()
            copies.append(copy)
    for copy in copies:
        copy.wait()


def on_device(n_gx, n_gy, right_side, diagonal, horizontal, vertical, precond, edge_rows):
    rows, cols, levels = right_side.shape
    f32 = jnp.float32
    block = (rows * cols, levels)
    column = (n_gy * rows, levels)
    sems = pltpu.SemaphoreType.DMA
    basis = pltpu.VMEM((ITERS,) + block, f32)
    fields, images, totals, start = pl.pallas_call(
        functools.partial(kernel, n_gx, n_gy, rows),
        out_shape=(basis, basis, pltpu.VMEM((1, levels), f32), pltpu.VMEM(block, f32)),
        in_specs=[ANY, ANY, ANY, ANY, ANY, ANY],
        out_specs=(VMEM, VMEM, VMEM, VMEM),
        scratch_shapes=[
            pltpu.VMEM(block, f32),
            pltpu.VMEM(block, f32),
            pltpu.VMEM((1, levels), f32),
            pltpu.VMEM((2 * levels, levels), f32),
            pltpu.VMEM((2, 2 * levels, 2 * levels), jnp.bfloat16),
            pltpu.VMEM((ITERS, 6 * rows + 2 * cols, levels), f32),
            pltpu.VMEM((6, rows, levels), f32),
            pltpu.VMEM((2, 16, levels), f32),
            pltpu.VMEM((2, 16, levels), f32),
            pltpu.VMEM((2, 4, rows + 16, levels), f32),
            pltpu.VMEM((2, 3, rows, levels), f32),
            pltpu.VMEM((2, 3, rows, levels), f32),
            pltpu.VMEM((4, 8, levels), f32),
            pltpu.VMEM((4, 8, levels), f32),
            pltpu.VMEM((2, rows + 16, levels), f32),
            pltpu.VMEM((ITERS, rows, levels), f32),
            pltpu.VMEM((ITERS, rows, levels), f32),
            pltpu.VMEM((ITERS, cols, levels), f32),
            pltpu.VMEM((ITERS, cols, levels), f32),
            pltpu.VMEM((4,) + column, f32),
            pltpu.VMEM((5,) + column, f32),
            pltpu.VMEM(column, f32),
            pltpu.VMEM((4,) + column, f32),
            pltpu.VMEM((10,) + column, f32),
            pltpu.VMEM((2 * rows, levels), f32),
            pltpu.VMEM((2 * rows, levels), f32),
            pltpu.VMEM((16, levels), f32),
            pltpu.VMEM((n_gx * n_gy, 1, levels), f32),
            pltpu.SMEM(edge_rows.shape, jnp.int32),
            sems((7,)),
            sems((ITERS, 2)),
            sems((ITERS,)),
            sems((ITERS,)),
            sems((2,)),
            sems((2,)),
            sems(()),
            sems(()),
            sems(()),
            sems(()),
            sems((2,)),
            sems((2,)),
            sems((2,)),
            sems((2,)),
            sems((4,)),
            sems((4,)),
            sems((ITERS, 2)),
            sems((ITERS,)),
            sems((ITERS,)),
            sems(()),
            sems(()),
        ],
        compiler_params=pltpu.CompilerParams(collective_id=0, has_side_effects=True),
    )(
        edge_rows,
        right_side.reshape(block),
        diagonal.reshape(block),
        horizontal.reshape(block),
        vertical.reshape(1, levels),
        precond,
    )
    in_vmem = functools.partial(
        pltpu.with_memory_space_constraint, memory_space=pltpu.VMEM
    )
    total_cells = float(rows * cols * levels * n_gx * n_gy)
    x, r, norms = pl.pallas_call(
        functools.partial(finish, total_cells),
        out_shape=(
            jax.ShapeDtypeStruct(block, f32),
            jax.ShapeDtypeStruct(block, f32),
            jax.ShapeDtypeStruct((1, ITERS), f32),
        ),
        in_specs=[VMEM, VMEM, VMEM, VMEM],
        out_specs=(ANY, ANY, ANY),
        scratch_shapes=[
            pltpu.VMEM(block, f32),
            pltpu.VMEM(block, f32),
            pltpu.VMEM((1, ITERS), f32),
            sems((2, 2)),
            sems(()),
        ],
    )(in_vmem(totals), in_vmem(start), in_vmem(fields), in_vmem(images))
    shape = right_side.shape
    return x.reshape(shape), r.reshape(shape), norms.reshape(ITERS)


def solution(mesh):
    n_gx, n_gy = mesh.shape["gx"], mesh.shape["gy"]
    field = P("gy", "gx", None)
    return jax.shard_map(
        functools.partial(on_device, n_gx, n_gy),
        mesh=mesh,
        in_specs=(field, field, field, P(), P(), P()),
        out_specs=(field, field, P()),
        check_vma=False,
    )
```

```python
import functools

import jax
import jax.numpy as jnp
from jax import lax
from jax.experimental import pallas as pl
from jax.experimental.pallas import tpu as pltpu
from jax.sharding import PartitionSpec as P

ITERS = 3
KEYS = [(i, j) for j in range(ITERS + 1) for i in range(j + 1)]
MESH = pl.DeviceIdType.MESH
ANY = pl.BlockSpec(memory_space=pl.ANY)
VMEM = pl.BlockSpec(memory_space=pltpu.VMEM)


def kernel(
    n_gx,
    n_gy,
    out_rows,
    edge_table,
    right_side,
    diagonal,
    horizontal,
    vertical,
    precond,
    fields,
    images,
    out_totals,
    r0,
    diag,
    horiz,
    vert,
    matrix,
    weights,
    frame_z,
    pack,
    near_out,
    near_coef,
    mini_out,
    mini_in,
    wide,
    edge_out,
    edge_in,
    corner_out,
    corner_in,
    beyond,
    from_east,
    from_west,
    from_north,
    from_south,
    far_pack,
    near_pack,
    far_last,
    gathered,
    strip,
    strip_out,
    outside,
    partial,
    sums,
    edge_rows,
    meter,
    load_sem,
    small_sem,
    sent,
    sum_sent,
    col_recv,
    row_recv,
    far_recv,
    relay_recv,
    near_recv,
    mini_recv,
    strip_recv,
    sum_recv,
):
    rows, levels = out_rows, r0.shape[-1]
    cells = r0.shape[0]
    cols = cells // rows
    tall = n_gy * rows
    gx, gy = lax.axis_index("gx"), lax.axis_index("gy")
    n_all = n_gx * n_gy
    half = n_gx // 2
    me = gx * n_gy + gy

    def for_others(visit):
        def step(i, carry):
            for j in range(n_gy):
                visit(lax.rem(gx + i, n_gx), lax.rem(gy + j, n_gy))
            return carry

        if n_all <= 64:
            for i in sorted(range(1, n_gx), key=lambda i: min(i, n_gx - i)):
                step(i, 0)
        else:
            lax.fori_loop(1, n_gx, step, 0)
        for j in range(1, n_gy):
            visit(gx, lax.rem(gy + j, n_gy))

    barrier = pltpu.get_barrier_semaphore()

    def greet(x, y):
        pl.semaphore_signal(barrier, inc=1, device_id=(x, y), device_id_type=MESH)

    for_others(greet)

    panel = lax.convert_element_type(gx >= half, jnp.int32)
    loads = [
        pltpu.make_async_copy(right_side, r0, load_sem),
        pltpu.make_async_copy(precond.at[panel], matrix.at[pl.ds(0, levels)], load_sem),
        pltpu.make_async_copy(horizontal, horiz, load_sem),
        pltpu.make_async_copy(diagonal, diag, load_sem),
        pltpu.make_async_copy(precond.at[1 - panel], matrix.at[pl.ds(levels, levels)], load_sem),
        pltpu.make_async_copy(vertical, vert, small_sem.at[0]),
        pltpu.make_async_copy(edge_table, edge_rows, small_sem.at[1]),
    ]
    for load in loads:
        load.start()

    east_x, west_x = lax.rem(gx + 1, n_gx), lax.rem(gx + n_gx - 1, n_gx)
    east_border = (gx == half - 1) | (gx == n_gx - 1)
    west_border = (gx == half) | (gx == 0)
    border = east_border | west_border
    far_x = jnp.where(east_border, east_x, west_x)
    side = jnp.where(east_border, 0, 1)
    table = jnp.where((gx == half - 1) | (gx == half), 0, 1)
    edge_cols = [
        pl.ds(jnp.where(east_border, cols - 1 - i, i), rows, stride=cols) for i in range(3)
    ]
    first_row = pl.multiple_of(gy * rows, rows)
    own = pl.ds(first_row, rows)
    has_north, has_south = gy < n_gy - 1, gy > 0
    between = has_north & has_south

    def wait_count(count, sem):
        part = meter.at[pl.ds(0, count)]
        pltpu.make_async_copy(part, part, sem).wait()

    def wait_cases(count, sem):
        for n_sides, on_border in ((1, border), (2, jnp.logical_not(border))):
            for n_rows, here in ((1, jnp.logical_not(between)), (2, between)):
                pl.when(on_border & here)(
                    functools.partial(wait_count, count(n_sides, n_rows), sem)
                )

    @pl.when(jnp.logical_not(has_north))
    def _():
        from_north[...] = jnp.zeros_like(from_north)

    @pl.when(jnp.logical_not(has_south))
    def _():
        from_south[...] = jnp.zeros_like(from_south)

    outside[...] = jnp.zeros_like(outside)

    def split(v):
        high = v.astype(jnp.bfloat16)
        return high, (v - high.astype(jnp.float32)).astype(jnp.bfloat16)

    def prepare_weights():
        for which in range(2):
            for part, value in enumerate(split(matrix[pl.ds(which * levels, levels), :])):
                for twice in range(2):
                    weights[
                        which, pl.ds(part * levels, levels), pl.ds(twice * levels, levels)
                    ] = value

    def precondition(v, which=0):
        out = lax.dot_general(
            jnp.concatenate(split(v), 1),
            weights[which],
            (((1,), (1,)), ((), ())),
            preferred_element_type=jnp.float32,
        )
        return out[:, :levels] + out[:, levels:]

    def col_copy(t, side):
        buffer, x = (from_west, east_x) if side == 0 else (from_east, west_x)
        return pltpu.make_async_remote_copy(
            src_ref=frame_z.at[t, pl.ds(side * rows, rows)],
            dst_ref=buffer.at[t],
            send_sem=sent,
            recv_sem=col_recv.at[t // 2],
            device_id=(x, gy),
            device_id_type=MESH,
        )

    def far_copy(t, g):
        return pltpu.make_async_remote_copy(
            src_ref=pack.at[pl.ds(0, 4)] if t == 0 else pack.at[4],
            dst_ref=far_pack.at[:, own] if t == 0 else far_last.at[own],
            send_sem=sent,
            recv_sem=far_recv.at[t],
            device_id=(far_x, g),
            device_id_type=MESH,
        )

    def relay_copy(g, block):
        return pltpu.make_async_remote_copy(
            src_ref=far_pack.at[:, block],
            dst_ref=far_pack.at[:, block],
            send_sem=sent,
            recv_sem=relay_recv,
            device_id=(gx, g),
            device_id_type=MESH,
        )

    def near_copy(g):
        return pltpu.make_async_remote_copy(
            src_ref=near_out,
            dst_ref=near_pack.at[:, own],
            send_sem=sent,
            recv_sem=near_recv,
            device_id=(gx, g),
            device_id_type=MESH,
        )

    def mini_copy(side):
        return pltpu.make_async_remote_copy(
            src_ref=mini_out.at[side],
            dst_ref=mini_in.at[side],
            send_sem=sent,
            recv_sem=mini_recv,
            device_id=(gx, gy + 1 if side == 0 else gy - 1),
            device_id_type=MESH,
        )

    def row_copy(t, side):
        buffer, y, row = (
            (from_south, gy + 1, 2 * rows + cols)
            if side == 0
            else (from_north, gy - 1, 2 * rows)
        )
        return pltpu.make_async_remote_copy(
            src_ref=frame_z.at[t, pl.ds(row, cols)],
            dst_ref=buffer.at[t],
            send_sem=sent,
            recv_sem=row_recv.at[t],
            device_id=(gx, y),
            device_id_type=MESH,
        )

    def edge_copy(side):
        return pltpu.make_async_remote_copy(
            src_ref=edge_out.at[side],
            dst_ref=edge_in.at[1 - side],
            send_sem=sent,
            recv_sem=strip_recv,
            device_id=(east_x if side == 0 else west_x, gy),
            device_id_type=MESH,
        )

    def corner_copy(k):
        return pltpu.make_async_remote_copy(
            src_ref=corner_out.at[k],
            dst_ref=corner_in.at[k],
            send_sem=sent,
            recv_sem=strip_recv,
            device_id=(west_x if k < 2 else east_x, gy + 1 if k % 2 == 0 else gy - 1),
            device_id_type=MESH,
        )

    def for_sides(visit):
        pl.when(jnp.logical_not(east_border))(functools.partial(visit, 0))
        pl.when(jnp.logical_not(west_border))(functools.partial(visit, 1))

    def for_corners(visit, sending):
        for k in range(4):
            east = (k < 2) != sending
            north = (k % 2 == 0) == sending
            condition = jnp.logical_not(east_border if east else west_border)
            pl.when(condition & (has_north if north else has_south))(functools.partial(visit, k))

    def for_rows(visit):
        @pl.when(has_north)
        def _():
            visit(0)

        @pl.when(has_south)
        def _():
            visit(1)

    inward = 2 * (rows + cols)
    mid = pl.ds(8, rows)

    def side_cols(side, k):
        return pl.ds(k if side else cols - 1 - k, rows, stride=cols)

    def fill_edges():
        for side in range(2):
            items = [
                frame_z[0, pl.ds(side * rows, rows), :],
                frame_z[0, pl.ds(inward + side * rows, rows), :],
                horiz[side_cols(side, 0), :],
                diag[side_cols(side, 0), :],
            ]
            for k, item in enumerate(items):
                wide[side, k] = jnp.zeros_like(wide[side, k])
                wide[side, k, mid, :] = item
                if k:
                    edge_out[side, k - 1] = item
            for to, first, second in ((0, rows - 1, rows - 2), (1, 0, 1)):
                picks = [(0, first), (0, second), (1, first), (2, first), (3, first)]
                for k, (item, row) in enumerate(picks):
                    mini_out[to, pl.ds(8 * side + k, 1), :] = items[item][row : row + 1]
                next_horiz = horiz[pl.ds(first * cols + (1 if side else cols - 2), 1), :]
                mini_out[to, pl.ds(8 * side + 5, 1), :] = next_horiz
                mini_out[to, pl.ds(8 * side + 6, 2), :] = jnp.zeros((2, levels), jnp.float32)
                corner_out[2 * (1 - side) + to] = jnp.zeros((8, levels), jnp.float32)
                corner_out[2 * (1 - side) + to, pl.ds(0, 1), :] = items[0][first : first + 1]
        beyond[...] = jnp.zeros_like(beyond)

    def fill_packs():
        c0, c1, c2 = edge_cols
        z_edge = frame_z[0, pl.ds(side * rows, rows), :]
        h_edge, d_edge = horiz[c0, :], diag[c0, :]
        z_next = frame_z[0, pl.ds(inward + side * rows, rows), :]
        for k, item in enumerate([z_edge, z_next, h_edge, d_edge]):
            pack[k] = item
        for k, item in enumerate([z_edge, h_edge]):
            near_out[k] = item
            near_pack[k, own, :] = item
        for k, item in enumerate([d_edge, horiz[c1, :]]):
            near_coef[k] = jnp.zeros_like(near_coef[k])
            near_coef[k, own, :] = item

    def send_first(frame):
        frame_z[0] = precondition(frame)
        fill_edges()
        pl.when(border)(fill_packs)
        pl.semaphore_wait(barrier, n_all - 1)

        @pl.when(gx == 0)
        def _():
            for g in range(1, n_gy, 2):
                far_copy(0, g).start()

        for_sides(lambda side: col_copy(0, side).start())
        for_rows(lambda side: mini_copy(side).start())
        for_rows(lambda side: row_copy(0, side).start())
        for_corners(lambda k: corner_copy(k).start(), True)
        for_sides(lambda side: edge_copy(side).start())

        pl.when(border & (gx > 0))(lambda: far_copy(0, gy).start())

    def send_rows(t, frame):
        frame_z[t, pl.ds(2 * rows, 2 * cols), :] = precondition(frame)
        for_rows(lambda side: row_copy(t, side).start())

    def send_far_last():
        for j in sorted(range(n_gy), key=lambda j: abs(2 * j - n_gy)):
            far_copy(1, lax.rem(gy + j, n_gy)).start()
        for j in range(1, n_gy):
            near_copy(lax.rem(gy + j, n_gy)).start()

    def receive_rows(t):
        wait_cases(lambda sides, beside: beside * cols, row_recv.at[t])

    def receive_cols(t):
        wait_cases(lambda sides, beside: sides * rows, col_recv.at[t // 2])

        def take(side):
            buffer = from_west if side else from_east
            outside[pl.ds(side * rows, rows), :] = buffer[t]
            if t == 0:
                beyond[side, mid, :] = buffer[t]

        for_sides(take)

    col_id = lax.rem(lax.broadcasted_iota(jnp.int32, (cells, levels), 0), cols)
    east_edge = pl.ds(cols - 1, rows, stride=cols)
    west_edge = pl.ds(0, rows, stride=cols)
    south_edge = pl.ds(0, cols)
    north_edge = pl.ds(cells - cols, cols)

    def edge_columns(ref):
        return jnp.concatenate([ref[east_edge, :], ref[west_edge, :]], 0)

    def column_part(z):
        lane = lax.broadcasted_iota(jnp.int32, z.shape, 1)
        up = jnp.where(lane < levels - 1, pltpu.roll(z, levels - 1, 1), 0.0)
        down = jnp.where(lane > 0, pltpu.roll(z, 1, 1), 0.0)
        return vert[...] * (2.0 * z - (up + down))

    def inner_image(z):
        east = jnp.where(col_id < cols - 1, pltpu.roll(z, cells - 1, 0), 0.0)
        west = jnp.where(col_id > 0, pltpu.roll(z, 1, 0), 0.0)
        none = jnp.zeros((cols, levels), jnp.float32)
        north = jnp.concatenate([z[cols:], none], 0)
        south = jnp.concatenate([none, z[:-cols]], 0)
        beside = east + west + north + south
        return diag[...] * z + horiz[...] * (4.0 * z - beside) + column_part(z)

    def product(a, b):
        both = (a * b).reshape(-1, 8, levels)
        return jnp.sum(jnp.sum(both, axis=0), axis=0, keepdims=True)

    tall_id = lax.broadcasted_iota(jnp.int32, (tall, levels), 0)

    def along(w):
        north = jnp.where(tall_id < tall - 1, pltpu.roll(w, tall - 1, 0), 0.0)
        south = jnp.where(tall_id > 0, pltpu.roll(w, 1, 0), 0.0)
        return north + south

    def stencil(w, d, h):
        return d * w + h * (4.0 * w - along(w)) + column_part(w)

    def gather_rows(start, count, pairs):
        def one(y):
            row = edge_rows[table, start + y]
            for dst, src in pairs:
                gathered[dst, pl.ds(y, 1), :] = src[pl.ds(row, 1), :]

        if count <= 64:
            for y in range(count):
                one(y)
        else:

            def body(y, carry):
                one(y)
                return carry

            lax.fori_loop(0, count, body, 0)

    def wait_bytes(ref, sem):
        pltpu.make_async_copy(ref, ref, sem).wait()

    near_rest = pl.ds(0, (n_gy - 1) * rows)
    last = gx == n_gx - 1
    relays = border & jnp.logical_not(last)
    alike = pl.ds(0, n_gy // 2 * rows)

    crosses = last & (lax.rem(gy, 2) == 1)
    crossed = last & (lax.rem(gy, 2) == 0)

    def relay_across():
        wait_bytes(far_pack, far_recv.at[0])
        relay_copy(gy - 1, pl.ds(0, tall)).start()

    def relay():
        wait_bytes(far_pack.at[:, own], far_recv.at[0])
        for j in sorted(range(1, n_gy), key=lambda j: abs(2 * j - n_gy)):
            relay_copy(lax.rem(gy + j, n_gy), own).start()


    def next_to(w):
        return pltpu.roll(w, w.shape[0] - 1, 0) + pltpu.roll(w, 1, 0)

    def strip_image(side, k, z, left, right):
        c = side_cols(side, k)
        return diag[c, :] * z + horiz[c, :] * (4.0 * z - left - right) + column_part(z)

    def look_ahead():
        c1 = edge_cols[1]

        def take(direction, near, far, row):
            for k in range(2):
                near_coef[k, pl.ds(row, 1), :] = mini_in[direction, pl.ds(8 * side + 4 + k, 1), :]
            for k_side in range(2):
                given = mini_in.at[direction]
                wide[k_side, 0, pl.ds(near, 1), :] = given[pl.ds(8 * k_side, 1), :]
                wide[k_side, 0, pl.ds(far, 1), :] = given[pl.ds(8 * k_side + 1, 1), :]
                for k in (1, 2, 3):
                    wide[k_side, k, pl.ds(near, 1), :] = given[pl.ds(8 * k_side + k + 1, 1), :]

        wait_cases(lambda sides, beside: 16 * beside, mini_recv)
        pl.when(has_south)(functools.partial(take, 0, 7, 6, first_row - 1))
        pl.when(has_north)(functools.partial(take, 1, 8 + rows, 9 + rows, first_row + rows))
        z_edge, z_next, h_edge, d_edge = (wide[side, k] for k in range(4))
        v_edge = (
            d_edge * z_edge
            + h_edge * (4.0 * z_edge - z_next - next_to(z_edge))
            + column_part(z_edge)
        )
        beside = next_to(z_next)[8 : 8 + rows] + z_edge[8 : 8 + rows]
        z1 = z_next[8 : 8 + rows]
        z2 = frame_z[0, pl.ds(inward + (2 + side) * rows, rows), :]
        v_next = (
            diag[c1, :] * z1 + horiz[c1, :] * (4.0 * z1 - beside - z2) + column_part(z1)
        )
        z = precondition(jnp.concatenate([v_edge, v_next], 0))
        z_edge, z_next = z[: rows + 16], z[rows + 16 :]
        beside = next_to(z_edge)[8 : 8 + rows] + z_next
        z_edge = z_edge[8 : 8 + rows]
        near_out[2] = z_edge
        near_pack[2, own, :] = z_edge
        h_own, d_own = h_edge[8 : 8 + rows], d_edge[8 : 8 + rows]
        v = d_own * z_edge + h_own * (4.0 * z_edge - beside) + column_part(z_edge)
        pack[4] = precondition(v)
        pl.when(border)(send_far_last)

    def look_across():
        wait_cases(lambda sides, beside: sides * (3 * rows + 8 * beside), strip_recv)

        def take(k):
            row = 8 + rows if k % 2 else 7
            beyond[k // 2, pl.ds(row, 1), :] = corner_in[k, pl.ds(0, 1), :]

        for_corners(take, False)
        images_first = []
        for side in range(2):
            z_edge, z_next, h_edge, d_edge = (wide[side, k] for k in range(4))
            z_out = beyond[side]
            own_edge, own_out = z_edge[8 : 8 + rows], z_out[8 : 8 + rows]
            v_edge = (
                d_edge * z_edge
                + h_edge * (4.0 * z_edge - z_next - z_out - next_to(z_edge))
                + column_part(z_edge)
            )
            z1 = z_next[8 : 8 + rows]
            z2 = frame_z[0, pl.ds(inward + (2 + side) * rows, rows), :]
            v_next = strip_image(side, 1, z1, next_to(z_next)[8 : 8 + rows] + own_edge, z2)
            v_out = (
                edge_in[side, 2] * own_out
                + edge_in[side, 1]
                * (4.0 * own_out - edge_in[side, 0] - own_edge - next_to(z_out)[8 : 8 + rows])
                + column_part(own_out)
            )
            images_first += [v_edge, v_next, v_out]
        z = precondition(jnp.concatenate(images_first, 0))
        second = []
        each = 3 * rows + 16
        for side in range(2):
            part = z[side * each : (side + 1) * each]
            z_edge, z_next, z_out = part[: rows + 16], part[rows + 16 : each - rows], part[each - rows :]
            strip_out[pl.ds(side * rows, rows), :] = z_out
            beside = next_to(z_edge)[8 : 8 + rows]
            second.append(strip_image(side, 0, z_edge[8 : 8 + rows], beside + z_next, z_out))
        frame_z[2, pl.ds(0, 2 * rows), :] = precondition(jnp.concatenate(second, 0))

        def give(side):
            col_copy(2, side).start()
            outside[pl.ds(side * rows, rows), :] = strip_out[pl.ds(side * rows, rows), :]

        for_sides(give)

    def correct_early():
        @pl.when(border)
        def _():
            pl.when(crossed)(lambda: wait_bytes(far_pack, relay_recv))
            pl.when(relays)(lambda: wait_bytes(far_pack.at[:, near_rest], relay_recv))
            wait_bytes(near_pack.at[:, near_rest], near_recv)

        gather_rows(0, tall, [(0, far_pack.at[0]), (1, near_pack.at[0])])
        h_near, d_near = near_pack[1], near_coef[0]
        h_far, d_far = far_pack[2], far_pack[3]
        b_near, b_far = -(h_near * gathered[0]), -(h_far * gathered[1])
        v_far = stencil(far_pack[0], d_far, h_far) - h_far * far_pack[1] + b_far
        w_near = precondition(b_near)
        far = precondition(jnp.concatenate([b_far, v_far], 0), 1)
        w_far = far[:tall]
        strip[0] = b_near
        strip[1] = w_near
        strip[3] = far[tall:]
        strip[4] = near_pack[2] + w_near
        gather_rows(0, tall, [(0, strip.at[3]), (1, strip.at[4])])
        b_near = stencil(w_near, d_near, h_near) - h_near * gathered[0]
        b_far = stencil(w_far, d_far, h_far) - h_far * gathered[1]
        b_next = -(near_coef[1] * w_near)
        near = precondition(jnp.concatenate([b_near, b_next], 0))
        w_edge, w_next = near[:tall], near[tall:]
        strip[3] = b_near
        strip[4] = b_next
        strip[5] = precondition(b_far, 1)
        strip[6] = w_edge
        strip[7] = w_next
        strip[8] = along(w_next)
        strip[9] = stencil(w_edge, d_near, h_near) - h_near * w_next

    def correct_third():
        c0, c1, c2 = edge_cols
        w_edge, w_next, beside = strip[6, own, :], strip[7, own, :], strip[8, own, :]
        h1 = horiz[c1, :]
        later = diag[c1, :] * w_next + h1 * (4.0 * w_next - beside - w_edge) + column_part(w_next)
        b_third = -(horiz[c2, :] * w_next)
        gather_rows(first_row, rows, [(2, strip.at[5])])
        wait_bytes(far_last, far_recv.at[1])
        gather_rows(first_row, rows, [(3, far_last)])
        across = gathered[2, pl.ds(0, rows), :] + gathered[3, pl.ds(0, rows), :]
        b_edge = strip[9, own, :] - horiz[c0, :] * across
        none = jnp.zeros((rows, levels), jnp.float32)
        changes = [
            [strip[0, own, :], none, none],
            [strip[3, own, :], strip[4, own, :], none],
            [b_edge, later, b_third],
        ]
        before = [jnp.concatenate([r0[c, :] for c in edge_cols], 0)]
        after = [before[0]]
        for t in range(ITERS):
            old = jnp.concatenate([images[t, c, :] for c in edge_cols], 0)
            new = old + jnp.concatenate(changes[t], 0)
            before.append(old)
            after.append(new)
            for k in range(t + 1):
                images[t, edge_cols[k], :] = new[k * rows : (k + 1) * rows]
        for k, (i, j) in enumerate(KEYS):
            if j > 0:
                partial[pl.ds(k, 1), :] += product(after[i], after[j]) - product(before[i], before[j])

    wait_count(3 * cells + 2 * levels, load_sem)
    for load in loads[5:]:
        load.wait()
    prepare_weights()
    terms = {}
    spaces = [r0]
    frame = [edge_columns(r0), r0[south_edge, :], r0[north_edge, :]]
    frame += [r0[side_cols(side, k), :] for k in (1, 2) for side in range(2)]
    send_first(jnp.concatenate(frame, 0))
    edge_horiz = edge_columns(horiz)
    for t in range(ITERS):
        image = images.at[t]
        z = precondition(spaces[-1][...])
        fields[t] = z
        newest = len(spaces) - 1
        for i in range(len(spaces)):
            terms[(i, newest)] = product(spaces[i][...], spaces[newest][...])
        image[...] = inner_image(z)
        if t == 0:
            look_ahead()
        if t == 1:
            pl.when(relays)(relay)
            look_across()
        if t == 2:
            pl.when(crosses)(relay_across)
            correct_early()
        receive_rows(t)
        image[south_edge, :] = image[south_edge, :] - horiz[south_edge, :] * from_south[t]
        image[north_edge, :] = image[north_edge, :] - horiz[north_edge, :] * from_north[t]
        inside = edge_columns(image)
        if t != 1:
            receive_cols(t)
        edges = inside - edge_horiz * outside[...]
        image[east_edge, :] = edges[:rows]
        image[west_edge, :] = edges[rows:]
        if t < ITERS - 1:
            send_rows(t + 1, jnp.concatenate([image[south_edge, :], image[north_edge, :]], 0))
        spaces.append(image)
    newest = len(spaces) - 1
    for i in range(len(spaces)):
        terms[(i, newest)] = product(spaces[i][...], spaces[newest][...])
    for k, key in enumerate(KEYS):
        partial[pl.ds(k, 1), :] = terms[key]

    @pl.when(border)
    def _():
        correct_third()

    height = -(-len(KEYS) // 8) * 8
    row_id = lax.broadcasted_iota(jnp.int32, (height, levels), 0)
    lane = lax.broadcasted_iota(jnp.int32, (height, levels), 1)
    stacked = jnp.where(row_id < len(KEYS), partial[...], 0.0)
    summed = jnp.sum(stacked, axis=1, keepdims=True)
    sums[me] = jnp.sum(jnp.where(lane == row_id, summed, 0.0), axis=0, keepdims=True)

    def tell(x, y):
        pltpu.make_async_remote_copy(
            src_ref=sums.at[me],
            dst_ref=sums.at[me],
            send_sem=sum_sent,
            recv_sem=sum_recv,
            device_id=(x, y),
            device_id_type=MESH,
        ).start()

    for_others(tell)
    def all_sent(sides, beside, border_part):
        per_side = 5 * rows + 8 * beside
        return sides * per_side + beside * (ITERS * cols + 16) + border_part * rows

    common = n_gy + 3 * (n_gy - 1)
    first, inner = gx == 0, border & jnp.logical_not(last | (gx == 0))
    for condition, sides, border_part in (
        (jnp.logical_not(border), 2, 0),
        (first, 1, common + 2 * n_gy + 4 * (n_gy - 1)),
        (inner, 1, common + 4 + 4 * (n_gy - 1)),
        (crosses, 1, common + 4 + 4 * n_gy),
        (crossed, 1, common + 4),
    ):
        for beside, here in ((1, jnp.logical_not(between)), (2, between)):
            pl.when(condition & here)(
                functools.partial(wait_count, all_sent(sides, beside, border_part), sent)
            )

    @pl.when(border)
    def _():
        c0, c1, c2 = edge_cols
        fields[1, c0, :] += strip[1, own, :]
        fields[2, c0, :] += strip[6, own, :]
        fields[2, c1, :] += strip[7, own, :]

    others = sums.at[pl.ds(0, n_all - 1)]
    wait_bytes(others, sum_recv)
    out_totals[...] = jnp.sum(sums[...], axis=0)
    wait_bytes(others, sum_sent)


def finish(
    total_cells, all_totals, r0, fields, images, out_x, out_r, out_norms, x, r, norms_out, sem, norm_sem
):
    levels = r0.shape[-1]
    totals = all_totals[...]
    value = {
        key: jnp.broadcast_to(totals[:, k : k + 1], (8, levels)) for k, key in enumerate(KEYS)
    }

    rho, g0, g1, g2 = value[(0, 0)], value[(0, 1)], value[(0, 2)], value[(0, 3)]
    a00, a01, a02 = value[(1, 1)], value[(1, 2)], value[(1, 3)]
    a11, a12, a22 = value[(2, 2)], value[(2, 3)], value[(3, 3)]
    l10, l20, y0 = a01 / a00, a02 / a00, g0 / a00
    d1, e12, f1 = a11 - l10 * a01, a12 - l10 * a02, g1 - l10 * g0
    l21, y1 = e12 / d1, f1 / d1
    d2, f2 = a22 - l20 * a02 - l21 * e12, g2 - l20 * g0 - l21 * f1
    y2 = f2 / d2
    norm0 = rho - y0 * g0
    norm1 = norm0 - y1 * f1
    norm2 = norm1 - y2 * f2
    y1 = y1 - l21 * y2
    y0 = y0 - l10 * y1 - l20 * y2
    norm_lane = lax.broadcasted_iota(jnp.int32, (8, levels), 1)
    norms = jnp.where(norm_lane == 0, norm0, jnp.where(norm_lane == 1, norm1, norm2))
    norms_out[...] = norms[:1, :ITERS] / total_cells
    copies = [pltpu.make_async_copy(norms_out, out_norms, norm_sem)]
    copies[0].start()
    rows = r0.shape[0]
    pieces = 2 if rows % 16 == 0 else 1
    size = rows // pieces
    y0, y1, y2 = (jnp.tile(y, (size // 8, 1)) for y in (y0, y1, y2))
    for p in range(pieces):
        span = pl.ds(p * size, size)
        x[span] = y0 * fields[0, span] + y1 * fields[1, span] + y2 * fields[2, span]
        r[span] = (
            r0[span] - y0 * images[0, span] - y1 * images[1, span] - y2 * images[2, span]
        )
        for k, (src, dst) in enumerate(((x, out_x), (r, out_r))):
            copy = pltpu.make_async_copy(src.at[span], dst.at[span], sem.at[p, k])
            copy.start()
            copies.append(copy)
    for copy in copies:
        copy.wait()


def on_device(n_gx, n_gy, right_side, diagonal, horizontal, vertical, precond, edge_rows):
    rows, cols, levels = right_side.shape
    f32 = jnp.float32
    block = (rows * cols, levels)
    column = (n_gy * rows, levels)
    sems = pltpu.SemaphoreType.DMA
    meter_rows = 3 * rows * cols + 2 * levels + (16 + 10 * n_gy) * rows + 8 * cols + 64
    basis = pltpu.VMEM((ITERS,) + block, f32)
    fields, images, totals, start = pl.pallas_call(
        functools.partial(kernel, n_gx, n_gy, rows),
        out_shape=(basis, basis, pltpu.VMEM((1, levels), f32), pltpu.VMEM(block, f32)),
        in_specs=[ANY, ANY, ANY, ANY, ANY, ANY],
        out_specs=(VMEM, VMEM, VMEM, VMEM),
        scratch_shapes=[
            pltpu.VMEM(block, f32),
            pltpu.VMEM(block, f32),
            pltpu.VMEM((1, levels), f32),
            pltpu.VMEM((2 * levels, levels), f32),
            pltpu.VMEM((2, 2 * levels, 2 * levels), jnp.bfloat16),
            pltpu.VMEM((ITERS, 6 * rows + 2 * cols, levels), f32),
            pltpu.VMEM((5, rows, levels), f32),
            pltpu.VMEM((3, rows, levels), f32),
            pltpu.VMEM((2,) + column, f32),
            pltpu.VMEM((2, 16, levels), f32),
            pltpu.VMEM((2, 16, levels), f32),
            pltpu.VMEM((2, 4, rows + 16, levels), f32),
            pltpu.VMEM((2, 3, rows, levels), f32),
            pltpu.VMEM((2, 3, rows, levels), f32),
            pltpu.VMEM((4, 8, levels), f32),
            pltpu.VMEM((4, 8, levels), f32),
            pltpu.VMEM((2, rows + 16, levels), f32),
            pltpu.VMEM((ITERS, rows, levels), f32),
            pltpu.VMEM((ITERS, rows, levels), f32),
            pltpu.VMEM((ITERS, cols, levels), f32),
            pltpu.VMEM((ITERS, cols, levels), f32),
            pltpu.VMEM((4,) + column, f32),
            pltpu.VMEM((3,) + column, f32),
            pltpu.VMEM(column, f32),
            pltpu.VMEM((4,) + column, f32),
            pltpu.VMEM((10,) + column, f32),
            pltpu.VMEM((2 * rows, levels), f32),
            pltpu.VMEM((2 * rows, levels), f32),
            pltpu.VMEM((16, levels), f32),
            pltpu.VMEM((n_gx * n_gy, 1, levels), f32),
            pltpu.SMEM(edge_rows.shape, jnp.int32),
            pltpu.VMEM((meter_rows, levels), f32),
            sems(()),
            sems((2,)),
            sems(()),
            sems(()),
            sems((2,)),
            sems((ITERS,)),
            sems((2,)),
            sems(()),
            sems(()),
            sems(()),
            sems(()),
            sems(()),
        ],
        compiler_params=pltpu.CompilerParams(collective_id=0, has_side_effects=True),
    )(
        edge_rows,
        right_side.reshape(block),
        diagonal.reshape(block),
        horizontal.reshape(block),
        vertical.reshape(1, levels),
        precond,
    )
    in_vmem = functools.partial(
        pltpu.with_memory_space_constraint, memory_space=pltpu.VMEM
    )
    total_cells = float(rows * cols * levels * n_gx * n_gy)
    x, r, norms = pl.pallas_call(
        functools.partial(finish, total_cells),
        out_shape=(
            jax.ShapeDtypeStruct(block, f32),
            jax.ShapeDtypeStruct(block, f32),
            jax.ShapeDtypeStruct((1, ITERS), f32),
        ),
        in_specs=[VMEM, VMEM, VMEM, VMEM],
        out_specs=(ANY, ANY, ANY),
        scratch_shapes=[
            pltpu.VMEM(block, f32),
            pltpu.VMEM(block, f32),
            pltpu.VMEM((1, ITERS), f32),
            sems((2, 2)),
            sems(()),
        ],
    )(in_vmem(totals), in_vmem(start), in_vmem(fields), in_vmem(images))
    shape = right_side.shape
    return x.reshape(shape), r.reshape(shape), norms.reshape(ITERS)


def solution(mesh):
    n_gx, n_gy = mesh.shape["gx"], mesh.shape["gy"]
    field = P("gy", "gx", None)
    return jax.shard_map(
        functools.partial(on_device, n_gx, n_gy),
        mesh=mesh,
        in_specs=(field, field, field, P(), P(), P()),
        out_specs=(field, field, P()),
        check_vma=False,
    )
```

```python
import functools

import jax
import jax.numpy as jnp
from jax import lax
from jax.experimental import pallas as pl
from jax.experimental.pallas import tpu as pltpu
from jax.sharding import PartitionSpec as P

ITERS = 3
KEYS = [(i, j) for j in range(ITERS + 1) for i in range(j + 1)]
MESH = pl.DeviceIdType.MESH
ANY = pl.BlockSpec(memory_space=pl.ANY)
VMEM = pl.BlockSpec(memory_space=pltpu.VMEM)


def kernel(
    n_gx,
    n_gy,
    out_rows,
    edge_table,
    right_side,
    diagonal,
    horizontal,
    vertical,
    precond,
    fields,
    images,
    out_totals,
    r0,
    diag,
    horiz,
    vert,
    matrix,
    weights,
    frame_z,
    pack,
    near_out,
    near_coef,
    mini_out,
    mini_in,
    wide,
    edge_out,
    edge_in,
    corner_out,
    corner_in,
    beyond,
    from_east,
    from_west,
    from_north,
    from_south,
    far_pack,
    near_pack,
    far_last,
    gathered,
    strip,
    strip_out,
    outside,
    partial,
    extra,
    sums,
    edge_rows,
    meter,
    load_sem,
    small_sem,
    sent,
    sum_sent,
    col_recv,
    row_recv,
    far_recv,
    relay_recv,
    near_recv,
    mini_recv,
    strip_recv,
    sum_recv,
):
    rows, levels = out_rows, r0.shape[-1]
    cells = r0.shape[0]
    cols = cells // rows
    tall = n_gy * rows
    gx, gy = lax.axis_index("gx"), lax.axis_index("gy")
    n_all = n_gx * n_gy
    half = n_gx // 2
    me = gx * n_gy + gy

    def for_others(visit):
        def step(i, carry):
            for j in range(n_gy):
                visit(lax.rem(gx + i, n_gx), lax.rem(gy + j, n_gy))
            return carry

        if n_all <= 64:
            for i in sorted(range(1, n_gx), key=lambda i: min(i, n_gx - i)):
                step(i, 0)
        else:
            lax.fori_loop(1, n_gx, step, 0)
        for j in range(1, n_gy):
            visit(gx, lax.rem(gy + j, n_gy))

    barrier = pltpu.get_barrier_semaphore()

    def greet(x, y):
        pl.semaphore_signal(barrier, inc=1, device_id=(x, y), device_id_type=MESH)

    for_others(greet)

    panel = lax.convert_element_type(gx >= half, jnp.int32)
    loads = [
        pltpu.make_async_copy(right_side, r0, load_sem),
        pltpu.make_async_copy(precond.at[panel], matrix.at[pl.ds(0, levels)], load_sem),
        pltpu.make_async_copy(horizontal, horiz, load_sem),
        pltpu.make_async_copy(diagonal, diag, load_sem),
        pltpu.make_async_copy(precond.at[1 - panel], matrix.at[pl.ds(levels, levels)], load_sem),
        pltpu.make_async_copy(vertical, vert, small_sem.at[0]),
        pltpu.make_async_copy(edge_table, edge_rows, small_sem.at[1]),
    ]
    for load in loads:
        load.start()

    east_x, west_x = lax.rem(gx + 1, n_gx), lax.rem(gx + n_gx - 1, n_gx)
    east_border = (gx == half - 1) | (gx == n_gx - 1)
    west_border = (gx == half) | (gx == 0)
    border = east_border | west_border
    far_x = jnp.where(east_border, east_x, west_x)
    side = jnp.where(east_border, 0, 1)
    table = jnp.where((gx == half - 1) | (gx == half), 0, 1)
    edge_cols = [
        pl.ds(jnp.where(east_border, cols - 1 - i, i), rows, stride=cols) for i in range(3)
    ]
    first_row = pl.multiple_of(gy * rows, rows)
    own = pl.ds(first_row, rows)
    has_north, has_south = gy < n_gy - 1, gy > 0
    between = has_north & has_south

    def wait_count(count, sem):
        part = meter.at[pl.ds(0, count)]
        pltpu.make_async_copy(part, part, sem).wait()

    def wait_cases(count, sem):
        for n_sides, on_border in ((1, border), (2, jnp.logical_not(border))):
            for n_rows, here in ((1, jnp.logical_not(between)), (2, between)):
                pl.when(on_border & here)(
                    functools.partial(wait_count, count(n_sides, n_rows), sem)
                )

    @pl.when(jnp.logical_not(has_north))
    def _():
        from_north[...] = jnp.zeros_like(from_north)

    @pl.when(jnp.logical_not(has_south))
    def _():
        from_south[...] = jnp.zeros_like(from_south)

    outside[...] = jnp.zeros_like(outside)
    extra[...] = jnp.zeros_like(extra)

    def split(v):
        high = v.astype(jnp.bfloat16)
        return high, (v - high.astype(jnp.float32)).astype(jnp.bfloat16)

    def prepare_weights():
        for which in range(2):
            for part, value in enumerate(split(matrix[pl.ds(which * levels, levels), :])):
                for twice in range(2):
                    weights[
                        which, pl.ds(part * levels, levels), pl.ds(twice * levels, levels)
                    ] = value

    def precondition(v, which=0):
        out = lax.dot_general(
            jnp.concatenate(split(v), 1),
            weights[which],
            (((1,), (1,)), ((), ())),
            preferred_element_type=jnp.float32,
        )
        return out[:, :levels] + out[:, levels:]

    def col_copy(t, side):
        buffer, x = (from_west, east_x) if side == 0 else (from_east, west_x)
        return pltpu.make_async_remote_copy(
            src_ref=frame_z.at[t, pl.ds(side * rows, rows)],
            dst_ref=buffer.at[t],
            send_sem=sent,
            recv_sem=col_recv.at[t // 2],
            device_id=(x, gy),
            device_id_type=MESH,
        )

    def far_copy(t, g):
        return pltpu.make_async_remote_copy(
            src_ref=pack.at[pl.ds(0, 4)] if t == 0 else pack.at[4],
            dst_ref=far_pack.at[:, own] if t == 0 else far_last.at[own],
            send_sem=sent,
            recv_sem=far_recv.at[t],
            device_id=(far_x, g),
            device_id_type=MESH,
        )

    def relay_copy(g, block):
        return pltpu.make_async_remote_copy(
            src_ref=far_pack.at[:, block],
            dst_ref=far_pack.at[:, block],
            send_sem=sent,
            recv_sem=relay_recv,
            device_id=(gx, g),
            device_id_type=MESH,
        )

    def near_copy(g):
        return pltpu.make_async_remote_copy(
            src_ref=near_out,
            dst_ref=near_pack.at[:, own],
            send_sem=sent,
            recv_sem=near_recv,
            device_id=(gx, g),
            device_id_type=MESH,
        )

    def mini_copy(side):
        return pltpu.make_async_remote_copy(
            src_ref=mini_out.at[side],
            dst_ref=mini_in.at[side],
            send_sem=sent,
            recv_sem=mini_recv,
            device_id=(gx, gy + 1 if side == 0 else gy - 1),
            device_id_type=MESH,
        )

    def row_copy(t, side):
        buffer, y, row = (
            (from_south, gy + 1, 2 * rows + cols)
            if side == 0
            else (from_north, gy - 1, 2 * rows)
        )
        return pltpu.make_async_remote_copy(
            src_ref=frame_z.at[t, pl.ds(row, cols)],
            dst_ref=buffer.at[t],
            send_sem=sent,
            recv_sem=row_recv.at[t],
            device_id=(gx, y),
            device_id_type=MESH,
        )

    def edge_copy(side):
        return pltpu.make_async_remote_copy(
            src_ref=edge_out.at[side],
            dst_ref=edge_in.at[1 - side],
            send_sem=sent,
            recv_sem=strip_recv,
            device_id=(east_x if side == 0 else west_x, gy),
            device_id_type=MESH,
        )

    def corner_copy(k):
        return pltpu.make_async_remote_copy(
            src_ref=corner_out.at[k],
            dst_ref=corner_in.at[k],
            send_sem=sent,
            recv_sem=strip_recv,
            device_id=(west_x if k < 2 else east_x, gy + 1 if k % 2 == 0 else gy - 1),
            device_id_type=MESH,
        )

    def for_sides(visit):
        pl.when(jnp.logical_not(east_border))(functools.partial(visit, 0))
        pl.when(jnp.logical_not(west_border))(functools.partial(visit, 1))

    def for_corners(visit, sending):
        for k in range(4):
            east = (k < 2) != sending
            north = (k % 2 == 0) == sending
            condition = jnp.logical_not(east_border if east else west_border)
            pl.when(condition & (has_north if north else has_south))(functools.partial(visit, k))

    def for_rows(visit):
        @pl.when(has_north)
        def _():
            visit(0)

        @pl.when(has_south)
        def _():
            visit(1)

    inward = 2 * (rows + cols)
    mid = pl.ds(8, rows)

    def side_cols(side, k):
        return pl.ds(k if side else cols - 1 - k, rows, stride=cols)

    def fill_edges():
        for side in range(2):
            items = [
                frame_z[0, pl.ds(side * rows, rows), :],
                frame_z[0, pl.ds(inward + side * rows, rows), :],
                horiz[side_cols(side, 0), :],
                diag[side_cols(side, 0), :],
            ]
            for k, item in enumerate(items):
                wide[side, k] = jnp.zeros_like(wide[side, k])
                wide[side, k, mid, :] = item
                if k:
                    edge_out[side, k - 1] = item
            for to, first, second in ((0, rows - 1, rows - 2), (1, 0, 1)):
                picks = [(0, first), (0, second), (1, first), (2, first), (3, first)]
                for k, (item, row) in enumerate(picks):
                    mini_out[to, pl.ds(8 * side + k, 1), :] = items[item][row : row + 1]
                next_horiz = horiz[pl.ds(first * cols + (1 if side else cols - 2), 1), :]
                mini_out[to, pl.ds(8 * side + 5, 1), :] = next_horiz
                mini_out[to, pl.ds(8 * side + 6, 2), :] = jnp.zeros((2, levels), jnp.float32)
                corner_out[2 * (1 - side) + to] = jnp.zeros((8, levels), jnp.float32)
                corner_out[2 * (1 - side) + to, pl.ds(0, 1), :] = items[0][first : first + 1]
        beyond[...] = jnp.zeros_like(beyond)

    def fill_packs():
        c0, c1, c2 = edge_cols
        z_edge = frame_z[0, pl.ds(side * rows, rows), :]
        h_edge, d_edge = horiz[c0, :], diag[c0, :]
        z_next = frame_z[0, pl.ds(inward + side * rows, rows), :]
        for k, item in enumerate([z_edge, z_next, h_edge, d_edge]):
            pack[k] = item
        for k, item in enumerate([z_edge, h_edge]):
            near_out[k] = item
            near_pack[k, own, :] = item
        for k, item in enumerate([d_edge, horiz[c1, :]]):
            near_coef[k] = jnp.zeros_like(near_coef[k])
            near_coef[k, own, :] = item

    def send_first(frame):
        frame_z[0] = precondition(frame)
        fill_edges()
        pl.when(border)(fill_packs)
        pl.semaphore_wait(barrier, n_all - 1)

        for_rows(lambda side: mini_copy(side).start())

        @pl.when(gx == 0)
        def _():
            for g in range(1, n_gy, 2):
                far_copy(0, g).start()

        for_sides(lambda side: col_copy(0, side).start())
        for_rows(lambda side: row_copy(0, side).start())
        for_corners(lambda k: corner_copy(k).start(), True)
        for_sides(lambda side: edge_copy(side).start())

        pl.when(border & (gx > 0))(lambda: far_copy(0, gy).start())

    def send_rows(t, frame):
        frame_z[t, pl.ds(2 * rows, 2 * cols), :] = precondition(frame)
        for_rows(lambda side: row_copy(t, side).start())

    def send_far_last():
        for j in sorted(range(n_gy), key=lambda j: abs(2 * j - n_gy)):
            far_copy(1, lax.rem(gy + j, n_gy)).start()

    def send_near():
        for j in range(1, n_gy):
            near_copy(lax.rem(gy + j, n_gy)).start()

    def receive_rows(t):
        wait_cases(lambda sides, beside: beside * cols, row_recv.at[t])

    def receive_cols(t):
        wait_cases(lambda sides, beside: sides * rows, col_recv.at[t // 2])

        def take(side):
            buffer = from_west if side else from_east
            outside[pl.ds(side * rows, rows), :] = buffer[t]
            if t == 0:
                beyond[side, mid, :] = buffer[t]

        for_sides(take)

    col_id = lax.rem(lax.broadcasted_iota(jnp.int32, (cells, levels), 0), cols)
    east_edge = pl.ds(cols - 1, rows, stride=cols)
    west_edge = pl.ds(0, rows, stride=cols)
    south_edge = pl.ds(0, cols)
    north_edge = pl.ds(cells - cols, cols)

    def edge_columns(ref):
        return jnp.concatenate([ref[east_edge, :], ref[west_edge, :]], 0)

    def column_part(z):
        lane = lax.broadcasted_iota(jnp.int32, z.shape, 1)
        up = jnp.where(lane < levels - 1, pltpu.roll(z, levels - 1, 1), 0.0)
        down = jnp.where(lane > 0, pltpu.roll(z, 1, 1), 0.0)
        return vert[...] * (2.0 * z - (up + down))

    def inner_image(z):
        east = jnp.where(col_id < cols - 1, pltpu.roll(z, cells - 1, 0), 0.0)
        west = jnp.where(col_id > 0, pltpu.roll(z, 1, 0), 0.0)
        none = jnp.zeros((cols, levels), jnp.float32)
        north = jnp.concatenate([z[cols:], none], 0)
        south = jnp.concatenate([none, z[:-cols]], 0)
        beside = east + west + north + south
        return diag[...] * z + horiz[...] * (4.0 * z - beside) + column_part(z)

    def product(a, b):
        both = (a * b).reshape(-1, 8, levels)
        return jnp.sum(jnp.sum(both, axis=0), axis=0, keepdims=True)

    tall_id = lax.broadcasted_iota(jnp.int32, (tall, levels), 0)

    def along(w):
        north = jnp.where(tall_id < tall - 1, pltpu.roll(w, tall - 1, 0), 0.0)
        south = jnp.where(tall_id > 0, pltpu.roll(w, 1, 0), 0.0)
        return north + south

    def stencil(w, d, h):
        return d * w + h * (4.0 * w - along(w)) + column_part(w)

    def gather_rows(start, count, pairs):
        def one(y):
            row = edge_rows[table, start + y]
            for dst, src in pairs:
                gathered[dst, pl.ds(y, 1), :] = src[pl.ds(row, 1), :]

        if count <= 64:
            for y in range(count):
                one(y)
        else:

            def body(y, carry):
                one(y)
                return carry

            lax.fori_loop(0, count, body, 0)

    def wait_bytes(ref, sem):
        pltpu.make_async_copy(ref, ref, sem).wait()

    near_rest = pl.ds(0, (n_gy - 1) * rows)
    last = gx == n_gx - 1
    relays = border & jnp.logical_not(last)
    alike = pl.ds(0, n_gy // 2 * rows)

    crosses = last & (lax.rem(gy, 2) == 1)
    crossed = last & (lax.rem(gy, 2) == 0)

    def relay_across():
        wait_bytes(far_pack, far_recv.at[0])
        relay_copy(gy - 1, pl.ds(0, tall)).start()

    def relay():
        wait_bytes(far_pack.at[:, own], far_recv.at[0])
        for j in sorted(range(1, n_gy), key=lambda j: abs(2 * j - n_gy)):
            relay_copy(lax.rem(gy + j, n_gy), own).start()


    def next_to(w):
        return pltpu.roll(w, w.shape[0] - 1, 0) + pltpu.roll(w, 1, 0)

    def strip_image(side, k, z, left, right):
        c = side_cols(side, k)
        return diag[c, :] * z + horiz[c, :] * (4.0 * z - left - right) + column_part(z)

    def look_ahead():
        c1 = edge_cols[1]

        def take(direction, near, far, row):
            for k in range(2):
                near_coef[k, pl.ds(row, 1), :] = mini_in[direction, pl.ds(8 * side + 4 + k, 1), :]
            for k_side in range(2):
                given = mini_in.at[direction]
                wide[k_side, 0, pl.ds(near, 1), :] = given[pl.ds(8 * k_side, 1), :]
                wide[k_side, 0, pl.ds(far, 1), :] = given[pl.ds(8 * k_side + 1, 1), :]
                for k in (1, 2, 3):
                    wide[k_side, k, pl.ds(near, 1), :] = given[pl.ds(8 * k_side + k + 1, 1), :]

        wait_cases(lambda sides, beside: 16 * beside, mini_recv)
        pl.when(has_south)(functools.partial(take, 0, 7, 6, first_row - 1))
        pl.when(has_north)(functools.partial(take, 1, 8 + rows, 9 + rows, first_row + rows))
        z_edge, z_next, h_edge, d_edge = (wide[side, k] for k in range(4))
        v_edge = (
            d_edge * z_edge
            + h_edge * (4.0 * z_edge - z_next - next_to(z_edge))
            + column_part(z_edge)
        )
        beside = next_to(z_next)[8 : 8 + rows] + z_edge[8 : 8 + rows]
        z1 = z_next[8 : 8 + rows]
        z2 = frame_z[0, pl.ds(inward + (2 + side) * rows, rows), :]
        v_next = (
            diag[c1, :] * z1 + horiz[c1, :] * (4.0 * z1 - beside - z2) + column_part(z1)
        )
        z = precondition(jnp.concatenate([v_edge, v_next], 0))
        z_edge, z_next = z[: rows + 16], z[rows + 16 :]
        beside = next_to(z_edge)[8 : 8 + rows] + z_next
        z_edge = z_edge[8 : 8 + rows]
        near_out[2] = z_edge
        near_pack[2, own, :] = z_edge
        h_own, d_own = h_edge[8 : 8 + rows], d_edge[8 : 8 + rows]
        v = d_own * z_edge + h_own * (4.0 * z_edge - beside) + column_part(z_edge)
        pack[4] = precondition(v)
        pl.when(border)(send_far_last)

    def look_across():
        wait_cases(lambda sides, beside: sides * (3 * rows + 8 * beside), strip_recv)

        def take(k):
            row = 8 + rows if k % 2 else 7
            beyond[k // 2, pl.ds(row, 1), :] = corner_in[k, pl.ds(0, 1), :]

        for_corners(take, False)
        images_first = []
        for side in range(2):
            z_edge, z_next, h_edge, d_edge = (wide[side, k] for k in range(4))
            z_out = beyond[side]
            own_edge, own_out = z_edge[8 : 8 + rows], z_out[8 : 8 + rows]
            v_edge = (
                d_edge * z_edge
                + h_edge * (4.0 * z_edge - z_next - z_out - next_to(z_edge))
                + column_part(z_edge)
            )
            z1 = z_next[8 : 8 + rows]
            z2 = frame_z[0, pl.ds(inward + (2 + side) * rows, rows), :]
            v_next = strip_image(side, 1, z1, next_to(z_next)[8 : 8 + rows] + own_edge, z2)
            v_out = (
                edge_in[side, 2] * own_out
                + edge_in[side, 1]
                * (4.0 * own_out - edge_in[side, 0] - own_edge - next_to(z_out)[8 : 8 + rows])
                + column_part(own_out)
            )
            images_first += [v_edge, v_next, v_out]
        z = precondition(jnp.concatenate(images_first, 0))
        second = []
        each = 3 * rows + 16
        for side in range(2):
            part = z[side * each : (side + 1) * each]
            z_edge, z_next, z_out = part[: rows + 16], part[rows + 16 : each - rows], part[each - rows :]
            strip_out[pl.ds(side * rows, rows), :] = z_out
            beside = next_to(z_edge)[8 : 8 + rows]
            second.append(strip_image(side, 0, z_edge[8 : 8 + rows], beside + z_next, z_out))
        frame_z[2, pl.ds(0, 2 * rows), :] = precondition(jnp.concatenate(second, 0))

        def give(side):
            col_copy(2, side).start()
            outside[pl.ds(side * rows, rows), :] = strip_out[pl.ds(side * rows, rows), :]

        for_sides(give)

    def correct_early():
        @pl.when(border)
        def _():
            pl.when(crossed)(lambda: wait_bytes(far_pack, relay_recv))
            pl.when(relays)(lambda: wait_bytes(far_pack.at[:, near_rest], relay_recv))
            wait_bytes(near_pack.at[:, near_rest], near_recv)

        gather_rows(0, tall, [(0, far_pack.at[0]), (1, near_pack.at[0])])
        h_near, d_near = near_pack[1], near_coef[0]
        h_far, d_far = far_pack[2], far_pack[3]
        b_near, b_far = -(h_near * gathered[0]), -(h_far * gathered[1])
        v_far = stencil(far_pack[0], d_far, h_far) - h_far * far_pack[1] + b_far
        w_near = precondition(b_near)
        far = precondition(jnp.concatenate([b_far, v_far], 0), 1)
        w_far = far[:tall]
        strip[0] = b_near
        strip[1] = w_near
        strip[3] = far[tall:]
        strip[4] = near_pack[2] + w_near
        gather_rows(0, tall, [(0, strip.at[3]), (1, strip.at[4])])
        b_near = stencil(w_near, d_near, h_near) - h_near * gathered[0]
        b_far = stencil(w_far, d_far, h_far) - h_far * gathered[1]
        b_next = -(near_coef[1] * w_near)
        near = precondition(jnp.concatenate([b_near, b_next], 0))
        w_edge, w_next = near[:tall], near[tall:]
        strip[3] = b_near
        strip[4] = b_next
        strip[5] = precondition(b_far, 1)
        strip[6] = w_edge
        strip[7] = w_next
        strip[8] = along(w_next)
        strip[9] = stencil(w_edge, d_near, h_near) - h_near * w_next

    def strip_of(ref):
        return jnp.concatenate([ref[c, :] for c in edge_cols], 0)

    def add_to(key, value):
        extra[pl.ds(KEYS.index(key), 1), :] += value

    def correct_two():
        none = jnp.zeros((rows, levels), jnp.float32)
        changes = [
            [strip[0, own, :], none, none],
            [strip[3, own, :], strip[4, own, :], none],
        ]
        before = [strip_of(r0)]
        after = [before[0]]
        for t in range(2):
            old = strip_of(images.at[t])
            new = old + jnp.concatenate(changes[t], 0)
            before.append(old)
            after.append(new)
            for k in range(t + 1):
                images[t, edge_cols[k], :] = new[k * rows : (k + 1) * rows]
        for i, j in KEYS:
            if 0 < j < 3:
                add_to((i, j), product(after[i], after[j]) - product(before[i], before[j]))
        gather_rows(first_row, rows, [(2, strip.at[5])])

    def correct_third():
        c0, c1, c2 = edge_cols
        w_edge, w_next, beside = strip[6, own, :], strip[7, own, :], strip[8, own, :]
        h0, h1 = horiz[c0, :], horiz[c1, :]
        later = diag[c1, :] * w_next + h1 * (4.0 * w_next - beside - w_edge) + column_part(w_next)
        rest = jnp.concatenate([later, -(horiz[c2, :] * w_next)], 0)
        spaces_here = [strip_of(r0), strip_of(images.at[0]), strip_of(images.at[1])]
        old = strip_of(images.at[2])
        new_rest = old[rows:] + rest
        images[2, c1, :] = new_rest[:rows]
        images[2, c2, :] = new_rest[rows:]
        for i, space in enumerate(spaces_here):
            add_to((i, 3), product(space[rows:], rest))
        add_to((3, 3), product(new_rest, new_rest) - product(old, old))
        base = strip[9, own, :] - h0 * gathered[2, pl.ds(0, rows), :]
        wait_bytes(far_last, far_recv.at[1])
        gather_rows(first_row, rows, [(3, far_last)])
        b_edge = base - h0 * gathered[3, pl.ds(0, rows), :]
        new = old[:rows] + b_edge
        images[2, c0, :] = new
        for i, space in enumerate(spaces_here):
            add_to((i, 3), product(space[:rows], b_edge))
        add_to((3, 3), product(new, new))

    wait_count(3 * cells + 2 * levels, load_sem)
    for load in loads[5:]:
        load.wait()
    prepare_weights()
    terms = {}
    spaces = [r0]
    frame = [edge_columns(r0), r0[south_edge, :], r0[north_edge, :]]
    frame += [r0[side_cols(side, k), :] for k in (1, 2) for side in range(2)]
    send_first(jnp.concatenate(frame, 0))
    edge_horiz = edge_columns(horiz)
    for t in range(ITERS):
        image = images.at[t]
        z = precondition(spaces[-1][...])
        fields[t] = z
        newest = len(spaces) - 1
        for i in range(len(spaces)):
            terms[(i, newest)] = product(spaces[i][...], spaces[newest][...])
        image[...] = inner_image(z)
        if t == 0:
            look_ahead()
        if t == 1:
            pl.when(relays)(relay)
            look_across()
        if t == 2:
            pl.when(crosses)(relay_across)
            correct_early()
            pl.when(border)(correct_two)
        receive_rows(t)
        image[south_edge, :] = image[south_edge, :] - horiz[south_edge, :] * from_south[t]
        image[north_edge, :] = image[north_edge, :] - horiz[north_edge, :] * from_north[t]
        inside = edge_columns(image)
        if t != 1:
            receive_cols(t)
        edges = inside - edge_horiz * outside[...]
        image[east_edge, :] = edges[:rows]
        image[west_edge, :] = edges[rows:]
        if t < ITERS - 1:
            send_rows(t + 1, jnp.concatenate([image[south_edge, :], image[north_edge, :]], 0))
        if t == 0:
            pl.when(border)(send_near)
        spaces.append(image)
    newest = len(spaces) - 1
    for i in range(len(spaces)):
        terms[(i, newest)] = product(spaces[i][...], spaces[newest][...])
    for k, key in enumerate(KEYS):
        partial[pl.ds(k, 1), :] = terms[key]

    @pl.when(border)
    def _():
        correct_third()

    height = -(-len(KEYS) // 8) * 8
    row_id = lax.broadcasted_iota(jnp.int32, (height, levels), 0)
    lane = lax.broadcasted_iota(jnp.int32, (height, levels), 1)
    stacked = jnp.where(row_id < len(KEYS), partial[...] + extra[...], 0.0)
    summed = jnp.sum(stacked, axis=1, keepdims=True)
    sums[me] = jnp.sum(jnp.where(lane == row_id, summed, 0.0), axis=0, keepdims=True)

    def tell(x, y):
        pltpu.make_async_remote_copy(
            src_ref=sums.at[me],
            dst_ref=sums.at[me],
            send_sem=sum_sent,
            recv_sem=sum_recv,
            device_id=(x, y),
            device_id_type=MESH,
        ).start()

    for_others(tell)
    def all_sent(sides, beside, border_part):
        per_side = 5 * rows + 8 * beside
        return sides * per_side + beside * (ITERS * cols + 16) + border_part * rows

    common = n_gy + 3 * (n_gy - 1)
    first, inner = gx == 0, border & jnp.logical_not(last | (gx == 0))
    for condition, sides, border_part in (
        (jnp.logical_not(border), 2, 0),
        (first, 1, common + 2 * n_gy + 4 * (n_gy - 1)),
        (inner, 1, common + 4 + 4 * (n_gy - 1)),
        (crosses, 1, common + 4 + 4 * n_gy),
        (crossed, 1, common + 4),
    ):
        for beside, here in ((1, jnp.logical_not(between)), (2, between)):
            pl.when(condition & here)(
                functools.partial(wait_count, all_sent(sides, beside, border_part), sent)
            )

    @pl.when(border)
    def _():
        c0, c1, c2 = edge_cols
        fields[1, c0, :] += strip[1, own, :]
        fields[2, c0, :] += strip[6, own, :]
        fields[2, c1, :] += strip[7, own, :]

    others = sums.at[pl.ds(0, n_all - 1)]
    wait_bytes(others, sum_recv)
    out_totals[...] = jnp.sum(sums[...], axis=0)
    wait_bytes(others, sum_sent)


def finish(
    total_cells, all_totals, r0, fields, images, out_x, out_r, out_norms, x, r, norms_out, sem, norm_sem
):
    levels = r0.shape[-1]
    totals = all_totals[...]
    value = {
        key: jnp.broadcast_to(totals[:, k : k + 1], (8, levels)) for k, key in enumerate(KEYS)
    }

    rho, g0, g1, g2 = value[(0, 0)], value[(0, 1)], value[(0, 2)], value[(0, 3)]
    a00, a01, a02 = value[(1, 1)], value[(1, 2)], value[(1, 3)]
    a11, a12, a22 = value[(2, 2)], value[(2, 3)], value[(3, 3)]
    l10, l20, y0 = a01 / a00, a02 / a00, g0 / a00
    d1, e12, f1 = a11 - l10 * a01, a12 - l10 * a02, g1 - l10 * g0
    l21, y1 = e12 / d1, f1 / d1
    d2, f2 = a22 - l20 * a02 - l21 * e12, g2 - l20 * g0 - l21 * f1
    y2 = f2 / d2
    norm0 = rho - y0 * g0
    norm1 = norm0 - y1 * f1
    norm2 = norm1 - y2 * f2
    y1 = y1 - l21 * y2
    y0 = y0 - l10 * y1 - l20 * y2
    norm_lane = lax.broadcasted_iota(jnp.int32, (8, levels), 1)
    norms = jnp.where(norm_lane == 0, norm0, jnp.where(norm_lane == 1, norm1, norm2))
    norms_out[...] = norms[:1, :ITERS] / total_cells
    copies = [pltpu.make_async_copy(norms_out, out_norms, norm_sem)]
    copies[0].start()
    rows = r0.shape[0]
    pieces = 2 if rows % 16 == 0 else 1
    size = rows // pieces
    y0, y1, y2 = (jnp.tile(y, (size // 8, 1)) for y in (y0, y1, y2))
    for p in range(pieces):
        span = pl.ds(p * size, size)
        x[span] = y0 * fields[0, span] + y1 * fields[1, span] + y2 * fields[2, span]
        r[span] = (
            r0[span] - y0 * images[0, span] - y1 * images[1, span] - y2 * images[2, span]
        )
        for k, (src, dst) in enumerate(((x, out_x), (r, out_r))):
            copy = pltpu.make_async_copy(src.at[span], dst.at[span], sem.at[p, k])
            copy.start()
            copies.append(copy)
    for copy in copies:
        copy.wait()


def on_device(n_gx, n_gy, right_side, diagonal, horizontal, vertical, precond, edge_rows):
    rows, cols, levels = right_side.shape
    f32 = jnp.float32
    block = (rows * cols, levels)
    column = (n_gy * rows, levels)
    sems = pltpu.SemaphoreType.DMA
    meter_rows = 3 * rows * cols + 2 * levels + (16 + 10 * n_gy) * rows + 8 * cols + 64
    basis = pltpu.VMEM((ITERS,) + block, f32)
    fields, images, totals, start = pl.pallas_call(
        functools.partial(kernel, n_gx, n_gy, rows),
        out_shape=(basis, basis, pltpu.VMEM((1, levels), f32), pltpu.VMEM(block, f32)),
        in_specs=[ANY, ANY, ANY, ANY, ANY, ANY],
        out_specs=(VMEM, VMEM, VMEM, VMEM),
        scratch_shapes=[
            pltpu.VMEM(block, f32),
            pltpu.VMEM(block, f32),
            pltpu.VMEM((1, levels), f32),
            pltpu.VMEM((2 * levels, levels), f32),
            pltpu.VMEM((2, 2 * levels, 2 * levels), jnp.bfloat16),
            pltpu.VMEM((ITERS, 6 * rows + 2 * cols, levels), f32),
            pltpu.VMEM((5, rows, levels), f32),
            pltpu.VMEM((3, rows, levels), f32),
            pltpu.VMEM((2,) + column, f32),
            pltpu.VMEM((2, 16, levels), f32),
            pltpu.VMEM((2, 16, levels), f32),
            pltpu.VMEM((2, 4, rows + 16, levels), f32),
            pltpu.VMEM((2, 3, rows, levels), f32),
            pltpu.VMEM((2, 3, rows, levels), f32),
            pltpu.VMEM((4, 8, levels), f32),
            pltpu.VMEM((4, 8, levels), f32),
            pltpu.VMEM((2, rows + 16, levels), f32),
            pltpu.VMEM((ITERS, rows, levels), f32),
            pltpu.VMEM((ITERS, rows, levels), f32),
            pltpu.VMEM((ITERS, cols, levels), f32),
            pltpu.VMEM((ITERS, cols, levels), f32),
            pltpu.VMEM((4,) + column, f32),
            pltpu.VMEM((3,) + column, f32),
            pltpu.VMEM(column, f32),
            pltpu.VMEM((4,) + column, f32),
            pltpu.VMEM((10,) + column, f32),
            pltpu.VMEM((2 * rows, levels), f32),
            pltpu.VMEM((2 * rows, levels), f32),
            pltpu.VMEM((16, levels), f32),
            pltpu.VMEM((16, levels), f32),
            pltpu.VMEM((n_gx * n_gy, 1, levels), f32),
            pltpu.SMEM(edge_rows.shape, jnp.int32),
            pltpu.VMEM((meter_rows, levels), f32),
            sems(()),
            sems((2,)),
            sems(()),
            sems(()),
            sems((2,)),
            sems((ITERS,)),
            sems((2,)),
            sems(()),
            sems(()),
            sems(()),
            sems(()),
            sems(()),
        ],
        compiler_params=pltpu.CompilerParams(collective_id=0, has_side_effects=True),
    )(
        edge_rows,
        right_side.reshape(block),
        diagonal.reshape(block),
        horizontal.reshape(block),
        vertical.reshape(1, levels),
        precond,
    )
    in_vmem = functools.partial(
        pltpu.with_memory_space_constraint, memory_space=pltpu.VMEM
    )
    total_cells = float(rows * cols * levels * n_gx * n_gy)
    x, r, norms = pl.pallas_call(
        functools.partial(finish, total_cells),
        out_shape=(
            jax.ShapeDtypeStruct(block, f32),
            jax.ShapeDtypeStruct(block, f32),
            jax.ShapeDtypeStruct((1, ITERS), f32),
        ),
        in_specs=[VMEM, VMEM, VMEM, VMEM],
        out_specs=(ANY, ANY, ANY),
        scratch_shapes=[
            pltpu.VMEM(block, f32),
            pltpu.VMEM(block, f32),
            pltpu.VMEM((1, ITERS), f32),
            sems((2, 2)),
            sems(()),
        ],
    )(in_vmem(totals), in_vmem(start), in_vmem(fields), in_vmem(images))
    shape = right_side.shape
    return x.reshape(shape), r.reshape(shape), norms.reshape(ITERS)


def solution(mesh):
    n_gx, n_gy = mesh.shape["gx"], mesh.shape["gy"]
    field = P("gy", "gx", None)
    return jax.shard_map(
        functools.partial(on_device, n_gx, n_gy),
        mesh=mesh,
        in_specs=(field, field, field, P(), P(), P()),
        out_specs=(field, field, P()),
        check_vma=False,
    )
```

```python
import functools

import jax
import jax.numpy as jnp
from jax import lax
from jax.experimental import pallas as pl
from jax.experimental.pallas import tpu as pltpu
from jax.sharding import PartitionSpec as P

ITERS = 3
KEYS = [(i, j) for j in range(ITERS + 1) for i in range(j + 1)]
MESH = pl.DeviceIdType.MESH
ANY = pl.BlockSpec(memory_space=pl.ANY)
VMEM = pl.BlockSpec(memory_space=pltpu.VMEM)


def kernel(
    n_gx,
    n_gy,
    out_rows,
    edge_table,
    right_side,
    diagonal,
    horizontal,
    vertical,
    precond,
    fields,
    images,
    out_totals,
    r0,
    diag,
    horiz,
    vert,
    matrix,
    weights,
    frame_z,
    pack,
    near_out,
    near_coef,
    mini_out,
    mini_in,
    wide,
    edge_out,
    edge_in,
    corner_out,
    corner_in,
    beyond,
    from_east,
    from_west,
    from_north,
    from_south,
    far_pack,
    near_pack,
    far_last,
    gathered,
    strip,
    strip_out,
    outside,
    partial,
    extra,
    sums,
    edge_rows,
    meter,
    load_sem,
    small_sem,
    sent,
    sum_sent,
    col_recv,
    row_recv,
    far_recv,
    relay_recv,
    near_recv,
    mini_recv,
    strip_recv,
    sum_recv,
):
    rows, levels = out_rows, r0.shape[-1]
    cells = r0.shape[0]
    cols = cells // rows
    tall = n_gy * rows
    gx, gy = lax.axis_index("gx"), lax.axis_index("gy")
    n_all = n_gx * n_gy
    half = n_gx // 2
    me = gx * n_gy + gy

    def for_others(visit):
        def step(i, carry):
            for j in range(n_gy):
                visit(lax.rem(gx + i, n_gx), lax.rem(gy + j, n_gy))
            return carry

        if n_all <= 64:
            for i in sorted(range(1, n_gx), key=lambda i: min(i, n_gx - i)):
                step(i, 0)
        else:
            lax.fori_loop(1, n_gx, step, 0)
        for j in range(1, n_gy):
            visit(gx, lax.rem(gy + j, n_gy))

    barrier = pltpu.get_barrier_semaphore()

    def greet(x, y):
        pl.semaphore_signal(barrier, inc=1, device_id=(x, y), device_id_type=MESH)

    for_others(greet)

    panel = lax.convert_element_type(gx >= half, jnp.int32)
    loads = [
        pltpu.make_async_copy(right_side, r0, load_sem),
        pltpu.make_async_copy(precond.at[panel], matrix.at[pl.ds(0, levels)], load_sem),
        pltpu.make_async_copy(horizontal, horiz, load_sem),
        pltpu.make_async_copy(diagonal, diag, load_sem),
        pltpu.make_async_copy(precond.at[1 - panel], matrix.at[pl.ds(levels, levels)], load_sem),
        pltpu.make_async_copy(vertical, vert, small_sem.at[0]),
        pltpu.make_async_copy(edge_table, edge_rows, small_sem.at[1]),
    ]
    for load in loads:
        load.start()

    east_x, west_x = lax.rem(gx + 1, n_gx), lax.rem(gx + n_gx - 1, n_gx)
    east_border = (gx == half - 1) | (gx == n_gx - 1)
    west_border = (gx == half) | (gx == 0)
    border = east_border | west_border
    far_x = jnp.where(east_border, east_x, west_x)
    side = jnp.where(east_border, 0, 1)
    table = jnp.where((gx == half - 1) | (gx == half), 0, 1)
    edge_cols = [
        pl.ds(jnp.where(east_border, cols - 1 - i, i), rows, stride=cols) for i in range(3)
    ]
    first_row = pl.multiple_of(gy * rows, rows)
    own = pl.ds(first_row, rows)
    has_north, has_south = gy < n_gy - 1, gy > 0
    between = has_north & has_south

    def wait_count(count, sem):
        part = meter.at[pl.ds(0, count)]
        pltpu.make_async_copy(part, part, sem).wait()

    def wait_cases(count, sem):
        for n_sides, on_border in ((1, border), (2, jnp.logical_not(border))):
            for n_rows, here in ((1, jnp.logical_not(between)), (2, between)):
                pl.when(on_border & here)(
                    functools.partial(wait_count, count(n_sides, n_rows), sem)
                )

    @pl.when(jnp.logical_not(has_north))
    def _():
        from_north[...] = jnp.zeros_like(from_north)

    @pl.when(jnp.logical_not(has_south))
    def _():
        from_south[...] = jnp.zeros_like(from_south)

    outside[...] = jnp.zeros_like(outside)
    extra[...] = jnp.zeros_like(extra)

    def split(v):
        high = v.astype(jnp.bfloat16)
        return high, (v - high.astype(jnp.float32)).astype(jnp.bfloat16)

    def prepare_weights(which):
        turned = jnp.transpose(matrix[pl.ds(which * levels, levels), :])
        for part, value in enumerate(split(turned)):
            for twice in range(2):
                weights[
                    which, pl.ds(twice * levels, levels), pl.ds(part * levels, levels)
                ] = value

    def precondition(v, which=0):
        out = lax.dot_general(
            jnp.concatenate(split(v), 1),
            weights[which],
            (((1,), (0,)), ((), ())),
            preferred_element_type=jnp.float32,
        )
        return out[:, :levels] + out[:, levels:]

    def col_copy(t, side):
        buffer, x = (from_west, east_x) if side == 0 else (from_east, west_x)
        return pltpu.make_async_remote_copy(
            src_ref=frame_z.at[t, pl.ds(side * rows, rows)],
            dst_ref=buffer.at[t],
            send_sem=sent,
            recv_sem=col_recv.at[t // 2],
            device_id=(x, gy),
            device_id_type=MESH,
        )

    def far_copy(t, g):
        return pltpu.make_async_remote_copy(
            src_ref=pack.at[pl.ds(0, 4)] if t == 0 else pack.at[4],
            dst_ref=far_pack.at[:, own] if t == 0 else far_last.at[own],
            send_sem=sent,
            recv_sem=far_recv.at[t],
            device_id=(far_x, g),
            device_id_type=MESH,
        )

    def relay_copy(g, block):
        return pltpu.make_async_remote_copy(
            src_ref=far_pack.at[:, block],
            dst_ref=far_pack.at[:, block],
            send_sem=sent,
            recv_sem=relay_recv,
            device_id=(gx, g),
            device_id_type=MESH,
        )

    def near_copy(g):
        return pltpu.make_async_remote_copy(
            src_ref=near_out,
            dst_ref=near_pack.at[:, own],
            send_sem=sent,
            recv_sem=near_recv,
            device_id=(gx, g),
            device_id_type=MESH,
        )

    def mini_copy(side):
        return pltpu.make_async_remote_copy(
            src_ref=mini_out.at[side],
            dst_ref=mini_in.at[side],
            send_sem=sent,
            recv_sem=mini_recv,
            device_id=(gx, gy + 1 if side == 0 else gy - 1),
            device_id_type=MESH,
        )

    def row_copy(t, side):
        buffer, y, row = (
            (from_south, gy + 1, 2 * rows + cols)
            if side == 0
            else (from_north, gy - 1, 2 * rows)
        )
        return pltpu.make_async_remote_copy(
            src_ref=frame_z.at[t, pl.ds(row, cols)],
            dst_ref=buffer.at[t],
            send_sem=sent,
            recv_sem=row_recv.at[t],
            device_id=(gx, y),
            device_id_type=MESH,
        )

    def edge_copy(side):
        return pltpu.make_async_remote_copy(
            src_ref=edge_out.at[side],
            dst_ref=edge_in.at[1 - side],
            send_sem=sent,
            recv_sem=strip_recv,
            device_id=(east_x if side == 0 else west_x, gy),
            device_id_type=MESH,
        )

    def corner_copy(k):
        return pltpu.make_async_remote_copy(
            src_ref=corner_out.at[k],
            dst_ref=corner_in.at[k],
            send_sem=sent,
            recv_sem=strip_recv,
            device_id=(west_x if k < 2 else east_x, gy + 1 if k % 2 == 0 else gy - 1),
            device_id_type=MESH,
        )

    def for_sides(visit):
        pl.when(jnp.logical_not(east_border))(functools.partial(visit, 0))
        pl.when(jnp.logical_not(west_border))(functools.partial(visit, 1))

    def for_corners(visit, sending):
        for k in range(4):
            east = (k < 2) != sending
            north = (k % 2 == 0) == sending
            condition = jnp.logical_not(east_border if east else west_border)
            pl.when(condition & (has_north if north else has_south))(functools.partial(visit, k))

    def for_rows(visit):
        @pl.when(has_north)
        def _():
            visit(0)

        @pl.when(has_south)
        def _():
            visit(1)

    inward = 2 * (rows + cols)
    mid = pl.ds(8, rows)

    def side_cols(side, k):
        return pl.ds(k if side else cols - 1 - k, rows, stride=cols)

    def fill_edges():
        for side in range(2):
            items = [
                frame_z[0, pl.ds(side * rows, rows), :],
                frame_z[0, pl.ds(inward + side * rows, rows), :],
                horiz[side_cols(side, 0), :],
                diag[side_cols(side, 0), :],
            ]
            for k, item in enumerate(items):
                wide[side, k] = jnp.zeros_like(wide[side, k])
                wide[side, k, mid, :] = item
                if k:
                    edge_out[side, k - 1] = item
            for to, first, second in ((0, rows - 1, rows - 2), (1, 0, 1)):
                picks = [(0, first), (0, second), (1, first), (2, first), (3, first)]
                for k, (item, row) in enumerate(picks):
                    mini_out[to, pl.ds(8 * side + k, 1), :] = items[item][row : row + 1]
                next_horiz = horiz[pl.ds(first * cols + (1 if side else cols - 2), 1), :]
                mini_out[to, pl.ds(8 * side + 5, 1), :] = next_horiz
                mini_out[to, pl.ds(8 * side + 6, 2), :] = jnp.zeros((2, levels), jnp.float32)
                corner_out[2 * (1 - side) + to] = jnp.zeros((8, levels), jnp.float32)
                corner_out[2 * (1 - side) + to, pl.ds(0, 1), :] = items[0][first : first + 1]
        beyond[...] = jnp.zeros_like(beyond)

    def fill_packs():
        c0, c1, c2 = edge_cols
        z_edge = frame_z[0, pl.ds(side * rows, rows), :]
        h_edge, d_edge = horiz[c0, :], diag[c0, :]
        z_next = frame_z[0, pl.ds(inward + side * rows, rows), :]
        for k, item in enumerate([z_edge, z_next, h_edge, d_edge]):
            pack[k] = item
        for k, item in enumerate([z_edge, h_edge]):
            near_out[k] = item
            near_pack[k, own, :] = item
        for k, item in enumerate([d_edge, horiz[c1, :]]):
            near_coef[k] = jnp.zeros_like(near_coef[k])
            near_coef[k, own, :] = item

    def send_first(frame):
        frame_z[0] = precondition(frame)
        fill_edges()
        pl.when(border)(fill_packs)
        pl.semaphore_wait(barrier, n_all - 1)

        for_rows(lambda side: mini_copy(side).start())

        pl.when(gx == 0)(send_far_pack)
        for_sides(lambda side: col_copy(0, side).start())
        for_rows(lambda side: row_copy(0, side).start())
        for_corners(lambda k: corner_copy(k).start(), True)
        for_sides(lambda side: edge_copy(side).start())

        pl.when(border & (gx > 0))(send_far_pack)

    def send_rows(t, frame):
        frame_z[t, pl.ds(2 * rows, 2 * cols), :] = precondition(frame)
        for_rows(lambda side: row_copy(t, side).start())

    def send_far_pack():
        for g in range(1, n_gy, 2):
            far_copy(0, g).start()

    def send_far_last():
        for g in sorted(range(n_gy), key=lambda g: g % 2):
            far_copy(1, g).start()

    def send_near():
        for j in range(1, n_gy):
            near_copy(lax.rem(gy + j, n_gy)).start()

    def receive_rows(t):
        wait_cases(lambda sides, beside: beside * cols, row_recv.at[t])

    def receive_cols(t):
        wait_cases(lambda sides, beside: sides * rows, col_recv.at[t // 2])

        def take(side):
            buffer = from_west if side else from_east
            outside[pl.ds(side * rows, rows), :] = buffer[t]
            if t == 0:
                beyond[side, mid, :] = buffer[t]

        for_sides(take)

    col_id = lax.rem(lax.broadcasted_iota(jnp.int32, (cells, levels), 0), cols)
    east_edge = pl.ds(cols - 1, rows, stride=cols)
    west_edge = pl.ds(0, rows, stride=cols)
    south_edge = pl.ds(0, cols)
    north_edge = pl.ds(cells - cols, cols)

    def edge_columns(ref):
        return jnp.concatenate([ref[east_edge, :], ref[west_edge, :]], 0)

    def column_part(z):
        lane = lax.broadcasted_iota(jnp.int32, z.shape, 1)
        up = jnp.where(lane < levels - 1, pltpu.roll(z, levels - 1, 1), 0.0)
        down = jnp.where(lane > 0, pltpu.roll(z, 1, 1), 0.0)
        return vert[...] * (2.0 * z - (up + down))

    def inner_image(z):
        east = jnp.where(col_id < cols - 1, pltpu.roll(z, cells - 1, 0), 0.0)
        west = jnp.where(col_id > 0, pltpu.roll(z, 1, 0), 0.0)
        none = jnp.zeros((cols, levels), jnp.float32)
        north = jnp.concatenate([z[cols:], none], 0)
        south = jnp.concatenate([none, z[:-cols]], 0)
        beside = east + west + north + south
        return diag[...] * z + horiz[...] * (4.0 * z - beside) + column_part(z)

    def product(a, b):
        both = (a * b).reshape(-1, 8, levels)
        return jnp.sum(jnp.sum(both, axis=0), axis=0, keepdims=True)

    tall_id = lax.broadcasted_iota(jnp.int32, (tall, levels), 0)

    def along(w):
        north = jnp.where(tall_id < tall - 1, pltpu.roll(w, tall - 1, 0), 0.0)
        south = jnp.where(tall_id > 0, pltpu.roll(w, 1, 0), 0.0)
        return north + south

    def stencil(w, d, h):
        return d * w + h * (4.0 * w - along(w)) + column_part(w)

    def gather_rows(start, count, pairs):
        def one(y):
            row = edge_rows[table, start + y]
            for dst, src in pairs:
                gathered[dst, pl.ds(y, 1), :] = src[pl.ds(row, 1), :]

        if count <= 64:
            for y in range(count):
                one(y)
        else:

            def body(y, carry):
                one(y)
                return carry

            lax.fori_loop(0, count, body, 0)

    def wait_bytes(ref, sem):
        pltpu.make_async_copy(ref, ref, sem).wait()

    near_rest = pl.ds(0, (n_gy - 1) * rows)
    last = gx == n_gx - 1
    crosses = border & (lax.rem(gy, 2) == 1)
    crossed = border & (lax.rem(gy, 2) == 0)

    def relay_across():
        wait_bytes(far_pack, far_recv.at[0])
        relay_copy(gy - 1, pl.ds(0, tall)).start()

    def next_to(w):
        return pltpu.roll(w, w.shape[0] - 1, 0) + pltpu.roll(w, 1, 0)

    def strip_image(side, k, z, left, right):
        c = side_cols(side, k)
        return diag[c, :] * z + horiz[c, :] * (4.0 * z - left - right) + column_part(z)

    def look_ahead():
        c1 = edge_cols[1]

        def take(direction, near, far, row):
            for k in range(2):
                near_coef[k, pl.ds(row, 1), :] = mini_in[direction, pl.ds(8 * side + 4 + k, 1), :]
            for k_side in range(2):
                given = mini_in.at[direction]
                wide[k_side, 0, pl.ds(near, 1), :] = given[pl.ds(8 * k_side, 1), :]
                wide[k_side, 0, pl.ds(far, 1), :] = given[pl.ds(8 * k_side + 1, 1), :]
                for k in (1, 2, 3):
                    wide[k_side, k, pl.ds(near, 1), :] = given[pl.ds(8 * k_side + k + 1, 1), :]

        wait_cases(lambda sides, beside: 16 * beside, mini_recv)
        pl.when(has_south)(functools.partial(take, 0, 7, 6, first_row - 1))
        pl.when(has_north)(functools.partial(take, 1, 8 + rows, 9 + rows, first_row + rows))
        z_edge, z_next, h_edge, d_edge = (wide[side, k] for k in range(4))
        v_edge = (
            d_edge * z_edge
            + h_edge * (4.0 * z_edge - z_next - next_to(z_edge))
            + column_part(z_edge)
        )
        beside = next_to(z_next)[8 : 8 + rows] + z_edge[8 : 8 + rows]
        z1 = z_next[8 : 8 + rows]
        z2 = frame_z[0, pl.ds(inward + (2 + side) * rows, rows), :]
        v_next = (
            diag[c1, :] * z1 + horiz[c1, :] * (4.0 * z1 - beside - z2) + column_part(z1)
        )
        z = precondition(jnp.concatenate([v_edge, v_next], 0))
        z_edge, z_next = z[: rows + 16], z[rows + 16 :]
        beside = next_to(z_edge)[8 : 8 + rows] + z_next
        z_edge = z_edge[8 : 8 + rows]
        near_out[2] = z_edge
        near_pack[2, own, :] = z_edge
        h_own, d_own = h_edge[8 : 8 + rows], d_edge[8 : 8 + rows]
        v = d_own * z_edge + h_own * (4.0 * z_edge - beside) + column_part(z_edge)
        pack[4] = precondition(v)
        pl.when(border)(send_far_last)

    def look_across():
        wait_cases(lambda sides, beside: sides * (3 * rows + 8 * beside), strip_recv)

        def take(k):
            row = 8 + rows if k % 2 else 7
            beyond[k // 2, pl.ds(row, 1), :] = corner_in[k, pl.ds(0, 1), :]

        for_corners(take, False)
        images_first = []
        for side in range(2):
            z_edge, z_next, h_edge, d_edge = (wide[side, k] for k in range(4))
            z_out = beyond[side]
            own_edge, own_out = z_edge[8 : 8 + rows], z_out[8 : 8 + rows]
            v_edge = (
                d_edge * z_edge
                + h_edge * (4.0 * z_edge - z_next - z_out - next_to(z_edge))
                + column_part(z_edge)
            )
            z1 = z_next[8 : 8 + rows]
            z2 = frame_z[0, pl.ds(inward + (2 + side) * rows, rows), :]
            v_next = strip_image(side, 1, z1, next_to(z_next)[8 : 8 + rows] + own_edge, z2)
            v_out = (
                edge_in[side, 2] * own_out
                + edge_in[side, 1]
                * (4.0 * own_out - edge_in[side, 0] - own_edge - next_to(z_out)[8 : 8 + rows])
                + column_part(own_out)
            )
            images_first += [v_edge, v_next, v_out]
        z = precondition(jnp.concatenate(images_first, 0))
        second = []
        each = 3 * rows + 16
        for side in range(2):
            part = z[side * each : (side + 1) * each]
            z_edge, z_next, z_out = part[: rows + 16], part[rows + 16 : each - rows], part[each - rows :]
            strip_out[pl.ds(side * rows, rows), :] = z_out
            beside = next_to(z_edge)[8 : 8 + rows]
            second.append(strip_image(side, 0, z_edge[8 : 8 + rows], beside + z_next, z_out))
        frame_z[2, pl.ds(0, 2 * rows), :] = precondition(jnp.concatenate(second, 0))

        def give(side):
            col_copy(2, side).start()
            outside[pl.ds(side * rows, rows), :] = strip_out[pl.ds(side * rows, rows), :]

        for_sides(give)

    def correct_early():
        pl.when(border)(lambda: wait_bytes(near_pack.at[:, near_rest], near_recv))
        gather_rows(0, tall, [(1, near_pack.at[0])])

        @pl.when(border)
        def _():
            pl.when(crossed)(lambda: wait_bytes(far_pack, relay_recv))
        gather_rows(0, tall, [(0, far_pack.at[0])])
        h_near, d_near = near_pack[1], near_coef[0]
        h_far, d_far = far_pack[2], far_pack[3]
        b_near, b_far = -(h_near * gathered[0]), -(h_far * gathered[1])
        v_far = stencil(far_pack[0], d_far, h_far) - h_far * far_pack[1] + b_far
        w_near = precondition(b_near)
        far = precondition(jnp.concatenate([b_far, v_far], 0), 1)
        w_far = far[:tall]
        strip[0] = b_near
        strip[1] = w_near
        strip[3] = far[tall:]
        strip[4] = near_pack[2] + w_near
        gather_rows(0, tall, [(0, strip.at[3]), (1, strip.at[4])])
        b_near = stencil(w_near, d_near, h_near) - h_near * gathered[0]
        b_far = stencil(w_far, d_far, h_far) - h_far * gathered[1]
        b_next = -(near_coef[1] * w_near)
        near = precondition(jnp.concatenate([b_near, b_next], 0))
        w_edge, w_next = near[:tall], near[tall:]
        strip[3] = b_near
        strip[4] = b_next
        strip[5] = precondition(b_far, 1)
        strip[6] = w_edge
        strip[7] = w_next
        strip[8] = along(w_next)
        strip[9] = stencil(w_edge, d_near, h_near) - h_near * w_next

    def strip_of(ref):
        return jnp.concatenate([ref[c, :] for c in edge_cols], 0)

    def add_to(key, value):
        extra[pl.ds(KEYS.index(key), 1), :] += value

    def correct_two():
        none = jnp.zeros((rows, levels), jnp.float32)
        changes = [
            [strip[0, own, :], none, none],
            [strip[3, own, :], strip[4, own, :], none],
        ]
        before = [strip_of(r0)]
        after = [before[0]]
        for t in range(2):
            old = strip_of(images.at[t])
            new = old + jnp.concatenate(changes[t], 0)
            before.append(old)
            after.append(new)
            for k in range(t + 1):
                images[t, edge_cols[k], :] = new[k * rows : (k + 1) * rows]
        for i, j in KEYS:
            if 0 < j < 3:
                add_to((i, j), product(after[i], after[j]) - product(before[i], before[j]))
        gather_rows(first_row, rows, [(2, strip.at[5])])

    def correct_third():
        c0, c1, c2 = edge_cols
        w_edge, w_next, beside = strip[6, own, :], strip[7, own, :], strip[8, own, :]
        h0, h1 = horiz[c0, :], horiz[c1, :]
        later = diag[c1, :] * w_next + h1 * (4.0 * w_next - beside - w_edge) + column_part(w_next)
        rest = jnp.concatenate([later, -(horiz[c2, :] * w_next)], 0)
        spaces_here = [strip_of(r0), strip_of(images.at[0]), strip_of(images.at[1])]
        old = strip_of(images.at[2])
        new_rest = old[rows:] + rest
        images[2, c1, :] = new_rest[:rows]
        images[2, c2, :] = new_rest[rows:]
        for i, space in enumerate(spaces_here):
            add_to((i, 3), product(space[rows:], rest))
        add_to((3, 3), product(new_rest, new_rest) - product(old, old))
        base = strip[9, own, :] - h0 * gathered[2, pl.ds(0, rows), :]
        wait_bytes(far_last, far_recv.at[1])
        gather_rows(first_row, rows, [(3, far_last)])
        b_edge = base - h0 * gathered[3, pl.ds(0, rows), :]
        new = old[:rows] + b_edge
        images[2, c0, :] = new
        for i, space in enumerate(spaces_here):
            add_to((i, 3), product(space[:rows], b_edge))
        add_to((3, 3), product(new, new))

    wait_count(3 * cells + 2 * levels, load_sem)
    for load in loads[5:]:
        load.wait()
    prepare_weights(0)
    terms = {}
    spaces = [r0]
    frame = [edge_columns(r0), r0[south_edge, :], r0[north_edge, :]]
    frame += [r0[side_cols(side, k), :] for k in (1, 2) for side in range(2)]
    send_first(jnp.concatenate(frame, 0))
    edge_horiz = edge_columns(horiz)
    for t in range(ITERS):
        image = images.at[t]
        z = precondition(spaces[-1][...])
        fields[t] = z
        newest = len(spaces) - 1
        for i in range(len(spaces)):
            terms[(i, newest)] = product(spaces[i][...], spaces[newest][...])
        image[...] = inner_image(z)
        if t == 0:
            prepare_weights(1)
            look_ahead()
            pl.when(border & jnp.logical_not(last))(send_near)
        if t == 1:
            look_across()
        if t == 2:
            pl.when(crosses)(relay_across)
            correct_early()
            pl.when(border)(correct_two)
        receive_rows(t)
        image[south_edge, :] = image[south_edge, :] - horiz[south_edge, :] * from_south[t]
        image[north_edge, :] = image[north_edge, :] - horiz[north_edge, :] * from_north[t]
        inside = edge_columns(image)
        if t != 1:
            receive_cols(t)
        edges = inside - edge_horiz * outside[...]
        image[east_edge, :] = edges[:rows]
        image[west_edge, :] = edges[rows:]
        if t < ITERS - 1:
            send_rows(t + 1, jnp.concatenate([image[south_edge, :], image[north_edge, :]], 0))
        if t == 0:
            pl.when(last)(send_near)
        spaces.append(image)
    newest = len(spaces) - 1
    for i in range(len(spaces)):
        terms[(i, newest)] = product(spaces[i][...], spaces[newest][...])
    for k, key in enumerate(KEYS):
        partial[pl.ds(k, 1), :] = terms[key]

    @pl.when(border)
    def _():
        correct_third()

    height = -(-len(KEYS) // 8) * 8
    row_id = lax.broadcasted_iota(jnp.int32, (height, levels), 0)
    lane = lax.broadcasted_iota(jnp.int32, (height, levels), 1)
    stacked = jnp.where(row_id < len(KEYS), partial[...] + extra[...], 0.0)
    summed = jnp.sum(stacked, axis=1, keepdims=True)
    sums[me] = jnp.sum(jnp.where(lane == row_id, summed, 0.0), axis=0, keepdims=True)

    def tell(x, y):
        pltpu.make_async_remote_copy(
            src_ref=sums.at[me],
            dst_ref=sums.at[me],
            send_sem=sum_sent,
            recv_sem=sum_recv,
            device_id=(x, y),
            device_id_type=MESH,
        ).start()

    def tell_all(x, carry):
        for y in range(n_gy):
            pl.when(me != x * n_gy + y)(functools.partial(tell, x, y))
        return carry

    if n_all <= 64:
        for x in range(n_gx):
            tell_all(x, 0)
    else:
        lax.fori_loop(0, n_gx, tell_all, 0)
    def all_sent(sides, beside, border_part):
        per_side = 5 * rows + 8 * beside
        return sides * per_side + beside * (ITERS * cols + 16) + border_part * rows

    common = n_gy + 3 * (n_gy - 1) + 2 * n_gy
    for condition, sides, border_part in (
        (jnp.logical_not(border), 2, 0),
        (crosses, 1, common + 4 * n_gy),
        (crossed, 1, common),
    ):
        for beside, here in ((1, jnp.logical_not(between)), (2, between)):
            pl.when(condition & here)(
                functools.partial(wait_count, all_sent(sides, beside, border_part), sent)
            )

    @pl.when(border)
    def _():
        c0, c1, c2 = edge_cols
        fields[1, c0, :] += strip[1, own, :]
        fields[2, c0, :] += strip[6, own, :]
        fields[2, c1, :] += strip[7, own, :]

    others = sums.at[pl.ds(0, n_all - 1)]
    wait_bytes(others, sum_recv)
    out_totals[...] = jnp.sum(sums[...], axis=0)
    wait_bytes(others, sum_sent)


def finish(
    total_cells, all_totals, r0, fields, images, out_x, out_r, out_norms, x, r, norms_out, sem, norm_sem
):
    levels = r0.shape[-1]
    totals = all_totals[...]
    value = {
        key: jnp.broadcast_to(totals[:, k : k + 1], (8, levels)) for k, key in enumerate(KEYS)
    }

    rho, g0, g1, g2 = value[(0, 0)], value[(0, 1)], value[(0, 2)], value[(0, 3)]
    a00, a01, a02 = value[(1, 1)], value[(1, 2)], value[(1, 3)]
    a11, a12, a22 = value[(2, 2)], value[(2, 3)], value[(3, 3)]
    l10, l20, y0 = a01 / a00, a02 / a00, g0 / a00
    d1, e12, f1 = a11 - l10 * a01, a12 - l10 * a02, g1 - l10 * g0
    l21, y1 = e12 / d1, f1 / d1
    d2, f2 = a22 - l20 * a02 - l21 * e12, g2 - l20 * g0 - l21 * f1
    y2 = f2 / d2
    norm0 = rho - y0 * g0
    norm1 = norm0 - y1 * f1
    norm2 = norm1 - y2 * f2
    y1 = y1 - l21 * y2
    y0 = y0 - l10 * y1 - l20 * y2
    norm_lane = lax.broadcasted_iota(jnp.int32, (8, levels), 1)
    norms = jnp.where(norm_lane == 0, norm0, jnp.where(norm_lane == 1, norm1, norm2))
    norms_out[...] = norms[:1, :ITERS] / total_cells
    copies = [pltpu.make_async_copy(norms_out, out_norms, norm_sem)]
    copies[0].start()
    rows = r0.shape[0]
    pieces = 2 if rows % 16 == 0 else 1
    size = rows // pieces
    y0, y1, y2 = (jnp.tile(y, (size // 8, 1)) for y in (y0, y1, y2))
    for p in range(pieces):
        span = pl.ds(p * size, size)
        x[span] = y0 * fields[0, span] + y1 * fields[1, span] + y2 * fields[2, span]
        r[span] = (
            r0[span] - y0 * images[0, span] - y1 * images[1, span] - y2 * images[2, span]
        )
        for k, (src, dst) in enumerate(((x, out_x), (r, out_r))):
            copy = pltpu.make_async_copy(src.at[span], dst.at[span], sem.at[p, k])
            copy.start()
            copies.append(copy)
    for copy in copies:
        copy.wait()


def on_device(n_gx, n_gy, right_side, diagonal, horizontal, vertical, precond, edge_rows):
    rows, cols, levels = right_side.shape
    f32 = jnp.float32
    block = (rows * cols, levels)
    column = (n_gy * rows, levels)
    sems = pltpu.SemaphoreType.DMA
    meter_rows = 3 * rows * cols + 2 * levels + (16 + 10 * n_gy) * rows + 8 * cols + 64
    basis = pltpu.VMEM((ITERS,) + block, f32)
    fields, images, totals, start = pl.pallas_call(
        functools.partial(kernel, n_gx, n_gy, rows),
        out_shape=(basis, basis, pltpu.VMEM((1, levels), f32), pltpu.VMEM(block, f32)),
        in_specs=[ANY, ANY, ANY, ANY, ANY, ANY],
        out_specs=(VMEM, VMEM, VMEM, VMEM),
        scratch_shapes=[
            pltpu.VMEM(block, f32),
            pltpu.VMEM(block, f32),
            pltpu.VMEM((1, levels), f32),
            pltpu.VMEM((2 * levels, levels), f32),
            pltpu.VMEM((2, 2 * levels, 2 * levels), jnp.bfloat16),
            pltpu.VMEM((ITERS, 6 * rows + 2 * cols, levels), f32),
            pltpu.VMEM((5, rows, levels), f32),
            pltpu.VMEM((3, rows, levels), f32),
            pltpu.VMEM((2,) + column, f32),
            pltpu.VMEM((2, 16, levels), f32),
            pltpu.VMEM((2, 16, levels), f32),
            pltpu.VMEM((2, 4, rows + 16, levels), f32),
            pltpu.VMEM((2, 3, rows, levels), f32),
            pltpu.VMEM((2, 3, rows, levels), f32),
            pltpu.VMEM((4, 8, levels), f32),
            pltpu.VMEM((4, 8, levels), f32),
            pltpu.VMEM((2, rows + 16, levels), f32),
            pltpu.VMEM((ITERS, rows, levels), f32),
            pltpu.VMEM((ITERS, rows, levels), f32),
            pltpu.VMEM((ITERS, cols, levels), f32),
            pltpu.VMEM((ITERS, cols, levels), f32),
            pltpu.VMEM((4,) + column, f32),
            pltpu.VMEM((3,) + column, f32),
            pltpu.VMEM(column, f32),
            pltpu.VMEM((4,) + column, f32),
            pltpu.VMEM((10,) + column, f32),
            pltpu.VMEM((2 * rows, levels), f32),
            pltpu.VMEM((2 * rows, levels), f32),
            pltpu.VMEM((16, levels), f32),
            pltpu.VMEM((16, levels), f32),
            pltpu.VMEM((n_gx * n_gy, 1, levels), f32),
            pltpu.SMEM(edge_rows.shape, jnp.int32),
            pltpu.VMEM((meter_rows, levels), f32),
            sems(()),
            sems((2,)),
            sems(()),
            sems(()),
            sems((2,)),
            sems((ITERS,)),
            sems((2,)),
            sems(()),
            sems(()),
            sems(()),
            sems(()),
            sems(()),
        ],
        compiler_params=pltpu.CompilerParams(collective_id=0, has_side_effects=True),
    )(
        edge_rows,
        right_side.reshape(block),
        diagonal.reshape(block),
        horizontal.reshape(block),
        vertical.reshape(1, levels),
        precond,
    )
    in_vmem = functools.partial(
        pltpu.with_memory_space_constraint, memory_space=pltpu.VMEM
    )
    total_cells = float(rows * cols * levels * n_gx * n_gy)
    x, r, norms = pl.pallas_call(
        functools.partial(finish, total_cells),
        out_shape=(
            jax.ShapeDtypeStruct(block, f32),
            jax.ShapeDtypeStruct(block, f32),
            jax.ShapeDtypeStruct((1, ITERS), f32),
        ),
        in_specs=[VMEM, VMEM, VMEM, VMEM],
        out_specs=(ANY, ANY, ANY),
        scratch_shapes=[
            pltpu.VMEM(block, f32),
            pltpu.VMEM(block, f32),
            pltpu.VMEM((1, ITERS), f32),
            sems((2, 2)),
            sems(()),
        ],
    )(in_vmem(totals), in_vmem(start), in_vmem(fields), in_vmem(images))
    shape = right_side.shape
    return x.reshape(shape), r.reshape(shape), norms.reshape(ITERS)


def solution(mesh):
    n_gx, n_gy = mesh.shape["gx"], mesh.shape["gy"]
    field = P("gy", "gx", None)
    return jax.shard_map(
        functools.partial(on_device, n_gx, n_gy),
        mesh=mesh,
        in_specs=(field, field, field, P(), P(), P()),
        out_specs=(field, field, P()),
        check_vma=False,
    )
```

```python
import functools

import jax
import jax.numpy as jnp
from jax import lax
from jax.experimental import pallas as pl
from jax.experimental.pallas import tpu as pltpu
from jax.sharding import PartitionSpec as P

ITERS = 3
KEYS = [(i, j) for j in range(ITERS + 1) for i in range(j + 1)]
MESH = pl.DeviceIdType.MESH
ANY = pl.BlockSpec(memory_space=pl.ANY)
VMEM = pl.BlockSpec(memory_space=pltpu.VMEM)


def kernel(
    n_gx,
    n_gy,
    out_rows,
    edge_table,
    right_side,
    diagonal,
    horizontal,
    vertical,
    precond,
    fields,
    images,
    out_totals,
    r0,
    diag,
    horiz,
    vert,
    matrix,
    weights,
    frame_z,
    pack,
    near_out,
    near_coef,
    mini_out,
    mini_in,
    wide,
    edge_out,
    edge_in,
    corner_out,
    corner_in,
    beyond,
    from_east,
    from_west,
    from_north,
    from_south,
    far_pack,
    near_pack,
    far_last,
    gathered,
    strip,
    strip_out,
    outside,
    partial,
    extra,
    sums,
    edge_rows,
    meter,
    load_sem,
    small_sem,
    sent,
    sum_sent,
    col_recv,
    row_recv,
    far_recv,
    relay_recv,
    near_recv,
    mini_recv,
    strip_recv,
    sum_recv,
):
    rows, levels = out_rows, r0.shape[-1]
    cells = r0.shape[0]
    cols = cells // rows
    tall = n_gy * rows
    gx, gy = lax.axis_index("gx"), lax.axis_index("gy")
    n_all = n_gx * n_gy
    half = n_gx // 2
    me = gx * n_gy + gy

    def for_others(visit):
        def step(i, carry):
            for j in range(n_gy):
                visit(lax.rem(gx + i, n_gx), lax.rem(gy + j, n_gy))
            return carry

        if n_all <= 64:
            for i in sorted(range(1, n_gx), key=lambda i: min(i, n_gx - i)):
                step(i, 0)
        else:
            lax.fori_loop(1, n_gx, step, 0)
        for j in range(1, n_gy):
            visit(gx, lax.rem(gy + j, n_gy))

    barrier = pltpu.get_barrier_semaphore()

    def greet(x, y):
        pl.semaphore_signal(barrier, inc=1, device_id=(x, y), device_id_type=MESH)

    for_others(greet)

    panel = lax.convert_element_type(gx >= half, jnp.int32)
    loads = [
        pltpu.make_async_copy(right_side, r0, load_sem),
        pltpu.make_async_copy(precond.at[panel], matrix.at[pl.ds(0, levels)], load_sem),
        pltpu.make_async_copy(horizontal, horiz, load_sem),
        pltpu.make_async_copy(diagonal, diag, load_sem),
        pltpu.make_async_copy(precond.at[1 - panel], matrix.at[pl.ds(levels, levels)], load_sem),
        pltpu.make_async_copy(vertical, vert, small_sem.at[0]),
        pltpu.make_async_copy(edge_table, edge_rows, small_sem.at[1]),
    ]
    for load in loads:
        load.start()

    east_x, west_x = lax.rem(gx + 1, n_gx), lax.rem(gx + n_gx - 1, n_gx)
    east_border = (gx == half - 1) | (gx == n_gx - 1)
    west_border = (gx == half) | (gx == 0)
    border = east_border | west_border
    far_x = jnp.where(east_border, east_x, west_x)
    side = jnp.where(east_border, 0, 1)
    table = jnp.where((gx == half - 1) | (gx == half), 0, 1)
    edge_cols = [
        pl.ds(jnp.where(east_border, cols - 1 - i, i), rows, stride=cols) for i in range(3)
    ]
    first_row = pl.multiple_of(gy * rows, rows)
    own = pl.ds(first_row, rows)
    has_north, has_south = gy < n_gy - 1, gy > 0
    between = has_north & has_south

    def wait_count(count, sem):
        part = meter.at[pl.ds(0, count)]
        pltpu.make_async_copy(part, part, sem).wait()

    def wait_cases(count, sem):
        for n_sides, on_border in ((1, border), (2, jnp.logical_not(border))):
            for n_rows, here in ((1, jnp.logical_not(between)), (2, between)):
                pl.when(on_border & here)(
                    functools.partial(wait_count, count(n_sides, n_rows), sem)
                )

    @pl.when(jnp.logical_not(has_north))
    def _():
        from_north[...] = jnp.zeros_like(from_north)

    @pl.when(jnp.logical_not(has_south))
    def _():
        from_south[...] = jnp.zeros_like(from_south)

    outside[...] = jnp.zeros_like(outside)
    extra[...] = jnp.zeros_like(extra)

    def split(v):
        high = v.astype(jnp.bfloat16)
        return high, (v - high.astype(jnp.float32)).astype(jnp.bfloat16)

    def prepare_weights(which):
        turned = jnp.transpose(matrix[pl.ds(which * levels, levels), :])
        for part, value in enumerate(split(turned)):
            for twice in range(2):
                weights[
                    which, pl.ds(twice * levels, levels), pl.ds(part * levels, levels)
                ] = value

    def precondition(v, which=0):
        out = lax.dot_general(
            jnp.concatenate(split(v), 1),
            weights[which],
            (((1,), (0,)), ((), ())),
            preferred_element_type=jnp.float32,
        )
        return out[:, :levels] + out[:, levels:]

    def col_copy(t, side):
        buffer, x = (from_west, east_x) if side == 0 else (from_east, west_x)
        return pltpu.make_async_remote_copy(
            src_ref=frame_z.at[t, pl.ds(side * rows, rows)],
            dst_ref=buffer.at[t],
            send_sem=sent,
            recv_sem=col_recv.at[t // 2],
            device_id=(x, gy),
            device_id_type=MESH,
        )

    def far_copy(t, g):
        return pltpu.make_async_remote_copy(
            src_ref=pack.at[pl.ds(0, 4)] if t == 0 else pack.at[4],
            dst_ref=far_pack.at[:, own] if t == 0 else far_last.at[own],
            send_sem=sent,
            recv_sem=far_recv.at[t],
            device_id=(far_x, g),
            device_id_type=MESH,
        )

    def relay_copy(g, block):
        return pltpu.make_async_remote_copy(
            src_ref=far_pack.at[:, block],
            dst_ref=far_pack.at[:, block],
            send_sem=sent,
            recv_sem=relay_recv,
            device_id=(gx, g),
            device_id_type=MESH,
        )

    def near_copy(g):
        return pltpu.make_async_remote_copy(
            src_ref=near_out,
            dst_ref=near_pack.at[:, own],
            send_sem=sent,
            recv_sem=near_recv,
            device_id=(gx, g),
            device_id_type=MESH,
        )

    def mini_copy(side):
        return pltpu.make_async_remote_copy(
            src_ref=mini_out.at[side],
            dst_ref=mini_in.at[side],
            send_sem=sent,
            recv_sem=mini_recv,
            device_id=(gx, gy + 1 if side == 0 else gy - 1),
            device_id_type=MESH,
        )

    def row_copy(t, side):
        buffer, y, row = (
            (from_south, gy + 1, 2 * rows + cols)
            if side == 0
            else (from_north, gy - 1, 2 * rows)
        )
        return pltpu.make_async_remote_copy(
            src_ref=frame_z.at[t, pl.ds(row, cols)],
            dst_ref=buffer.at[t],
            send_sem=sent,
            recv_sem=row_recv.at[t],
            device_id=(gx, y),
            device_id_type=MESH,
        )

    def edge_copy(side):
        return pltpu.make_async_remote_copy(
            src_ref=edge_out.at[side],
            dst_ref=edge_in.at[1 - side],
            send_sem=sent,
            recv_sem=strip_recv,
            device_id=(east_x if side == 0 else west_x, gy),
            device_id_type=MESH,
        )

    def corner_copy(k):
        return pltpu.make_async_remote_copy(
            src_ref=corner_out.at[k],
            dst_ref=corner_in.at[k],
            send_sem=sent,
            recv_sem=strip_recv,
            device_id=(west_x if k < 2 else east_x, gy + 1 if k % 2 == 0 else gy - 1),
            device_id_type=MESH,
        )

    def for_sides(visit):
        pl.when(jnp.logical_not(east_border))(functools.partial(visit, 0))
        pl.when(jnp.logical_not(west_border))(functools.partial(visit, 1))

    def for_corners(visit, sending):
        for k in range(4):
            east = (k < 2) != sending
            north = (k % 2 == 0) == sending
            condition = jnp.logical_not(east_border if east else west_border)
            pl.when(condition & (has_north if north else has_south))(functools.partial(visit, k))

    def for_rows(visit):
        @pl.when(has_north)
        def _():
            visit(0)

        @pl.when(has_south)
        def _():
            visit(1)

    inward = 2 * (rows + cols)
    mid = pl.ds(8, rows)

    def side_cols(side, k):
        return pl.ds(k if side else cols - 1 - k, rows, stride=cols)

    def fill_edges():
        for side in range(2):
            items = [
                frame_z[0, pl.ds(side * rows, rows), :],
                frame_z[0, pl.ds(inward + side * rows, rows), :],
                horiz[side_cols(side, 0), :],
                diag[side_cols(side, 0), :],
            ]
            for k, item in enumerate(items):
                wide[side, k] = jnp.zeros_like(wide[side, k])
                wide[side, k, mid, :] = item
                if k:
                    edge_out[side, k - 1] = item
            for to, first, second in ((0, rows - 1, rows - 2), (1, 0, 1)):
                picks = [(0, first), (0, second), (1, first), (2, first), (3, first)]
                for k, (item, row) in enumerate(picks):
                    mini_out[to, pl.ds(8 * side + k, 1), :] = items[item][row : row + 1]
                next_horiz = horiz[pl.ds(first * cols + (1 if side else cols - 2), 1), :]
                mini_out[to, pl.ds(8 * side + 5, 1), :] = next_horiz
                mini_out[to, pl.ds(8 * side + 6, 2), :] = jnp.zeros((2, levels), jnp.float32)
                corner_out[2 * (1 - side) + to] = jnp.zeros((8, levels), jnp.float32)
                corner_out[2 * (1 - side) + to, pl.ds(0, 1), :] = items[0][first : first + 1]
        beyond[...] = jnp.zeros_like(beyond)

    def fill_packs():
        c0, c1, c2 = edge_cols
        z_edge = frame_z[0, pl.ds(side * rows, rows), :]
        h_edge, d_edge = horiz[c0, :], diag[c0, :]
        z_next = frame_z[0, pl.ds(inward + side * rows, rows), :]
        for k, item in enumerate([z_edge, z_next, h_edge, d_edge]):
            pack[k] = item
        for k, item in enumerate([z_edge, h_edge]):
            near_out[k] = item
            near_pack[k, own, :] = item
        for k, item in enumerate([d_edge, horiz[c1, :]]):
            near_coef[k] = jnp.zeros_like(near_coef[k])
            near_coef[k, own, :] = item

    def send_first(frame):
        frame_z[0] = precondition(frame)
        fill_edges()
        pl.when(border)(fill_packs)
        pl.semaphore_wait(barrier, n_all - 1)

        for_rows(lambda side: mini_copy(side).start())
        for_rows(lambda side: row_copy(0, side).start())
        pl.when(gx == 0)(send_far_pack)
        for_sides(lambda side: col_copy(0, side).start())
        for_corners(lambda k: corner_copy(k).start(), True)
        for_sides(lambda side: edge_copy(side).start())

        pl.when(border & (gx > 0))(send_far_pack)

    def send_rows(t, frame):
        frame_z[t, pl.ds(2 * rows, 2 * cols), :] = precondition(frame)
        for_rows(lambda side: row_copy(t, side).start())

    def send_far_pack():
        for g in range(1, n_gy, 2):
            far_copy(0, g).start()

    def send_far_last():
        for g in sorted(range(n_gy), key=lambda g: g % 2):
            far_copy(1, g).start()

    def send_near():
        for j in range(1, n_gy):
            near_copy(lax.rem(gy + j, n_gy)).start()

    def receive_rows(t):
        wait_cases(lambda sides, beside: beside * cols, row_recv.at[t])

    def receive_cols(t):
        wait_cases(lambda sides, beside: sides * rows, col_recv.at[t // 2])

        def take(side):
            buffer = from_west if side else from_east
            outside[pl.ds(side * rows, rows), :] = buffer[t]
            if t == 0:
                beyond[side, mid, :] = buffer[t]

        for_sides(take)

    col_id = lax.rem(lax.broadcasted_iota(jnp.int32, (cells, levels), 0), cols)
    east_edge = pl.ds(cols - 1, rows, stride=cols)
    west_edge = pl.ds(0, rows, stride=cols)
    south_edge = pl.ds(0, cols)
    north_edge = pl.ds(cells - cols, cols)

    def edge_columns(ref):
        return jnp.concatenate([ref[east_edge, :], ref[west_edge, :]], 0)

    def column_part(z):
        lane = lax.broadcasted_iota(jnp.int32, z.shape, 1)
        up = jnp.where(lane < levels - 1, pltpu.roll(z, levels - 1, 1), 0.0)
        down = jnp.where(lane > 0, pltpu.roll(z, 1, 1), 0.0)
        return vert[...] * (2.0 * z - (up + down))

    def inner_image(z):
        east = jnp.where(col_id < cols - 1, pltpu.roll(z, cells - 1, 0), 0.0)
        west = jnp.where(col_id > 0, pltpu.roll(z, 1, 0), 0.0)
        none = jnp.zeros((cols, levels), jnp.float32)
        north = jnp.concatenate([z[cols:], none], 0)
        south = jnp.concatenate([none, z[:-cols]], 0)
        beside = east + west + north + south
        return diag[...] * z + horiz[...] * (4.0 * z - beside) + column_part(z)

    def product(a, b):
        both = (a * b).reshape(-1, 8, levels)
        return jnp.sum(jnp.sum(both, axis=0), axis=0, keepdims=True)

    tall_id = lax.broadcasted_iota(jnp.int32, (tall, levels), 0)

    def along(w):
        north = jnp.where(tall_id < tall - 1, pltpu.roll(w, tall - 1, 0), 0.0)
        south = jnp.where(tall_id > 0, pltpu.roll(w, 1, 0), 0.0)
        return north + south

    def stencil(w, d, h):
        return d * w + h * (4.0 * w - along(w)) + column_part(w)

    def gather_rows(start, count, pairs):
        def one(y):
            row = edge_rows[table, start + y]
            for dst, src in pairs:
                gathered[dst, pl.ds(y, 1), :] = src[pl.ds(row, 1), :]

        if count <= 64:
            for y in range(count):
                one(y)
        else:

            def body(y, carry):
                one(y)
                return carry

            lax.fori_loop(0, count, body, 0)

    def wait_bytes(ref, sem):
        pltpu.make_async_copy(ref, ref, sem).wait()

    near_rest = pl.ds(0, (n_gy - 1) * rows)
    last = gx == n_gx - 1
    crosses = border & (lax.rem(gy, 2) == 1)
    crossed = border & (lax.rem(gy, 2) == 0)

    def relay_across():
        wait_bytes(far_pack, far_recv.at[0])
        relay_copy(gy - 1, pl.ds(0, tall)).start()

    def next_to(w):
        return pltpu.roll(w, w.shape[0] - 1, 0) + pltpu.roll(w, 1, 0)

    def strip_image(side, k, z, left, right):
        c = side_cols(side, k)
        return diag[c, :] * z + horiz[c, :] * (4.0 * z - left - right) + column_part(z)

    def look_ahead():
        c1 = edge_cols[1]

        def take(direction, near, far, row):
            for k in range(2):
                near_coef[k, pl.ds(row, 1), :] = mini_in[direction, pl.ds(8 * side + 4 + k, 1), :]
            for k_side in range(2):
                given = mini_in.at[direction]
                wide[k_side, 0, pl.ds(near, 1), :] = given[pl.ds(8 * k_side, 1), :]
                wide[k_side, 0, pl.ds(far, 1), :] = given[pl.ds(8 * k_side + 1, 1), :]
                for k in (1, 2, 3):
                    wide[k_side, k, pl.ds(near, 1), :] = given[pl.ds(8 * k_side + k + 1, 1), :]

        wait_cases(lambda sides, beside: 16 * beside, mini_recv)
        pl.when(has_south)(functools.partial(take, 0, 7, 6, first_row - 1))
        pl.when(has_north)(functools.partial(take, 1, 8 + rows, 9 + rows, first_row + rows))
        z_edge, z_next, h_edge, d_edge = (wide[side, k] for k in range(4))
        v_edge = (
            d_edge * z_edge
            + h_edge * (4.0 * z_edge - z_next - next_to(z_edge))
            + column_part(z_edge)
        )
        beside = next_to(z_next)[8 : 8 + rows] + z_edge[8 : 8 + rows]
        z1 = z_next[8 : 8 + rows]
        z2 = frame_z[0, pl.ds(inward + (2 + side) * rows, rows), :]
        v_next = (
            diag[c1, :] * z1 + horiz[c1, :] * (4.0 * z1 - beside - z2) + column_part(z1)
        )
        z = precondition(jnp.concatenate([v_edge, v_next], 0))
        z_edge, z_next = z[: rows + 16], z[rows + 16 :]
        beside = next_to(z_edge)[8 : 8 + rows] + z_next
        z_edge = z_edge[8 : 8 + rows]
        near_out[2] = z_edge
        near_pack[2, own, :] = z_edge
        h_own, d_own = h_edge[8 : 8 + rows], d_edge[8 : 8 + rows]
        v = d_own * z_edge + h_own * (4.0 * z_edge - beside) + column_part(z_edge)
        pack[4] = precondition(v)
        pl.when(border)(send_far_last)

    def look_across():
        wait_cases(lambda sides, beside: sides * (3 * rows + 8 * beside), strip_recv)

        def take(k):
            row = 8 + rows if k % 2 else 7
            beyond[k // 2, pl.ds(row, 1), :] = corner_in[k, pl.ds(0, 1), :]

        for_corners(take, False)
        images_first = []
        for side in range(2):
            z_edge, z_next, h_edge, d_edge = (wide[side, k] for k in range(4))
            z_out = beyond[side]
            own_edge, own_out = z_edge[8 : 8 + rows], z_out[8 : 8 + rows]
            v_edge = (
                d_edge * z_edge
                + h_edge * (4.0 * z_edge - z_next - z_out - next_to(z_edge))
                + column_part(z_edge)
            )
            z1 = z_next[8 : 8 + rows]
            z2 = frame_z[0, pl.ds(inward + (2 + side) * rows, rows), :]
            v_next = strip_image(side, 1, z1, next_to(z_next)[8 : 8 + rows] + own_edge, z2)
            v_out = (
                edge_in[side, 2] * own_out
                + edge_in[side, 1]
                * (4.0 * own_out - edge_in[side, 0] - own_edge - next_to(z_out)[8 : 8 + rows])
                + column_part(own_out)
            )
            images_first += [v_edge, v_next, v_out]
        z = precondition(jnp.concatenate(images_first, 0))
        second = []
        each = 3 * rows + 16
        for side in range(2):
            part = z[side * each : (side + 1) * each]
            z_edge, z_next, z_out = part[: rows + 16], part[rows + 16 : each - rows], part[each - rows :]
            strip_out[pl.ds(side * rows, rows), :] = z_out
            beside = next_to(z_edge)[8 : 8 + rows]
            second.append(strip_image(side, 0, z_edge[8 : 8 + rows], beside + z_next, z_out))
        frame_z[2, pl.ds(0, 2 * rows), :] = precondition(jnp.concatenate(second, 0))

        def give(side):
            col_copy(2, side).start()
            outside[pl.ds(side * rows, rows), :] = strip_out[pl.ds(side * rows, rows), :]

        for_sides(give)

    def correct_early():
        pl.when(border)(lambda: wait_bytes(near_pack.at[:, near_rest], near_recv))
        gather_rows(0, tall, [(1, near_pack.at[0])])

        @pl.when(border)
        def _():
            pl.when(crossed)(lambda: wait_bytes(far_pack, relay_recv))
        gather_rows(0, tall, [(0, far_pack.at[0])])
        h_near, d_near = near_pack[1], near_coef[0]
        h_far, d_far = far_pack[2], far_pack[3]
        b_near, b_far = -(h_near * gathered[0]), -(h_far * gathered[1])
        v_far = stencil(far_pack[0], d_far, h_far) - h_far * far_pack[1] + b_far
        w_near = precondition(b_near)
        far = precondition(jnp.concatenate([b_far, v_far], 0), 1)
        w_far = far[:tall]
        strip[0] = b_near
        strip[1] = w_near
        strip[3] = far[tall:]
        strip[4] = near_pack[2] + w_near
        gather_rows(0, tall, [(0, strip.at[3]), (1, strip.at[4])])
        b_near = stencil(w_near, d_near, h_near) - h_near * gathered[0]
        b_far = stencil(w_far, d_far, h_far) - h_far * gathered[1]
        b_next = -(near_coef[1] * w_near)
        near = precondition(jnp.concatenate([b_near, b_next], 0))
        w_edge, w_next = near[:tall], near[tall:]
        strip[3] = b_near
        strip[4] = b_next
        strip[5] = precondition(b_far, 1)
        strip[6] = w_edge
        strip[7] = w_next
        strip[8] = along(w_next)
        strip[9] = stencil(w_edge, d_near, h_near) - h_near * w_next

    def strip_of(ref):
        return jnp.concatenate([ref[c, :] for c in edge_cols], 0)

    def add_to(key, value):
        extra[pl.ds(KEYS.index(key), 1), :] += value

    def correct_two():
        none = jnp.zeros((rows, levels), jnp.float32)
        changes = [
            [strip[0, own, :], none, none],
            [strip[3, own, :], strip[4, own, :], none],
        ]
        before = [strip_of(r0)]
        after = [before[0]]
        for t in range(2):
            old = strip_of(images.at[t])
            new = old + jnp.concatenate(changes[t], 0)
            before.append(old)
            after.append(new)
            for k in range(t + 1):
                images[t, edge_cols[k], :] = new[k * rows : (k + 1) * rows]
        for i, j in KEYS:
            if 0 < j < 3:
                add_to((i, j), product(after[i], after[j]) - product(before[i], before[j]))
        gather_rows(first_row, rows, [(2, strip.at[5])])

    def correct_third():
        c0, c1, c2 = edge_cols
        w_edge, w_next, beside = strip[6, own, :], strip[7, own, :], strip[8, own, :]
        h0, h1 = horiz[c0, :], horiz[c1, :]
        later = diag[c1, :] * w_next + h1 * (4.0 * w_next - beside - w_edge) + column_part(w_next)
        rest = jnp.concatenate([later, -(horiz[c2, :] * w_next)], 0)
        spaces_here = [strip_of(r0), strip_of(images.at[0]), strip_of(images.at[1])]
        old = strip_of(images.at[2])
        new_rest = old[rows:] + rest
        images[2, c1, :] = new_rest[:rows]
        images[2, c2, :] = new_rest[rows:]
        for i, space in enumerate(spaces_here):
            add_to((i, 3), product(space[rows:], rest))
        add_to((3, 3), product(new_rest, new_rest) - product(old, old))
        base = strip[9, own, :] - h0 * gathered[2, pl.ds(0, rows), :]
        wait_bytes(far_last, far_recv.at[1])
        gather_rows(first_row, rows, [(3, far_last)])
        b_edge = base - h0 * gathered[3, pl.ds(0, rows), :]
        new = old[:rows] + b_edge
        images[2, c0, :] = new
        for i, space in enumerate(spaces_here):
            add_to((i, 3), product(space[:rows], b_edge))
        add_to((3, 3), product(new, new))

    wait_count(3 * cells + 2 * levels, load_sem)
    for load in loads[5:]:
        load.wait()
    prepare_weights(0)
    terms = {}
    spaces = [r0]
    frame = [edge_columns(r0), r0[south_edge, :], r0[north_edge, :]]
    frame += [r0[side_cols(side, k), :] for k in (1, 2) for side in range(2)]
    send_first(jnp.concatenate(frame, 0))
    edge_horiz = edge_columns(horiz)
    for t in range(ITERS):
        image = images.at[t]
        z = precondition(spaces[-1][...])
        fields[t] = z
        newest = len(spaces) - 1
        for i in range(len(spaces)):
            terms[(i, newest)] = product(spaces[i][...], spaces[newest][...])
        image[...] = inner_image(z)
        if t == 0:
            prepare_weights(1)
            look_ahead()
            pl.when(border & jnp.logical_not(last))(send_near)
        if t == 1:
            look_across()
        if t == 2:
            pl.when(crosses)(relay_across)
            correct_early()
            pl.when(border)(correct_two)
        receive_rows(t)
        image[south_edge, :] = image[south_edge, :] - horiz[south_edge, :] * from_south[t]
        image[north_edge, :] = image[north_edge, :] - horiz[north_edge, :] * from_north[t]
        inside = edge_columns(image)
        if t != 1:
            receive_cols(t)
        edges = inside - edge_horiz * outside[...]
        image[east_edge, :] = edges[:rows]
        image[west_edge, :] = edges[rows:]
        if t < ITERS - 1:
            send_rows(t + 1, jnp.concatenate([image[south_edge, :], image[north_edge, :]], 0))
        if t == 0:
            pl.when(last)(send_near)
        spaces.append(image)
    newest = len(spaces) - 1
    for i in range(len(spaces)):
        terms[(i, newest)] = product(spaces[i][...], spaces[newest][...])
    for k, key in enumerate(KEYS):
        partial[pl.ds(k, 1), :] = terms[key]

    @pl.when(border)
    def _():
        correct_third()

    height = -(-len(KEYS) // 8) * 8
    row_id = lax.broadcasted_iota(jnp.int32, (height, levels), 0)
    lane = lax.broadcasted_iota(jnp.int32, (height, levels), 1)
    stacked = jnp.where(row_id < len(KEYS), partial[...] + extra[...], 0.0)
    summed = jnp.sum(stacked, axis=1, keepdims=True)
    sums[me] = jnp.sum(jnp.where(lane == row_id, summed, 0.0), axis=0, keepdims=True)

    def tell(x, y):
        pltpu.make_async_remote_copy(
            src_ref=sums.at[me],
            dst_ref=sums.at[me],
            send_sem=sum_sent,
            recv_sem=sum_recv,
            device_id=(x, y),
            device_id_type=MESH,
        ).start()

    def tell_all(x, carry):
        for y in range(n_gy):
            pl.when(me != x * n_gy + y)(functools.partial(tell, x, y))
        return carry

    if n_all <= 64:
        for x in range(n_gx):
            tell_all(x, 0)
    else:
        lax.fori_loop(0, n_gx, tell_all, 0)
    def all_sent(sides, beside, border_part):
        per_side = 5 * rows + 8 * beside
        return sides * per_side + beside * (ITERS * cols + 16) + border_part * rows

    common = n_gy + 3 * (n_gy - 1) + 2 * n_gy
    for condition, sides, border_part in (
        (jnp.logical_not(border), 2, 0),
        (crosses, 1, common + 4 * n_gy),
        (crossed, 1, common),
    ):
        for beside, here in ((1, jnp.logical_not(between)), (2, between)):
            pl.when(condition & here)(
                functools.partial(wait_count, all_sent(sides, beside, border_part), sent)
            )

    @pl.when(border)
    def _():
        c0, c1, c2 = edge_cols
        fields[1, c0, :] += strip[1, own, :]
        fields[2, c0, :] += strip[6, own, :]
        fields[2, c1, :] += strip[7, own, :]

    others = sums.at[pl.ds(0, n_all - 1)]
    wait_bytes(others, sum_recv)
    out_totals[...] = jnp.sum(sums[...], axis=0)
    wait_bytes(others, sum_sent)


def finish(
    total_cells, all_totals, r0, fields, images, out_x, out_r, out_norms, x, r, norms_out, sem, norm_sem
):
    levels = r0.shape[-1]
    totals = all_totals[...]
    value = {
        key: jnp.broadcast_to(totals[:, k : k + 1], (8, levels)) for k, key in enumerate(KEYS)
    }

    rho, g0, g1, g2 = value[(0, 0)], value[(0, 1)], value[(0, 2)], value[(0, 3)]
    a00, a01, a02 = value[(1, 1)], value[(1, 2)], value[(1, 3)]
    a11, a12, a22 = value[(2, 2)], value[(2, 3)], value[(3, 3)]
    l10, l20, y0 = a01 / a00, a02 / a00, g0 / a00
    d1, e12, f1 = a11 - l10 * a01, a12 - l10 * a02, g1 - l10 * g0
    l21, y1 = e12 / d1, f1 / d1
    d2, f2 = a22 - l20 * a02 - l21 * e12, g2 - l20 * g0 - l21 * f1
    y2 = f2 / d2
    norm0 = rho - y0 * g0
    norm1 = norm0 - y1 * f1
    norm2 = norm1 - y2 * f2
    y1 = y1 - l21 * y2
    y0 = y0 - l10 * y1 - l20 * y2
    norm_lane = lax.broadcasted_iota(jnp.int32, (8, levels), 1)
    norms = jnp.where(norm_lane == 0, norm0, jnp.where(norm_lane == 1, norm1, norm2))
    norms_out[...] = norms[:1, :ITERS] / total_cells
    copies = [pltpu.make_async_copy(norms_out, out_norms, norm_sem)]
    copies[0].start()
    rows = r0.shape[0]
    pieces = 2 if rows % 16 == 0 else 1
    size = rows // pieces
    y0, y1, y2 = (jnp.tile(y, (size // 8, 1)) for y in (y0, y1, y2))
    for p in range(pieces):
        span = pl.ds(p * size, size)
        x[span] = y0 * fields[0, span] + y1 * fields[1, span] + y2 * fields[2, span]
        r[span] = (
            r0[span] - y0 * images[0, span] - y1 * images[1, span] - y2 * images[2, span]
        )
        for k, (src, dst) in enumerate(((x, out_x), (r, out_r))):
            copy = pltpu.make_async_copy(src.at[span], dst.at[span], sem.at[p, k])
            copy.start()
            copies.append(copy)
    for copy in copies:
        copy.wait()


def on_device(n_gx, n_gy, right_side, diagonal, horizontal, vertical, precond, edge_rows):
    rows, cols, levels = right_side.shape
    f32 = jnp.float32
    block = (rows * cols, levels)
    column = (n_gy * rows, levels)
    sems = pltpu.SemaphoreType.DMA
    meter_rows = 3 * rows * cols + 2 * levels + (16 + 10 * n_gy) * rows + 8 * cols + 64
    basis = pltpu.VMEM((ITERS,) + block, f32)
    fields, images, totals, start = pl.pallas_call(
        functools.partial(kernel, n_gx, n_gy, rows),
        out_shape=(basis, basis, pltpu.VMEM((1, levels), f32), pltpu.VMEM(block, f32)),
        in_specs=[ANY, ANY, ANY, ANY, ANY, ANY],
        out_specs=(VMEM, VMEM, VMEM, VMEM),
        scratch_shapes=[
            pltpu.VMEM(block, f32),
            pltpu.VMEM(block, f32),
            pltpu.VMEM((1, levels), f32),
            pltpu.VMEM((2 * levels, levels), f32),
            pltpu.VMEM((2, 2 * levels, 2 * levels), jnp.bfloat16),
            pltpu.VMEM((ITERS, 6 * rows + 2 * cols, levels), f32),
            pltpu.VMEM((5, rows, levels), f32),
            pltpu.VMEM((3, rows, levels), f32),
            pltpu.VMEM((2,) + column, f32),
            pltpu.VMEM((2, 16, levels), f32),
            pltpu.VMEM((2, 16, levels), f32),
            pltpu.VMEM((2, 4, rows + 16, levels), f32),
            pltpu.VMEM((2, 3, rows, levels), f32),
            pltpu.VMEM((2, 3, rows, levels), f32),
            pltpu.VMEM((4, 8, levels), f32),
            pltpu.VMEM((4, 8, levels), f32),
            pltpu.VMEM((2, rows + 16, levels), f32),
            pltpu.VMEM((ITERS, rows, levels), f32),
            pltpu.VMEM((ITERS, rows, levels), f32),
            pltpu.VMEM((ITERS, cols, levels), f32),
            pltpu.VMEM((ITERS, cols, levels), f32),
            pltpu.VMEM((4,) + column, f32),
            pltpu.VMEM((3,) + column, f32),
            pltpu.VMEM(column, f32),
            pltpu.VMEM((4,) + column, f32),
            pltpu.VMEM((10,) + column, f32),
            pltpu.VMEM((2 * rows, levels), f32),
            pltpu.VMEM((2 * rows, levels), f32),
            pltpu.VMEM((16, levels), f32),
            pltpu.VMEM((16, levels), f32),
            pltpu.VMEM((n_gx * n_gy, 1, levels), f32),
            pltpu.SMEM(edge_rows.shape, jnp.int32),
            pltpu.VMEM((meter_rows, levels), f32),
            sems(()),
            sems((2,)),
            sems(()),
            sems(()),
            sems((2,)),
            sems((ITERS,)),
            sems((2,)),
            sems(()),
            sems(()),
            sems(()),
            sems(()),
            sems(()),
        ],
        compiler_params=pltpu.CompilerParams(collective_id=0, has_side_effects=True),
    )(
        edge_rows,
        right_side.reshape(block),
        diagonal.reshape(block),
        horizontal.reshape(block),
        vertical.reshape(1, levels),
        precond,
    )
    in_vmem = functools.partial(
        pltpu.with_memory_space_constraint, memory_space=pltpu.VMEM
    )
    total_cells = float(rows * cols * levels * n_gx * n_gy)
    x, r, norms = pl.pallas_call(
        functools.partial(finish, total_cells),
        out_shape=(
            jax.ShapeDtypeStruct(block, f32),
            jax.ShapeDtypeStruct(block, f32),
            jax.ShapeDtypeStruct((1, ITERS), f32),
        ),
        in_specs=[VMEM, VMEM, VMEM, VMEM],
        out_specs=(ANY, ANY, ANY),
        scratch_shapes=[
            pltpu.VMEM(block, f32),
            pltpu.VMEM(block, f32),
            pltpu.VMEM((1, ITERS), f32),
            sems((2, 2)),
            sems(()),
        ],
    )(in_vmem(totals), in_vmem(start), in_vmem(fields), in_vmem(images))
    shape = right_side.shape
    return x.reshape(shape), r.reshape(shape), norms.reshape(ITERS)


def solution(mesh):
    n_gx, n_gy = mesh.shape["gx"], mesh.shape["gy"]
    field = P("gy", "gx", None)
    return jax.shard_map(
        functools.partial(on_device, n_gx, n_gy),
        mesh=mesh,
        in_specs=(field, field, field, P(), P(), P()),
        out_specs=(field, field, P()),
        check_vma=False,
    )
```

```python
import functools

import jax
import jax.numpy as jnp
from jax import lax
from jax.experimental import pallas as pl
from jax.experimental.pallas import tpu as pltpu
from jax.sharding import PartitionSpec as P

ITERS = 3
KEYS = [(i, j) for j in range(ITERS + 1) for i in range(j + 1)]
MESH = pl.DeviceIdType.MESH
ANY = pl.BlockSpec(memory_space=pl.ANY)
VMEM = pl.BlockSpec(memory_space=pltpu.VMEM)


def kernel(
    n_gx,
    n_gy,
    out_rows,
    edge_table,
    right_side,
    diagonal,
    horizontal,
    vertical,
    precond,
    fields,
    images,
    out_totals,
    r0,
    diag,
    horiz,
    vert,
    matrix,
    weights,
    frame_z,
    pack,
    near_out,
    near_coef,
    mini_out,
    mini_in,
    wide,
    edge_out,
    edge_in,
    corner_out,
    corner_in,
    beyond,
    from_east,
    from_west,
    from_north,
    from_south,
    far_pack,
    near_pack,
    far_last,
    gathered,
    strip,
    strip_out,
    outside,
    partial,
    extra,
    sums,
    edge_rows,
    meter,
    load_sem,
    small_sem,
    sent,
    sum_sent,
    col_recv,
    row_recv,
    far_recv,
    relay_recv,
    near_recv,
    mini_recv,
    strip_recv,
    sum_recv,
):
    rows, levels = out_rows, r0.shape[-1]
    cells = r0.shape[0]
    cols = cells // rows
    tall = n_gy * rows
    gx, gy = lax.axis_index("gx"), lax.axis_index("gy")
    n_all = n_gx * n_gy
    half = n_gx // 2
    me = gx * n_gy + gy

    def for_others(visit):
        def step(i, carry):
            for j in range(n_gy):
                visit(lax.rem(gx + i, n_gx), lax.rem(gy + j, n_gy))
            return carry

        if n_all <= 64:
            for i in sorted(range(1, n_gx), key=lambda i: min(i, n_gx - i)):
                step(i, 0)
        else:
            lax.fori_loop(1, n_gx, step, 0)
        for j in range(1, n_gy):
            visit(gx, lax.rem(gy + j, n_gy))

    barrier = pltpu.get_barrier_semaphore()

    def greet(x, y):
        pl.semaphore_signal(barrier, inc=1, device_id=(x, y), device_id_type=MESH)

    for_others(greet)

    panel = lax.convert_element_type(gx >= half, jnp.int32)
    loads = [
        pltpu.make_async_copy(right_side, r0, load_sem),
        pltpu.make_async_copy(precond.at[panel], matrix.at[pl.ds(0, levels)], load_sem),
        pltpu.make_async_copy(horizontal, horiz, load_sem),
        pltpu.make_async_copy(diagonal, diag, load_sem),
        pltpu.make_async_copy(precond.at[1 - panel], matrix.at[pl.ds(levels, levels)], load_sem),
        pltpu.make_async_copy(vertical, vert, small_sem.at[0]),
        pltpu.make_async_copy(edge_table, edge_rows, small_sem.at[1]),
    ]
    for load in loads:
        load.start()

    east_x, west_x = lax.rem(gx + 1, n_gx), lax.rem(gx + n_gx - 1, n_gx)
    east_border = (gx == half - 1) | (gx == n_gx - 1)
    west_border = (gx == half) | (gx == 0)
    border = east_border | west_border
    far_x = jnp.where(east_border, east_x, west_x)
    side = jnp.where(east_border, 0, 1)
    table = jnp.where((gx == half - 1) | (gx == half), 0, 1)
    edge_cols = [
        pl.ds(jnp.where(east_border, cols - 1 - i, i), rows, stride=cols) for i in range(3)
    ]
    first_row = pl.multiple_of(gy * rows, rows)
    own = pl.ds(first_row, rows)
    has_north, has_south = gy < n_gy - 1, gy > 0
    between = has_north & has_south

    def wait_count(count, sem):
        part = meter.at[pl.ds(0, count)]
        pltpu.make_async_copy(part, part, sem).wait()

    def wait_cases(count, sem):
        for n_sides, on_border in ((1, border), (2, jnp.logical_not(border))):
            for n_rows, here in ((1, jnp.logical_not(between)), (2, between)):
                pl.when(on_border & here)(
                    functools.partial(wait_count, count(n_sides, n_rows), sem)
                )

    @pl.when(jnp.logical_not(has_north))
    def _():
        from_north[...] = jnp.zeros_like(from_north)

    @pl.when(jnp.logical_not(has_south))
    def _():
        from_south[...] = jnp.zeros_like(from_south)

    outside[...] = jnp.zeros_like(outside)
    extra[...] = jnp.zeros_like(extra)

    def split(v):
        high = v.astype(jnp.bfloat16)
        return high, (v - high.astype(jnp.float32)).astype(jnp.bfloat16)

    def prepare_weights(which):
        turned = jnp.transpose(matrix[pl.ds(which * levels, levels), :])
        for part, value in enumerate(split(turned)):
            for twice in range(2):
                weights[
                    which, pl.ds(twice * levels, levels), pl.ds(part * levels, levels)
                ] = value

    def precondition(v, which=0):
        out = lax.dot_general(
            jnp.concatenate(split(v), 1),
            weights[which],
            (((1,), (0,)), ((), ())),
            preferred_element_type=jnp.float32,
        )
        return out[:, :levels] + out[:, levels:]

    def col_copy(t, side):
        buffer, x = (from_west, east_x) if side == 0 else (from_east, west_x)
        return pltpu.make_async_remote_copy(
            src_ref=frame_z.at[t, pl.ds(side * rows, rows)],
            dst_ref=buffer.at[t],
            send_sem=sent,
            recv_sem=col_recv.at[t // 2],
            device_id=(x, gy),
            device_id_type=MESH,
        )

    def far_copy(t, g):
        return pltpu.make_async_remote_copy(
            src_ref=pack.at[pl.ds(0, 4)] if t == 0 else pack.at[4],
            dst_ref=far_pack.at[:, own] if t == 0 else far_last.at[own],
            send_sem=sent,
            recv_sem=far_recv.at[t],
            device_id=(far_x, g),
            device_id_type=MESH,
        )

    def relay_copy(g, block):
        return pltpu.make_async_remote_copy(
            src_ref=far_pack.at[:, block],
            dst_ref=far_pack.at[:, block],
            send_sem=sent,
            recv_sem=relay_recv,
            device_id=(gx, g),
            device_id_type=MESH,
        )

    def near_copy(g):
        return pltpu.make_async_remote_copy(
            src_ref=near_out,
            dst_ref=near_pack.at[:, own],
            send_sem=sent,
            recv_sem=near_recv,
            device_id=(gx, g),
            device_id_type=MESH,
        )

    def mini_copy(side):
        return pltpu.make_async_remote_copy(
            src_ref=mini_out.at[side],
            dst_ref=mini_in.at[side],
            send_sem=sent,
            recv_sem=mini_recv,
            device_id=(gx, gy + 1 if side == 0 else gy - 1),
            device_id_type=MESH,
        )

    def row_copy(t, side):
        buffer, y, row = (
            (from_south, gy + 1, 2 * rows + cols)
            if side == 0
            else (from_north, gy - 1, 2 * rows)
        )
        return pltpu.make_async_remote_copy(
            src_ref=frame_z.at[t, pl.ds(row, cols)],
            dst_ref=buffer.at[t],
            send_sem=sent,
            recv_sem=row_recv.at[t],
            device_id=(gx, y),
            device_id_type=MESH,
        )

    def edge_copy(side):
        return pltpu.make_async_remote_copy(
            src_ref=edge_out.at[side],
            dst_ref=edge_in.at[1 - side],
            send_sem=sent,
            recv_sem=strip_recv,
            device_id=(east_x if side == 0 else west_x, gy),
            device_id_type=MESH,
        )

    def corner_copy(k):
        return pltpu.make_async_remote_copy(
            src_ref=corner_out.at[k],
            dst_ref=corner_in.at[k],
            send_sem=sent,
            recv_sem=strip_recv,
            device_id=(west_x if k < 2 else east_x, gy + 1 if k % 2 == 0 else gy - 1),
            device_id_type=MESH,
        )

    def for_sides(visit):
        pl.when(jnp.logical_not(east_border))(functools.partial(visit, 0))
        pl.when(jnp.logical_not(west_border))(functools.partial(visit, 1))

    def for_corners(visit, sending):
        for k in range(4):
            east = (k < 2) != sending
            north = (k % 2 == 0) == sending
            condition = jnp.logical_not(east_border if east else west_border)
            pl.when(condition & (has_north if north else has_south))(functools.partial(visit, k))

    def for_rows(visit):
        @pl.when(has_north)
        def _():
            visit(0)

        @pl.when(has_south)
        def _():
            visit(1)

    inward = 2 * (rows + cols)
    mid = pl.ds(8, rows)

    def side_cols(side, k):
        return pl.ds(k if side else cols - 1 - k, rows, stride=cols)

    def fill_edges():
        for side in range(2):
            items = [
                frame_z[0, pl.ds(side * rows, rows), :],
                frame_z[0, pl.ds(inward + side * rows, rows), :],
                horiz[side_cols(side, 0), :],
                diag[side_cols(side, 0), :],
            ]
            for k, item in enumerate(items):
                wide[side, k] = jnp.zeros_like(wide[side, k])
                wide[side, k, mid, :] = item
                if k:
                    edge_out[side, k - 1] = item
            for to, first, second in ((0, rows - 1, rows - 2), (1, 0, 1)):
                picks = [(0, first), (0, second), (1, first), (2, first), (3, first)]
                for k, (item, row) in enumerate(picks):
                    mini_out[to, pl.ds(8 * side + k, 1), :] = items[item][row : row + 1]
                next_horiz = horiz[pl.ds(first * cols + (1 if side else cols - 2), 1), :]
                mini_out[to, pl.ds(8 * side + 5, 1), :] = next_horiz
                mini_out[to, pl.ds(8 * side + 6, 2), :] = jnp.zeros((2, levels), jnp.float32)
                corner_out[2 * (1 - side) + to] = jnp.zeros((8, levels), jnp.float32)
                corner_out[2 * (1 - side) + to, pl.ds(0, 1), :] = items[0][first : first + 1]
        beyond[...] = jnp.zeros_like(beyond)

    def fill_packs():
        c0, c1, c2 = edge_cols
        z_edge = frame_z[0, pl.ds(side * rows, rows), :]
        h_edge, d_edge = horiz[c0, :], diag[c0, :]
        z_next = frame_z[0, pl.ds(inward + side * rows, rows), :]
        for k, item in enumerate([z_edge, z_next, h_edge, d_edge]):
            pack[k] = item
        for k, item in enumerate([z_edge, h_edge]):
            near_out[k] = item
            near_pack[k, own, :] = item
        for k, item in enumerate([d_edge, horiz[c1, :]]):
            near_coef[k] = jnp.zeros_like(near_coef[k])
            near_coef[k, own, :] = item

    def send_first(frame):
        frame_z[0] = precondition(frame)
        fill_edges()
        pl.when(border)(fill_packs)
        pl.semaphore_wait(barrier, n_all - 1)

        for_rows(lambda side: mini_copy(side).start())
        for_rows(lambda side: row_copy(0, side).start())
        pl.when(gx == 0)(send_far_pack)
        for_sides(lambda side: col_copy(0, side).start())
        for_corners(lambda k: corner_copy(k).start(), True)
        for_sides(lambda side: edge_copy(side).start())

        pl.when(border & (gx > 0))(send_far_pack)

    def send_rows(t, frame):
        frame_z[t, pl.ds(2 * rows, 2 * cols), :] = precondition(frame)
        for_rows(lambda side: row_copy(t, side).start())

    def send_far_pack():
        for g in range(1, n_gy, 2):
            far_copy(0, g).start()

    def send_far_last():
        for g in sorted(range(n_gy), key=lambda g: g % 2):
            far_copy(1, g).start()

    def send_near():
        for j in range(1, n_gy):
            near_copy(lax.rem(gy + j, n_gy)).start()

    def receive_rows(t):
        wait_cases(lambda sides, beside: beside * cols, row_recv.at[t])

    def receive_cols(t):
        wait_cases(lambda sides, beside: sides * rows, col_recv.at[t // 2])

        def take(side):
            buffer = from_west if side else from_east
            outside[pl.ds(side * rows, rows), :] = buffer[t]
            if t == 0:
                beyond[side, mid, :] = buffer[t]

        for_sides(take)

    col_id = lax.rem(lax.broadcasted_iota(jnp.int32, (cells, levels), 0), cols)
    east_edge = pl.ds(cols - 1, rows, stride=cols)
    west_edge = pl.ds(0, rows, stride=cols)
    south_edge = pl.ds(0, cols)
    north_edge = pl.ds(cells - cols, cols)

    def edge_columns(ref):
        return jnp.concatenate([ref[east_edge, :], ref[west_edge, :]], 0)

    def column_part(z):
        lane = lax.broadcasted_iota(jnp.int32, z.shape, 1)
        up = jnp.where(lane < levels - 1, pltpu.roll(z, levels - 1, 1), 0.0)
        down = jnp.where(lane > 0, pltpu.roll(z, 1, 1), 0.0)
        return vert[...] * (2.0 * z - (up + down))

    def inner_image(z):
        east = jnp.where(col_id < cols - 1, pltpu.roll(z, cells - 1, 0), 0.0)
        west = jnp.where(col_id > 0, pltpu.roll(z, 1, 0), 0.0)
        none = jnp.zeros((cols, levels), jnp.float32)
        north = jnp.concatenate([z[cols:], none], 0)
        south = jnp.concatenate([none, z[:-cols]], 0)
        beside = east + west + north + south
        return diag[...] * z + horiz[...] * (4.0 * z - beside) + column_part(z)

    def product(a, b):
        both = (a * b).reshape(-1, 8, levels)
        return jnp.sum(jnp.sum(both, axis=0), axis=0, keepdims=True)

    tall_id = lax.broadcasted_iota(jnp.int32, (tall, levels), 0)

    def along(w):
        north = jnp.where(tall_id < tall - 1, pltpu.roll(w, tall - 1, 0), 0.0)
        south = jnp.where(tall_id > 0, pltpu.roll(w, 1, 0), 0.0)
        return north + south

    def stencil(w, d, h):
        return d * w + h * (4.0 * w - along(w)) + column_part(w)

    def gather_rows(start, count, pairs):
        def one(y):
            row = edge_rows[table, start + y]
            for dst, src in pairs:
                gathered[dst, pl.ds(y, 1), :] = src[pl.ds(row, 1), :]

        if count <= 64:
            for y in range(count):
                one(y)
        else:

            def body(y, carry):
                one(y)
                return carry

            lax.fori_loop(0, count, body, 0)

    def wait_bytes(ref, sem):
        pltpu.make_async_copy(ref, ref, sem).wait()

    near_rest = pl.ds(0, (n_gy - 1) * rows)
    last = gx == n_gx - 1
    crosses = border & (lax.rem(gy, 2) == 1)
    crossed = border & (lax.rem(gy, 2) == 0)

    def relay_across():
        wait_bytes(far_pack, far_recv.at[0])
        relay_copy(gy - 1, pl.ds(0, tall)).start()

    def next_to(w):
        return pltpu.roll(w, w.shape[0] - 1, 0) + pltpu.roll(w, 1, 0)

    def strip_image(side, k, z, left, right):
        c = side_cols(side, k)
        return diag[c, :] * z + horiz[c, :] * (4.0 * z - left - right) + column_part(z)

    def look_ahead():
        c1 = edge_cols[1]

        def take(direction, near, far, row):
            for k in range(2):
                near_coef[k, pl.ds(row, 1), :] = mini_in[direction, pl.ds(8 * side + 4 + k, 1), :]
            for k_side in range(2):
                given = mini_in.at[direction]
                wide[k_side, 0, pl.ds(near, 1), :] = given[pl.ds(8 * k_side, 1), :]
                wide[k_side, 0, pl.ds(far, 1), :] = given[pl.ds(8 * k_side + 1, 1), :]
                for k in (1, 2, 3):
                    wide[k_side, k, pl.ds(near, 1), :] = given[pl.ds(8 * k_side + k + 1, 1), :]

        wait_cases(lambda sides, beside: 16 * beside, mini_recv)
        pl.when(has_south)(functools.partial(take, 0, 7, 6, first_row - 1))
        pl.when(has_north)(functools.partial(take, 1, 8 + rows, 9 + rows, first_row + rows))
        z_edge, z_next, h_edge, d_edge = (wide[side, k] for k in range(4))
        v_edge = (
            d_edge * z_edge
            + h_edge * (4.0 * z_edge - z_next - next_to(z_edge))
            + column_part(z_edge)
        )
        beside = next_to(z_next)[8 : 8 + rows] + z_edge[8 : 8 + rows]
        z1 = z_next[8 : 8 + rows]
        z2 = frame_z[0, pl.ds(inward + (2 + side) * rows, rows), :]
        v_next = (
            diag[c1, :] * z1 + horiz[c1, :] * (4.0 * z1 - beside - z2) + column_part(z1)
        )
        z = precondition(jnp.concatenate([v_edge, v_next], 0))
        z_edge, z_next = z[: rows + 16], z[rows + 16 :]
        beside = next_to(z_edge)[8 : 8 + rows] + z_next
        z_edge = z_edge[8 : 8 + rows]
        near_out[2] = z_edge
        near_pack[2, own, :] = z_edge
        h_own, d_own = h_edge[8 : 8 + rows], d_edge[8 : 8 + rows]
        v = d_own * z_edge + h_own * (4.0 * z_edge - beside) + column_part(z_edge)
        pack[4] = precondition(v)
        pl.when(border)(send_far_last)

    def look_across():
        wait_cases(lambda sides, beside: sides * (3 * rows + 8 * beside), strip_recv)

        def take(k):
            row = 8 + rows if k % 2 else 7
            beyond[k // 2, pl.ds(row, 1), :] = corner_in[k, pl.ds(0, 1), :]

        for_corners(take, False)
        images_first = []
        for side in range(2):
            z_edge, z_next, h_edge, d_edge = (wide[side, k] for k in range(4))
            z_out = beyond[side]
            own_edge, own_out = z_edge[8 : 8 + rows], z_out[8 : 8 + rows]
            v_edge = (
                d_edge * z_edge
                + h_edge * (4.0 * z_edge - z_next - z_out - next_to(z_edge))
                + column_part(z_edge)
            )
            z1 = z_next[8 : 8 + rows]
            z2 = frame_z[0, pl.ds(inward + (2 + side) * rows, rows), :]
            v_next = strip_image(side, 1, z1, next_to(z_next)[8 : 8 + rows] + own_edge, z2)
            v_out = (
                edge_in[side, 2] * own_out
                + edge_in[side, 1]
                * (4.0 * own_out - edge_in[side, 0] - own_edge - next_to(z_out)[8 : 8 + rows])
                + column_part(own_out)
            )
            images_first += [v_edge, v_next, v_out]
        z = precondition(jnp.concatenate(images_first, 0))
        second = []
        each = 3 * rows + 16
        for side in range(2):
            part = z[side * each : (side + 1) * each]
            z_edge, z_next, z_out = part[: rows + 16], part[rows + 16 : each - rows], part[each - rows :]
            strip_out[pl.ds(side * rows, rows), :] = z_out
            beside = next_to(z_edge)[8 : 8 + rows]
            second.append(strip_image(side, 0, z_edge[8 : 8 + rows], beside + z_next, z_out))
        frame_z[2, pl.ds(0, 2 * rows), :] = precondition(jnp.concatenate(second, 0))

        def give(side):
            col_copy(2, side).start()
            outside[pl.ds(side * rows, rows), :] = strip_out[pl.ds(side * rows, rows), :]

        for_sides(give)

    def correct_early():
        pl.when(border)(lambda: wait_bytes(near_pack.at[:, near_rest], near_recv))
        gather_rows(0, tall, [(1, near_pack.at[0])])

        @pl.when(border)
        def _():
            pl.when(crossed)(lambda: wait_bytes(far_pack, relay_recv))
        gather_rows(0, tall, [(0, far_pack.at[0])])
        h_near, d_near = near_pack[1], near_coef[0]
        h_far, d_far = far_pack[2], far_pack[3]
        b_near, b_far = -(h_near * gathered[0]), -(h_far * gathered[1])
        v_far = stencil(far_pack[0], d_far, h_far) - h_far * far_pack[1] + b_far
        w_near = precondition(b_near)
        far = precondition(jnp.concatenate([b_far, v_far], 0), 1)
        w_far = far[:tall]
        strip[0] = b_near
        strip[1] = w_near
        strip[3] = far[tall:]
        strip[4] = near_pack[2] + w_near
        gather_rows(0, tall, [(0, strip.at[3]), (1, strip.at[4])])
        b_near = stencil(w_near, d_near, h_near) - h_near * gathered[0]
        b_far = stencil(w_far, d_far, h_far) - h_far * gathered[1]
        b_next = -(near_coef[1] * w_near)
        near = precondition(jnp.concatenate([b_near, b_next], 0))
        w_edge, w_next = near[:tall], near[tall:]
        strip[3] = b_near
        strip[4] = b_next
        strip[5] = precondition(b_far, 1)
        strip[6] = w_edge
        strip[7] = w_next
        strip[8] = along(w_next)
        strip[9] = stencil(w_edge, d_near, h_near) - h_near * w_next

    def strip_of(ref):
        return jnp.concatenate([ref[c, :] for c in edge_cols], 0)

    def add_to(key, value):
        extra[pl.ds(KEYS.index(key), 1), :] += value

    def correct_two():
        none = jnp.zeros((rows, levels), jnp.float32)
        changes = [
            [strip[0, own, :], none, none],
            [strip[3, own, :], strip[4, own, :], none],
        ]
        before = [strip_of(r0)]
        after = [before[0]]
        for t in range(2):
            old = strip_of(images.at[t])
            new = old + jnp.concatenate(changes[t], 0)
            before.append(old)
            after.append(new)
            for k in range(t + 1):
                images[t, edge_cols[k], :] = new[k * rows : (k + 1) * rows]
        for i, j in KEYS:
            if 0 < j < 3:
                add_to((i, j), product(after[i], after[j]) - product(before[i], before[j]))
        gather_rows(first_row, rows, [(2, strip.at[5])])

    def correct_third():
        c0, c1, c2 = edge_cols
        w_edge, w_next, beside = strip[6, own, :], strip[7, own, :], strip[8, own, :]
        h0, h1 = horiz[c0, :], horiz[c1, :]
        later = diag[c1, :] * w_next + h1 * (4.0 * w_next - beside - w_edge) + column_part(w_next)
        rest = jnp.concatenate([later, -(horiz[c2, :] * w_next)], 0)
        spaces_here = [strip_of(r0), strip_of(images.at[0]), strip_of(images.at[1])]
        old = strip_of(images.at[2])
        new_rest = old[rows:] + rest
        images[2, c1, :] = new_rest[:rows]
        images[2, c2, :] = new_rest[rows:]
        for i, space in enumerate(spaces_here):
            add_to((i, 3), product(space[rows:], rest))
        add_to((3, 3), product(new_rest, new_rest) - product(old, old))
        base = strip[9, own, :] - h0 * gathered[2, pl.ds(0, rows), :]
        wait_bytes(far_last, far_recv.at[1])
        gather_rows(first_row, rows, [(3, far_last)])
        b_edge = base - h0 * gathered[3, pl.ds(0, rows), :]
        new = old[:rows] + b_edge
        images[2, c0, :] = new
        for i, space in enumerate(spaces_here):
            add_to((i, 3), product(space[:rows], b_edge))
        add_to((3, 3), product(new, new))

    wait_count(3 * cells + 2 * levels, load_sem)
    for load in loads[5:]:
        load.wait()
    prepare_weights(0)
    terms = {}
    spaces = [r0]
    frame = [edge_columns(r0), r0[south_edge, :], r0[north_edge, :]]
    frame += [r0[side_cols(side, k), :] for k in (1, 2) for side in range(2)]
    send_first(jnp.concatenate(frame, 0))
    edge_horiz = edge_columns(horiz)
    for t in range(ITERS):
        image = images.at[t]
        z = precondition(spaces[-1][...])
        fields[t] = z
        newest = len(spaces) - 1
        for i in range(len(spaces)):
            terms[(i, newest)] = product(spaces[i][...], spaces[newest][...])
        image[...] = inner_image(z)
        if t == 0:
            prepare_weights(1)
            look_ahead()
        if t == 1:
            look_across()
        if t == 2:
            pl.when(crosses)(relay_across)
            correct_early()
            pl.when(border)(correct_two)
        receive_rows(t)
        image[south_edge, :] = image[south_edge, :] - horiz[south_edge, :] * from_south[t]
        image[north_edge, :] = image[north_edge, :] - horiz[north_edge, :] * from_north[t]
        inside = edge_columns(image)
        if t != 1:
            receive_cols(t)
        edges = inside - edge_horiz * outside[...]
        image[east_edge, :] = edges[:rows]
        image[west_edge, :] = edges[rows:]
        if t < ITERS - 1:
            send_rows(t + 1, jnp.concatenate([image[south_edge, :], image[north_edge, :]], 0))
        if t == 0:
            pl.when(border)(send_near)
        spaces.append(image)
    newest = len(spaces) - 1
    for i in range(len(spaces)):
        terms[(i, newest)] = product(spaces[i][...], spaces[newest][...])
    for k, key in enumerate(KEYS):
        partial[pl.ds(k, 1), :] = terms[key]

    @pl.when(border)
    def _():
        correct_third()

    height = -(-len(KEYS) // 8) * 8
    row_id = lax.broadcasted_iota(jnp.int32, (height, levels), 0)
    lane = lax.broadcasted_iota(jnp.int32, (height, levels), 1)
    stacked = jnp.where(row_id < len(KEYS), partial[...] + extra[...], 0.0)
    summed = jnp.sum(stacked, axis=1, keepdims=True)
    sums[me] = jnp.sum(jnp.where(lane == row_id, summed, 0.0), axis=0, keepdims=True)

    def tell(x, y):
        pltpu.make_async_remote_copy(
            src_ref=sums.at[me],
            dst_ref=sums.at[me],
            send_sem=sum_sent,
            recv_sem=sum_recv,
            device_id=(x, y),
            device_id_type=MESH,
        ).start()

    def tell_all(x, carry):
        for y in range(n_gy):
            pl.when(me != x * n_gy + y)(functools.partial(tell, x, y))
        return carry

    if n_all <= 64:
        for x in range(n_gx):
            tell_all(x, 0)
    else:
        lax.fori_loop(0, n_gx, tell_all, 0)
    def all_sent(sides, beside, border_part):
        per_side = 5 * rows + 8 * beside
        return sides * per_side + beside * (ITERS * cols + 16) + border_part * rows

    common = n_gy + 3 * (n_gy - 1) + 2 * n_gy
    for condition, sides, border_part in (
        (jnp.logical_not(border), 2, 0),
        (crosses, 1, common + 4 * n_gy),
        (crossed, 1, common),
    ):
        for beside, here in ((1, jnp.logical_not(between)), (2, between)):
            pl.when(condition & here)(
                functools.partial(wait_count, all_sent(sides, beside, border_part), sent)
            )

    @pl.when(border)
    def _():
        c0, c1, c2 = edge_cols
        fields[1, c0, :] += strip[1, own, :]
        fields[2, c0, :] += strip[6, own, :]
        fields[2, c1, :] += strip[7, own, :]

    others = sums.at[pl.ds(0, n_all - 1)]
    wait_bytes(others, sum_recv)
    out_totals[...] = jnp.sum(sums[...], axis=0)
    wait_bytes(others, sum_sent)


def finish(
    total_cells, all_totals, r0, fields, images, out_x, out_r, out_norms, x, r, norms_out, sem, norm_sem
):
    levels = r0.shape[-1]
    totals = all_totals[...]
    value = {
        key: jnp.broadcast_to(totals[:, k : k + 1], (8, levels)) for k, key in enumerate(KEYS)
    }

    rho, g0, g1, g2 = value[(0, 0)], value[(0, 1)], value[(0, 2)], value[(0, 3)]
    a00, a01, a02 = value[(1, 1)], value[(1, 2)], value[(1, 3)]
    a11, a12, a22 = value[(2, 2)], value[(2, 3)], value[(3, 3)]
    l10, l20, y0 = a01 / a00, a02 / a00, g0 / a00
    d1, e12, f1 = a11 - l10 * a01, a12 - l10 * a02, g1 - l10 * g0
    l21, y1 = e12 / d1, f1 / d1
    d2, f2 = a22 - l20 * a02 - l21 * e12, g2 - l20 * g0 - l21 * f1
    y2 = f2 / d2
    norm0 = rho - y0 * g0
    norm1 = norm0 - y1 * f1
    norm2 = norm1 - y2 * f2
    y1 = y1 - l21 * y2
    y0 = y0 - l10 * y1 - l20 * y2
    norm_lane = lax.broadcasted_iota(jnp.int32, (8, levels), 1)
    norms = jnp.where(norm_lane == 0, norm0, jnp.where(norm_lane == 1, norm1, norm2))
    norms_out[...] = norms[:1, :ITERS] / total_cells
    copies = [pltpu.make_async_copy(norms_out, out_norms, norm_sem)]
    copies[0].start()
    rows = r0.shape[0]
    pieces = 2 if rows % 16 == 0 else 1
    size = rows // pieces
    y0, y1, y2 = (jnp.tile(y, (size // 8, 1)) for y in (y0, y1, y2))
    for p in range(pieces):
        span = pl.ds(p * size, size)
        x[span] = y0 * fields[0, span] + y1 * fields[1, span] + y2 * fields[2, span]
        r[span] = (
            r0[span] - y0 * images[0, span] - y1 * images[1, span] - y2 * images[2, span]
        )
        for k, (src, dst) in enumerate(((x, out_x), (r, out_r))):
            copy = pltpu.make_async_copy(src.at[span], dst.at[span], sem.at[p, k])
            copy.start()
            copies.append(copy)
    for copy in copies:
        copy.wait()


def on_device(n_gx, n_gy, right_side, diagonal, horizontal, vertical, precond, edge_rows):
    rows, cols, levels = right_side.shape
    f32 = jnp.float32
    block = (rows * cols, levels)
    column = (n_gy * rows, levels)
    sems = pltpu.SemaphoreType.DMA
    meter_rows = 3 * rows * cols + 2 * levels + (16 + 10 * n_gy) * rows + 8 * cols + 64
    basis = pltpu.VMEM((ITERS,) + block, f32)
    fields, images, totals, start = pl.pallas_call(
        functools.partial(kernel, n_gx, n_gy, rows),
        out_shape=(basis, basis, pltpu.VMEM((1, levels), f32), pltpu.VMEM(block, f32)),
        in_specs=[ANY, ANY, ANY, ANY, ANY, ANY],
        out_specs=(VMEM, VMEM, VMEM, VMEM),
        scratch_shapes=[
            pltpu.VMEM(block, f32),
            pltpu.VMEM(block, f32),
            pltpu.VMEM((1, levels), f32),
            pltpu.VMEM((2 * levels, levels), f32),
            pltpu.VMEM((2, 2 * levels, 2 * levels), jnp.bfloat16),
            pltpu.VMEM((ITERS, 6 * rows + 2 * cols, levels), f32),
            pltpu.VMEM((5, rows, levels), f32),
            pltpu.VMEM((3, rows, levels), f32),
            pltpu.VMEM((2,) + column, f32),
            pltpu.VMEM((2, 16, levels), f32),
            pltpu.VMEM((2, 16, levels), f32),
            pltpu.VMEM((2, 4, rows + 16, levels), f32),
            pltpu.VMEM((2, 3, rows, levels), f32),
            pltpu.VMEM((2, 3, rows, levels), f32),
            pltpu.VMEM((4, 8, levels), f32),
            pltpu.VMEM((4, 8, levels), f32),
            pltpu.VMEM((2, rows + 16, levels), f32),
            pltpu.VMEM((ITERS, rows, levels), f32),
            pltpu.VMEM((ITERS, rows, levels), f32),
            pltpu.VMEM((ITERS, cols, levels), f32),
            pltpu.VMEM((ITERS, cols, levels), f32),
            pltpu.VMEM((4,) + column, f32),
            pltpu.VMEM((3,) + column, f32),
            pltpu.VMEM(column, f32),
            pltpu.VMEM((4,) + column, f32),
            pltpu.VMEM((10,) + column, f32),
            pltpu.VMEM((2 * rows, levels), f32),
            pltpu.VMEM((2 * rows, levels), f32),
            pltpu.VMEM((16, levels), f32),
            pltpu.VMEM((16, levels), f32),
            pltpu.VMEM((n_gx * n_gy, 1, levels), f32),
            pltpu.SMEM(edge_rows.shape, jnp.int32),
            pltpu.VMEM((meter_rows, levels), f32),
            sems(()),
            sems((2,)),
            sems(()),
            sems(()),
            sems((2,)),
            sems((ITERS,)),
            sems((2,)),
            sems(()),
            sems(()),
            sems(()),
            sems(()),
            sems(()),
        ],
        compiler_params=pltpu.CompilerParams(collective_id=0, has_side_effects=True),
    )(
        edge_rows,
        right_side.reshape(block),
        diagonal.reshape(block),
        horizontal.reshape(block),
        vertical.reshape(1, levels),
        precond,
    )
    in_vmem = functools.partial(
        pltpu.with_memory_space_constraint, memory_space=pltpu.VMEM
    )
    total_cells = float(rows * cols * levels * n_gx * n_gy)
    x, r, norms = pl.pallas_call(
        functools.partial(finish, total_cells),
        out_shape=(
            jax.ShapeDtypeStruct(block, f32),
            jax.ShapeDtypeStruct(block, f32),
            jax.ShapeDtypeStruct((1, ITERS), f32),
        ),
        in_specs=[VMEM, VMEM, VMEM, VMEM],
        out_specs=(ANY, ANY, ANY),
        scratch_shapes=[
            pltpu.VMEM(block, f32),
            pltpu.VMEM(block, f32),
            pltpu.VMEM((1, ITERS), f32),
            sems((2, 2)),
            sems(()),
        ],
    )(in_vmem(totals), in_vmem(start), in_vmem(fields), in_vmem(images))
    shape = right_side.shape
    return x.reshape(shape), r.reshape(shape), norms.reshape(ITERS)


def solution(mesh):
    n_gx, n_gy = mesh.shape["gx"], mesh.shape["gy"]
    field = P("gy", "gx", None)
    return jax.shard_map(
        functools.partial(on_device, n_gx, n_gy),
        mesh=mesh,
        in_specs=(field, field, field, P(), P(), P()),
        out_specs=(field, field, P()),
        check_vma=False,
    )
```
